512 devices in a mesh: groups: 2 (over y), blk: 32 (over z), head: 4 (over x), pair: 2 (over core).
Axes of the slice: x: 4, y: 2, z: 32, core: 2. Of those that a mesh axis runs over, the one named last changes fastest.
The devices are a block of a 4x8x32 slice.
Arguments:
- single: bfloat16 [2048, 384], P(('groups', 'blk')), parts along dimension 0, may hold values from -6 to 6
- pair: bfloat16 [2048, 32, 32, 128], P(('groups', 'blk'), None, 'pair'), parts along dimension 0, may hold values from -6 to 6
- frames: float32 [12, 2048], P(None, ('groups', 'blk')), parts along dimension 1, as said below
- chain: int32 [2048], P(('groups', 'blk')), parts along dimension 0, may hold values from 0 to 5, never falling along the last dimension, each value on 1 to 341 neighbouring positions
- mask: int32 [2048], P(('groups', 'blk')), parts along dimension 0, may hold values 0 or 1
- w_query: bfloat16 [384, 192], P(None, 'head'), may hold values from -0.3125 to 0.3125
- w_key_value: bfloat16 [384, 384], P(None, 'head'), may hold values from -0.3125 to 0.3125
- w_query_points: bfloat16 [384, 144], P(None, 'head'), may hold values from -0.3125 to 0.3125
- w_kv_points: bfloat16 [384, 432], P(None, 'head'), may hold values from -0.3125 to 0.3125
- w_pair_bias: bfloat16 [128, 12], P(None, 'head'), may hold values from -0.5 to 0.5
- head_weights: float32 [12], P('head'), may hold values from -9 to 1
- chain_bias: float32 [12], P('head'), may hold values from -3 to 3
- w_out: bfloat16 [12, 176, 384], P('head'), may hold values from -0.125 to 0.125
- out_gain: float32 [384], replicated, may hold values from 0.5 to 1.5
- w_backbone: bfloat16 [384, 6], replicated, may hold values from -0.3125 to 0.3125
Outputs:
- single_out: bfloat16 [2048, 384], P(('groups', 'blk')), parts along dimension 0
- frames_out: float32 [12, 2048], P(None, 'groups'), parts along dimension 1
The draws below stay inside these ranges and needn't reach their ends.
There are 2 independent parts, one for each index of `groups`. The reference program is written for one: setup_inputs(seed, part) draws one part's arguments, and reference() takes and returns one part's arrays. A program takes and returns all parts, laid end to end along the dimension named above; an argument that names none is the same for every part. Nothing has to cross between parts.
Inputs may be any that keep to these rules, and one draw needn't show every extreme that they name: `frames`: rows 0 to 8 of every column hold an orthonormal rotation matrix row by row; rows 9 to 11 the translation.
All inputs are finite; a program needn't handle non-finite values. No bound on the sum of `mask` on one device may be relied on, other than what follows from the above.
Results may differ from the reference program's by a relative error of at most 0.0048.
Values sent between devices are 32-bit elements; how exact they have to be, the bound alone decides.
A program may use at most 64 MiB of HBM per device.

```python
import math
import jax
import jax.numpy as jnp
import numpy as np
from jax import lax

C = 384
CZ = 128
HEADS = 12
CH = 16
PQ = 4
PV = 8
ROW_DEV = 32
N_RES = 1024
KEY_BLOCKS = 32
CAT = 176
N_BLK = 32


def draw_frames(key, part):
    key_turn = jax.random.fold_in(key, 101)
    key_walk = jax.random.fold_in(key, 202)
    quaternion = jax.random.normal(key_turn, (4, N_RES), jnp.float32)
    quaternion = quaternion / jnp.sqrt(jnp.sum(quaternion * quaternion, axis=0, keepdims=True) + 1e-12)
    quat_a = quaternion[0]
    quat_b = quaternion[1]
    quat_c = quaternion[2]
    quat_d = quaternion[3]
    spin = jnp.stack([quat_a * quat_a + quat_b * quat_b - quat_c * quat_c - quat_d * quat_d, 2.0 * (quat_b * quat_c - quat_a * quat_d), 2.0 * (quat_b * quat_d + quat_a * quat_c), 2.0 * (quat_b * quat_c + quat_a * quat_d), quat_a * quat_a - quat_b * quat_b + quat_c * quat_c - quat_d * quat_d, 2.0 * (quat_c * quat_d - quat_a * quat_b), 2.0 * (quat_b * quat_d - quat_a * quat_c), 2.0 * (quat_c * quat_d + quat_a * quat_b), quat_a * quat_a - quat_b * quat_b - quat_c * quat_c + quat_d * quat_d])
    steps = jax.random.normal(key_walk, (3, N_RES), jnp.float32) * 2.2
    walk = jnp.cumsum(steps, axis=1)
    walk = walk - jnp.mean(walk, axis=1, keepdims=True)
    return jnp.concatenate([spin, walk], axis=0).astype(jnp.float32)


def plant(array, stream_key, smallest, high):
    longest = array.shape.index(max(array.shape))
    spots = []
    for shift in (0, 1):
        where = [jax.random.randint(jax.random.fold_in(stream_key, axis), (), 0, length) for axis, length in enumerate(array.shape)]
        where[longest] = (where[longest] + shift) % array.shape[longest]
        spots.append(tuple(where))
    return array.at[spots[0]].set(smallest).at[spots[1]].set(high)


def block_scale(own_key, dims, cuts, least, largest):
    loudness = 1.0
    for dim, blocks in cuts:
        draws = jax.random.uniform(jax.random.fold_in(jax.random.fold_in(own_key, 6), dim), (blocks,), jnp.float32, least / len(cuts), largest / len(cuts))
        loudness = loudness * jnp.repeat(jnp.exp(draws), dims[dim] // blocks).reshape((-1,) + (1,) * (len(dims) - 1 - dim))
    return loudness


def length_profile(number_of, total, limit, slope):
    weights = [(1 << 20) // math.isqrt(rank ** slope) + 1 for rank in range(2, number_of + 1)]
    rest, counts = total - limit - (number_of - 1), [1] * (number_of - 1)
    while rest > 0:
        candidates = [i for i in range(number_of - 1) if counts[i] < limit]
        mass, left = sum([weights[i] for i in candidates]), rest
        for i in candidates:
            addition = min(limit - counts[i], max(1, left * weights[i] // mass), rest)
            counts[i] = counts[i] + addition
            rest = rest - addition
    return np.array([limit] + counts)


def uneven_parts(stream_key, number_of, total, limit, slope):
    if number_of == 2:
        one = jax.random.randint(stream_key, (), max(1, total - limit), min(limit, total - 1) + 1)
        return jnp.stack([one, total - one])
    tallies = jnp.asarray(length_profile(number_of, total, limit, slope), jnp.int32)
    twos = (number_of - 1) // 2
    source_of, taker = tallies[1:1 + 2 * twos:2], tallies[2:2 + 2 * twos:2]
    slack = jnp.minimum(source_of - 1, limit - taker)
    moved = jax.random.randint(jax.random.fold_in(stream_key, 1), (twos,), 0, 1 << 20) % (slack + 1)
    tallies = tallies.at[1:1 + 2 * twos:2].set(source_of - moved).at[2:2 + 2 * twos:2].set(taker + moved)
    return tallies[jax.random.permutation(jax.random.fold_in(stream_key, 2), number_of)]


def scatter_about(own_key, extent, scale, bound, split=(), held_as=jnp.bfloat16):
    entries = scale * jax.random.normal(own_key, extent, jnp.float32)
    if split:
        entries = entries * block_scale(own_key, extent, split, -0.22, 0.18)
    return jnp.clip(entries, -bound, bound).astype(held_as)


def setup_inputs(seed: int = 0, part: int = 0) -> dict:
    arg_keys = jax.random.split(jax.random.key(seed), 16)
    part_keys = jax.random.split(jax.random.fold_in(arg_keys[15], part), 16)
    single = scatter_about(part_keys[0], (N_RES, C), 1.0, 6.0, ((0, 32),))
    pair = scatter_about(part_keys[1], (N_RES, KEY_BLOCKS, ROW_DEV, CZ), 1.0, 6.0, ((0, 32), (2, 2)))
    frames = draw_frames(jax.random.fold_in(jax.random.fold_in(arg_keys[15], part), 71), part)
    chain = jnp.searchsorted(jnp.cumsum(uneven_parts(part_keys[3], 6, N_RES, N_RES // 3, 0)), jnp.arange(N_RES), side="right").astype(jnp.int32)
    mask = plant((jax.random.randint(part_keys[4], (N_RES,), 0, 8) < 7).astype(jnp.int32), jax.random.fold_in(part_keys[4], 1), 0, 1)
    w_query = scatter_about(arg_keys[5], (C, HEADS * CH), C ** -0.5, 0.3125, ((1, 4),))
    w_key_value = scatter_about(arg_keys[6], (C, HEADS * 2 * CH), C ** -0.5, 0.3125, ((1, 4),))
    w_query_points = scatter_about(arg_keys[7], (C, HEADS * PQ * 3), C ** -0.5, 0.3125, ((1, 4),))
    w_kv_points = scatter_about(arg_keys[8], (C, HEADS * (PQ + PV) * 3), C ** -0.5, 0.3125, ((1, 4),))
    w_pair_bias = scatter_about(arg_keys[9], (CZ, HEADS), CZ ** -0.5, 0.5, ((1, 4),))
    head_weights = jnp.clip(-9.0 + 10.0 * jax.random.uniform(arg_keys[10], (HEADS,), jnp.float32) ** block_scale(arg_keys[10], (HEADS,), ((0, 4),), -0.2, 0.2), -9.0, 1.0)
    chain_bias = jnp.clip(jax.random.uniform(arg_keys[11], (HEADS,), jnp.float32, -3.0, 3.0) * block_scale(arg_keys[11], (HEADS,), ((0, 4),), -0.4, 0.0), -3.0, 3.0)
    w_out = scatter_about(arg_keys[12], (HEADS, CAT, C), (HEADS * CAT) ** -0.5, 0.125, ((0, 4),))
    out_gain = jnp.clip(1.0 + 0.1 * jax.random.normal(arg_keys[13], (C,), jnp.float32), 0.5, 1.5)
    w_backbone = scatter_about(arg_keys[14], (C, 6), C ** -0.5, 0.3125)
    return dict(single=single, pair=pair, frames=frames, chain=chain, mask=mask, w_query=w_query, w_key_value=w_key_value, w_query_points=w_query_points, w_kv_points=w_kv_points, w_pair_bias=w_pair_bias, head_weights=head_weights, chain_bias=chain_bias, w_out=w_out, out_gain=out_gain, w_backbone=w_backbone)


HIGH = lax.Precision.HIGHEST
LOGIT_WEIGHT = math.sqrt(1.0 / 3.0)
MASK_PENALTY = 100000.0

def to_global(local, frames):
    rotation = frames[:9].reshape(3, 3, -1)
    moved = jnp.einsum('abn,ngb->nga', rotation, local, precision=HIGH)
    return moved + jnp.transpose(frames[9:12])[:, None, :]

def to_local(points, frames):
    rotation = frames[:9].reshape(3, 3, -1)
    moved = points - jnp.transpose(frames[9:12])[:, None, None, :]
    return jnp.einsum('abn,nhpa->nhpb', rotation, moved, precision=HIGH)

def compose(frames, motion):
    rotation = frames[:9].reshape(3, 3, -1)
    inverse = 1.0 / jnp.sqrt(1.0 + motion[:, 0] ** 2 + motion[:, 1] ** 2 + motion[:, 2] ** 2)
    quat_a = inverse
    quat_b = motion[:, 0] * inverse
    quat_c = motion[:, 1] * inverse
    quat_d = motion[:, 2] * inverse
    spin = jnp.stack([quat_a * quat_a + quat_b * quat_b - quat_c * quat_c - quat_d * quat_d, 2.0 * (quat_b * quat_c - quat_a * quat_d), 2.0 * (quat_b * quat_d + quat_a * quat_c), 2.0 * (quat_b * quat_c + quat_a * quat_d), quat_a * quat_a - quat_b * quat_b + quat_c * quat_c - quat_d * quat_d, 2.0 * (quat_c * quat_d - quat_a * quat_b), 2.0 * (quat_b * quat_d - quat_a * quat_c), 2.0 * (quat_c * quat_d + quat_a * quat_b), quat_a * quat_a - quat_b * quat_b - quat_c * quat_c + quat_d * quat_d]).reshape(3, 3, -1)
    new_rotation = jnp.einsum('abn,bcn->acn', rotation, spin, precision=HIGH)
    offset = jnp.einsum('abn,nb->an', rotation, motion[:, 3:6], precision=HIGH)
    return jnp.concatenate([new_rotation.reshape(9, -1), frames[9:12] + offset], axis=0)

def attention_logits(pair_rows, query_rows, query_points, query_chain, query_present, keys, key_points, key_chain, key_present, w_pair_bias, distance_scale, chain_bias):
    count_q = pair_rows.shape[0]
    count_k = pair_rows.shape[1]
    bias = jnp.dot(pair_rows.reshape(count_q * count_k, -1), w_pair_bias, preferred_element_type=jnp.float32).reshape(count_q, count_k, -1)
    dots = jnp.einsum('ihc,jhc->ijh', query_rows, keys, precision=HIGH) / math.sqrt(keys.shape[-1])
    gaps = query_points[:, None] - key_points[None]
    distance = lax.optimization_barrier(jnp.sum(gaps * gaps, axis=(3, 4)))
    differ = (query_chain[:, None] != key_chain[None, :]).astype(jnp.float32)
    logits = LOGIT_WEIGHT * (dots + bias - distance_scale * distance + chain_bias * differ[..., None])
    absent = 1.0 - query_present[:, None] * key_present[None, :]
    return logits - MASK_PENALTY * absent[..., None]

def reference(single, pair, frames, chain, mask, w_query, w_key_value, w_query_points, w_kv_points, w_pair_bias, head_weights, chain_bias, w_out, out_gain, w_backbone):
    count = N_RES
    query = jnp.dot(single, w_query, preferred_element_type=jnp.float32).reshape(count, HEADS, CH)
    key_value = jnp.dot(single, w_key_value, preferred_element_type=jnp.float32).reshape(count, HEADS, 2, CH)
    keys = key_value[:, :, 0]
    values = key_value[:, :, 1]
    query_local = jnp.dot(single, w_query_points, preferred_element_type=jnp.float32).reshape(count, HEADS * PQ, 3)
    query_points = to_global(query_local, frames).reshape(count, HEADS, PQ, 3)
    pair_local = jnp.dot(single, w_kv_points, preferred_element_type=jnp.float32).reshape(count, HEADS * (PQ + PV), 3)
    point_pairs = to_global(pair_local, frames).reshape(count, HEADS, PQ + PV, 3)
    key_points = point_pairs[:, :, :PQ]
    value_points = point_pairs[:, :, PQ:]
    distance_scale = jax.nn.softplus(head_weights) * math.sqrt(2.0 / (9.0 * PQ)) / 2.0
    chain_float = chain.astype(jnp.float32)
    present = mask.astype(jnp.float32)
    pair_flat = pair.reshape(count, count, CZ)
    w_flat = w_out.reshape(HEADS * CAT, C)

    def block_rows(start):
        pair_rows = lax.dynamic_slice_in_dim(pair_flat, start, ROW_DEV, 0)
        query_rows = lax.dynamic_slice_in_dim(query, start, ROW_DEV, 0)
        qpoint_rows = lax.dynamic_slice_in_dim(query_points, start, ROW_DEV, 0)
        chain_rows = lax.dynamic_slice_in_dim(chain_float, start, ROW_DEV, 0)
        present_rows = lax.dynamic_slice_in_dim(present, start, ROW_DEV, 0)
        frame_rows = lax.dynamic_slice_in_dim(frames, start, ROW_DEV, 1)
        logits = attention_logits(pair_rows, query_rows, qpoint_rows, chain_rows, present_rows, keys, key_points, chain_float, present, w_pair_bias, distance_scale, chain_bias)
        top = lax.optimization_barrier(jnp.max(logits, axis=1))
        weights = jnp.exp(logits - top[:, None, :])
        total = lax.optimization_barrier(jnp.sum(weights, axis=1))
        attended = jnp.einsum('ijh,jhc->ihc', weights, values, precision=HIGH) / total[..., None]
        pointed_global = jnp.einsum('ijh,jhpd->ihpd', weights, value_points, precision=HIGH) / total[..., None, None]
        rounded = lax.optimization_barrier(weights.astype(jnp.bfloat16)).astype(jnp.float32)
        paired = jnp.einsum('ijh,ijc->ihc', rounded, pair_rows.astype(jnp.float32), precision=HIGH) / total[..., None]
        pointed = to_local(pointed_global, frame_rows)
        point_norms = jnp.sqrt(lax.optimization_barrier(jnp.sum(pointed * pointed, axis=3)) + 1.0)
        joined = jnp.concatenate([attended, pointed.reshape(ROW_DEV, HEADS, PV * 3), point_norms, paired], axis=2).astype(jnp.bfloat16)
        return jnp.dot(joined.reshape(ROW_DEV, HEADS * CAT), w_flat, preferred_element_type=jnp.float32)
    starts = jnp.arange(N_BLK, dtype=jnp.int32) * ROW_DEV
    update = lax.map(block_rows, starts).reshape(count, C)
    mixed = single.astype(jnp.float32) + update
    centre = lax.optimization_barrier(jnp.mean(mixed, axis=1, keepdims=True))
    spread = lax.optimization_barrier(jnp.mean(jnp.square(mixed - centre), axis=1, keepdims=True))
    single_out = ((mixed - centre) * lax.rsqrt(spread + 1e-05) * out_gain).astype(jnp.bfloat16)
    motion = jnp.dot(single_out, w_backbone, preferred_element_type=jnp.float32)
    frames_out = compose(frames, motion)
    return (single_out, frames_out)
```

```python
import functools
import math

import jax
import jax.numpy as jnp
import numpy as np
from jax import lax
from jax.experimental import pallas as pl
from jax.experimental.pallas import tpu as pltpu
from jax.sharding import PartitionSpec as P

MESH = pl.DeviceIdType.MESH
HIGH = lax.Precision.HIGHEST
F32 = jnp.float32
BF16 = jnp.bfloat16
LW = math.sqrt(1.0 / 3.0)
MASK_PENALTY = 100000.0
LANES = 128
SUB = 8
NT = (((1,), (1,)), ((), ()))

CHAIN_LANE = 7
MASK_LANE = 15
ONE_LANE = 120
TOP_LANE = 121


def gather_plan(n, stride, fixed, hop, weight):
    low, high = -((n - 1) // 2), n // 2
    when, parent = {0: 0.0}, {}
    anchors = [0]
    for sign in (1, -1):
        for k in range(1, n):
            o = sign * k * stride
            if not (low <= o <= high) or abs(o) > n // 2 - 2:
                break
            anchors.append(o)
            parent[o] = (o - sign * stride, sign * stride)
            when[o] = when[o - sign * stride] + fixed + hop * stride
    for o in range(low, high + 1):
        if o in when:
            continue
        best = min(
            anchors,
            key=lambda a: (when[a] + fixed + (hop + weight) * abs(o - a), abs(a)),
        )
        parent[o] = (best, o - best)
        when[o] = when[best] + fixed + hop * abs(o - best)
    order = sorted(when, key=lambda o: (when[o], abs(o), o))
    children = {}
    for o, (p, delta) in parent.items():
        children.setdefault(p, []).append((o, delta))
    for p in children:
        children[p].sort(key=lambda c: (c[0] not in anchors, -abs(c[1])))
    return order, children


def constants(heads, ch, pq, pv):
    key_lane = lambda h, c: ((h * ch + c) // 4) * 8 + 3 + (h * ch + c) % 4
    kp_lane = lambda h, p, a: (p * 3 + a) * 8 + h
    v_lane = lambda h, c: h * ch + c
    vp_lane = lambda h, p, a: heads * ch + a * heads * pv + h * pv + p
    kv = np.zeros((heads * 2 * ch, 2 * LANES), np.float32)
    kp = np.zeros((heads * (pq + pv) * 3, 6 * LANES), np.float32)
    fr = np.zeros((16, 8 * LANES), np.float32)
    q = np.zeros((heads * ch, LANES), np.float32)
    qp = np.zeros((heads * pq * 3, 3 * LANES), np.float32)
    pa = np.zeros((LANES, LANES), np.float32)
    masks = np.zeros((3, SUB, LANES), np.float32)
    perm = np.zeros((2 * LANES, heads * (ch + 4 * pv)), np.float32)
    small = ch + 4 * pv
    for h in range(heads):
        for c in range(ch):
            kv[h * 2 * ch + c, key_lane(h, c)] = 1
            kv[h * 2 * ch + ch + c, LANES + v_lane(h, c)] = 1
            q[h * ch + c, key_lane(h, c)] = 1
            masks[0, h, key_lane(h, c)] = 1
            masks[2, h, v_lane(h, c)] = 1
            perm[v_lane(h, c), h * small + c] = 1
        for p in range(pq):
            for a in range(3):
                lane = kp_lane(h, p, a)
                masks[1, h, lane] = 1
                pa[lane, p * 3 + a] = 1
                for b in range(3):
                    kp[(h * (pq + pv) + p) * 3 + b, 2 * b * LANES + lane] = 1
                    qp[(h * pq + p) * 3 + b, b * LANES + lane] = 1
                    fr[3 * a + b, 2 * b * LANES + lane] = 1
                fr[9 + a, 6 * LANES + lane] = 1
        for p in range(pv):
            for a in range(3):
                lane = vp_lane(h, p, a)
                masks[2, h, lane] = 1
                perm[lane, h * small + ch + p * 3 + a] = 1
                for b in range(3):
                    kp[(h * (pq + pv) + pq + p) * 3 + b, (2 * b + 1) * LANES + lane] = 1
                    fr[3 * a + b, (2 * b + 1) * LANES + lane] = 1
                fr[9 + a, 7 * LANES + lane] = 1
            perm[LANES + vp_lane(h, p, 0), h * small + ch + 3 * pv + p] = 1
    masks[1, :heads, CHAIN_LANE] = 1
    masks[1, :heads, MASK_LANE] = 1
    pa[CHAIN_LANE, 12] = 1
    pa[MASK_LANE, 13] = 1
    fr[12, 6 * LANES + CHAIN_LANE] = 1
    fr[13, 6 * LANES + MASK_LANE] = 1
    fr[14, 7 * LANES + ONE_LANE] = 1
    return (kv, kp, fr, q, qp, pa, perm), masks.reshape(3 * SUB, LANES)


def pieces3(x):
    a = x.astype(BF16)
    r = x - a.astype(F32)
    b = r.astype(BF16)
    c = (r - b.astype(F32)).astype(BF16)
    return a, b, c


def select(x, onehot):
    m = x.shape[0]
    y = jnp.dot(jnp.concatenate(pieces3(x), axis=0), onehot, preferred_element_type=F32)
    return y[:m] + y[m : 2 * m] + y[2 * m :]


def roll(x, shift, axis):
    shift %= x.shape[axis]
    return x if shift == 0 else pltpu.roll(x, shift, axis)


def kernel(
    cfg,
    single,
    pair,
    frames,
    chain,
    mask,
    w_q,
    w_kv,
    w_qp,
    w_kvp,
    w_pb,
    head_w,
    chain_b,
    w_out,
    gain,
    w_bb,
    c_kv,
    c_kp,
    c_fr,
    c_q,
    c_qp,
    c_pa,
    c_perm,
    c_masks,
    out_single,
    out_frames,
    pv,
    buf,
    stack,
    ft,
    bias,
    qpb,
    qblk,
    kt,
    dots,
    wts,
    alpha,
    acc,
    mbuf,
    xbuf,
    fbuf,
    sbuf,
    wp,
    rb,
    rsel,
    pair_sem,
    send_sem,
    recv_sem,
    m_sem,
    x_send,
    x_recv,
    s_sem,
    f_send,
    f_recv,
):
    n, nx, heads, ch, pq, nv, half, chunk, order, children, deltas = cfg
    rows = 2 * half
    z = lax.axis_index("blk")
    x = lax.axis_index("head")
    p = lax.axis_index("pair")
    other = 1 - p
    slot_of = {o: i for i, o in enumerate(order)}

    def block(o):
        return lax.rem(z - o + 2 * n, n)

    pair_copies = []
    for o in order:
        copy = pltpu.make_async_copy(
            pair.at[:, block(o)], pv.at[:, slot_of[o]], pair_sem.at[slot_of[o]]
        )
        copy.start()
        pair_copies.append(copy)

    barrier = pltpu.get_barrier_semaphore()
    signals = 0
    for d in deltas:
        pl.semaphore_signal(
            barrier, inc=1, device_id={"blk": lax.rem(z + d + n, n)}, device_id_type=MESH
        )
        signals += 1
    for d in range(1, nx):
        pl.semaphore_signal(
            barrier, inc=1, device_id={"head": lax.rem(x + d, nx)}, device_id_type=MESH
        )
        signals += 1
    pl.semaphore_signal(barrier, inc=1, device_id={"pair": other}, device_id_type=MESH)
    signals += 1

    stack[...] = jnp.zeros_like(stack)
    stack[0:12, :] = frames[...]
    stack[12:13, :] = chain[...].astype(F32)
    stack[13:14, :] = mask[...].astype(F32)
    stack[14:15, :] = jnp.ones((1, rows), F32)
    eye = (
        lax.broadcasted_iota(jnp.int32, (rows, rows), 0)
        == lax.broadcasted_iota(jnp.int32, (rows, rows), 1)
    ).astype(F32)
    ft[...] = lax.dot_general(eye, stack[...], NT, precision=HIGH, preferred_element_type=F32)
    mine = pl.ds(pl.multiple_of(p * half, half), half)
    theirs = pl.ds(pl.multiple_of(other * half, half), half)
    ks = single[mine, :]
    key_value = jnp.dot(ks, w_kv[...], preferred_element_type=F32)
    key_local = jnp.dot(ks, w_kvp[...], preferred_element_type=F32)
    turn = select(ft[mine, :], c_fr[...])
    local = select(key_local, c_kp[...])
    width = 2 * LANES
    line = select(key_value, c_kv[...]) + turn[:, 3 * width :]
    for b in range(3):
        line += turn[:, b * width : (b + 1) * width] * local[:, b * width : (b + 1) * width]
    buf[0, 0] = line[:, :LANES]
    buf[0, 1] = line[:, LANES:]

    sends = []

    def relay(o):
        for child, delta in children.get(o, []):
            copy = pltpu.make_async_remote_copy(
                src_ref=buf.at[slot_of[o]],
                dst_ref=buf.at[slot_of[child]],
                send_sem=send_sem.at[slot_of[child]],
                recv_sem=recv_sem.at[slot_of[child]],
                device_id={"blk": lax.rem(z + delta + n, n)},
                device_id_type=MESH,
            )
            copy.start()
            sends.append(copy)

    arrived = set()

    def arrive(o):
        if o == 0 or o in arrived:
            return
        arrived.add(o)
        pltpu.make_async_remote_copy(
            src_ref=buf.at[slot_of[o]],
            dst_ref=buf.at[slot_of[o]],
            send_sem=send_sem.at[slot_of[o]],
            recv_sem=recv_sem.at[slot_of[o]],
            device_id={"blk": lax.rem(z + 1, n)},
            device_id_type=MESH,
        ).wait_recv()
        relay(o)

    pl.semaphore_wait(barrier, signals)
    relay(0)

    full = ft[...]
    query = jnp.dot(single[...], w_q[...], preferred_element_type=F32)
    query = select(query, c_q[...]) * (LW / math.sqrt(ch))
    q_local = select(jnp.dot(single[...], w_qp[...], preferred_element_type=F32), c_qp[...])
    q_turn = select(full, c_fr[...])
    q_line = q_turn[:, 3 * width : 3 * width + LANES]
    for b in range(3):
        q_line += (
            q_turn[:, b * width : b * width + LANES] * q_local[:, b * LANES : (b + 1) * LANES]
        )
    head_keys = c_masks[0:SUB, :]
    head_points = c_masks[SUB : 2 * SUB, :]
    head_values = c_masks[2 * SUB : 3 * SUB, :]
    qblk[...] = (query[:, None, :] * head_keys[None]).reshape(rows * SUB, LANES)
    spread = select((q_line[:, None, :] * head_points[None]).reshape(rows * SUB, LANES), c_pa[...])
    spread = spread.reshape(rows, SUB, LANES)
    marks = 3 * pq + 2
    for k in range(marks):
        qpb[:, k] = jnp.broadcast_to(spread[:, :, k : k + 1], (rows, SUB, LANES))

    head_row = lax.broadcasted_iota(jnp.int32, (SUB, LANES), 0)
    raw = jnp.zeros((SUB, LANES), F32)
    cross = jnp.zeros((SUB, LANES), F32)
    for h in range(heads):
        raw = jnp.where(head_row == h, head_w[h], raw)
        cross = jnp.where(head_row == h, chain_b[h] * LW, cross)
    soft = jnp.maximum(raw, 0.0) + jnp.log1p(jnp.exp(-jnp.abs(raw)))
    near = soft * (LW * math.sqrt(2.0 / (9.0 * pq)) / 2.0)

    eye_h = (
        lax.broadcasted_iota(jnp.int32, (SUB, heads), 0)
        == lax.broadcasted_iota(jnp.int32, (SUB, heads), 1)
    ).astype(BF16)
    w_bias = lax.dot_general(eye_h, w_pb[...], NT, preferred_element_type=F32).astype(BF16)

    for copy in pair_copies:
        copy.wait()

    keys = n * half

    def bias_of(i, _):
        bias[i] = LW * lax.dot_general(
            w_bias, pv[i].reshape(keys, LANES), NT, preferred_element_type=F32
        )
        return 0

    events = [o for o in order if children.get(o) and o != 0]
    lax.fori_loop(0, rows, bias_of, 0, unroll=4)

    short = w_out.shape[1] - LANES
    w_short = w_out[:, 0:short, :].reshape(heads * short, w_out.shape[2])
    wp[...] = jnp.dot(c_perm[...], w_short, preferred_element_type=F32).astype(BF16)
    mine_ft = ft[mine, :]
    for k in range(12):
        rb[k] = jnp.broadcast_to(mine_ft[:, k : k + 1], (half, LANES))
    lane = lax.broadcasted_iota(jnp.int32, (rows, LANES), 1)
    repeat = ((lane & (half - 1)) + p * half == lax.broadcasted_iota(jnp.int32, (rows, LANES), 0)).astype(BF16)
    wide = select(stack[...], repeat)
    lane8 = lax.broadcasted_iota(jnp.int32, (SUB, LANES), 1)
    part8 = lax.div(lane8, half)
    comp8 = lax.broadcasted_iota(jnp.int32, (SUB, LANES), 0) * (LANES // half) + part8
    for b in range(4):
        picked = jnp.zeros((SUB, LANES), F32)
        for k in range(12):
            source = (k - k % 3 + b if k < 9 else 3 * (k - 9) + b) if b < 3 else k
            if b == 3 and k < 9:
                continue
            picked = jnp.where(comp8 == k, wide[source : source + 1, :], picked)
        rsel[b] = picked
    eye_b = (
        lax.broadcasted_iota(jnp.int32, (SUB, w_bb.shape[1]), 0)
        == lax.broadcasted_iota(jnp.int32, (SUB, w_bb.shape[1]), 1)
    ).astype(BF16)
    w_motion = lax.dot_general(eye_b, w_bb[...], NT, preferred_element_type=F32).astype(BF16)

    span = chunk * half
    acc[...] = jnp.zeros_like(acc)
    alpha[...] = jnp.full(alpha.shape, -1e30, F32)
    for c in range(n // chunk):
        slots = slice(c * chunk, (c + 1) * chunk)
        for o in order[slots]:
            arrive(o)
        if c + 1 < n // chunk:
            pass
        kc = buf[slots, 0].reshape(span, LANES)
        vc = buf[slots, 1].reshape(span, LANES)
        kt[...] = kc.T.reshape(LANES // SUB, SUB, span)
        dots[...] = lax.dot_general(
            qblk[...], kc, NT, precision=HIGH, preferred_element_type=F32
        ).reshape(rows, SUB, span)
        chain_j = kt[0, 7:8, :]
        mask_j = kt[1, 7:8, :]

        def one_row(i, _):
            far = jnp.zeros((SUB, span), F32)
            for k in range(3 * pq):
                gap = qpb[i, k][:, :span] - kt[k]
                far += gap * gap
            differ = jnp.where(qpb[i, 3 * pq][:, :span] != chain_j, cross[:, :span], 0.0)
            absent = 1.0 - qpb[i, 3 * pq + 1][:, :span] * mask_j
            logits = (
                dots[i]
                + bias[i, :, c * span : (c + 1) * span]
                - near[:, :span] * far
                + differ
                - MASK_PENALTY * absent
            )
            old = alpha[i]
            top = jnp.maximum(old, jnp.max(logits, axis=1, keepdims=True))
            w = jnp.exp(logits - top[:, :span])
            wts[i] = w
            alpha[i] = top
            scale = jnp.exp(old - top)
            acc[i, 1] = acc[i, 1] * scale
            acc[i, 0] = acc[i, 0] * scale + jnp.dot(
                w.astype(BF16),
                pv[i, slots].reshape(span, LANES),
                preferred_element_type=F32,
            )
            return 0

        lax.fori_loop(0, rows, one_row, 0, unroll=4)
        acc[:, 1] += jnp.dot(
            wts[...].reshape(rows * SUB, span), vc, precision=HIGH, preferred_element_type=F32
        ).reshape(rows, SUB, LANES)

    lane3 = lax.broadcasted_iota(jnp.int32, (rows, SUB, LANES), 2)
    acc[:, 1] = jnp.where(lane3 == TOP_LANE, alpha[...], acc[:, 1])
    give = pltpu.make_async_remote_copy(
        src_ref=acc.at[theirs],
        dst_ref=mbuf,
        send_sem=m_sem.at[0],
        recv_sem=m_sem.at[1],
        device_id={"pair": other},
        device_id_type=MESH,
    )
    give.start()
    give.wait_recv()
    own_p, own_b = acc[mine, 0], acc[mine, 1]
    far_p, far_b = mbuf[:, 0], mbuf[:, 1]
    own_top, far_top = own_b[:, :, TOP_LANE : TOP_LANE + 1], far_b[:, :, TOP_LANE : TOP_LANE + 1]
    top = jnp.maximum(own_top, far_top)
    own_scale, far_scale = jnp.exp(own_top - top), jnp.exp(far_top - top)
    both_b = own_b * own_scale + far_b * far_scale
    total = both_b[:, :, ONE_LANE : ONE_LANE + 1]
    both_b = both_b / total * head_values[None]
    paired = (own_p * own_scale + far_p * far_scale) / total
    mbuf[:, 0] = paired
    sums = jnp.sum(both_b, axis=1)
    first = heads * ch
    third = heads * nv
    moved = [roll(sums, -a * third, 1) - rb[9 + a] for a in range(3)]
    pointed = [sum(rb[3 * a + b] * moved[a] for a in range(3)) for b in range(3)]
    norms = jnp.sqrt(pointed[0] * pointed[0] + pointed[1] * pointed[1] + pointed[2] * pointed[2] + 1.0)
    lane16 = lax.broadcasted_iota(jnp.int32, (half, LANES), 1)
    joined = sums
    for b in range(3):
        joined = jnp.where(
            (lane16 >= first + b * third) & (lane16 < first + (b + 1) * third),
            roll(pointed[b], b * third, 1),
            joined,
        )
    norms = jnp.where((lane16 >= first) & (lane16 < first + third), norms, 0.0)
    features = jnp.concatenate([joined, norms], axis=1).astype(BF16)
    update = jnp.dot(features, wp[...], preferred_element_type=F32)
    for h in range(heads):
        update += jnp.dot(
            mbuf[:, 0, h, :].astype(BF16), w_out[h, short:, :], preferred_element_type=F32
        )

    xbuf[x] = update
    x_copies = []
    for d in range(1, nx):
        copy = pltpu.make_async_remote_copy(
            src_ref=xbuf.at[x],
            dst_ref=xbuf.at[x],
            send_sem=x_send.at[d - 1],
            recv_sem=x_recv.at[d - 1],
            device_id={"head": lax.rem(x + d, nx)},
            device_id_type=MESH,
        )
        copy.start()
        x_copies.append(copy)
    for d in range(1, nx):
        source = lax.rem(x - d + nx, nx)
        pltpu.make_async_remote_copy(
            src_ref=xbuf.at[source],
            dst_ref=xbuf.at[source],
            send_sem=x_send.at[d - 1],
            recv_sem=x_recv.at[d - 1],
            device_id={"head": source},
            device_id_type=MESH,
        ).wait_recv()
    update = xbuf[0]
    for k in range(1, nx):
        update = update + xbuf[k]
    mixed = single[mine, :].astype(F32) + update
    count = mixed.shape[1]
    centre = jnp.sum(mixed, axis=1, keepdims=True) * (1.0 / count)
    apart = mixed - centre
    variance = jnp.sum(apart * apart, axis=1, keepdims=True) * (1.0 / count)
    result = (apart * lax.rsqrt(variance + 1e-05) * gain[...]).astype(BF16)
    out_single[mine, :] = result
    sbuf[0] = result.astype(F32)
    give_s = pltpu.make_async_remote_copy(
        src_ref=sbuf.at[0],
        dst_ref=sbuf.at[1],
        send_sem=s_sem.at[0],
        recv_sem=s_sem.at[1],
        device_id={"pair": other},
        device_id_type=MESH,
    )

    groups = LANES // half
    motion = lax.dot_general(
        w_motion,
        jnp.concatenate([result] * groups, axis=0),
        NT,
        preferred_element_type=F32,
    )
    m = [jnp.broadcast_to(motion[k : k + 1, :], (SUB, LANES)) for k in range(6)]
    qa = 1.0 / jnp.sqrt(1.0 + m[0] * m[0] + m[1] * m[1] + m[2] * m[2])
    qb, qc, qd = m[0] * qa, m[1] * qa, m[2] * qa
    aa, bb, cc, dd = qa * qa, qb * qb, qc * qc, qd * qd
    ab, ac, ad = qa * qb, qa * qc, qa * qd
    bc, bd, cd = qb * qc, qb * qd, qc * qd
    spin = [
        [aa + bb - cc - dd, 2.0 * (bc - ad), 2.0 * (bd + ac)],
        [2.0 * (bc + ad), aa - bb + cc - dd, 2.0 * (cd - ab)],
        [2.0 * (bd - ac), 2.0 * (cd + ab), aa - bb - cc + dd],
    ]
    column = lax.rem(comp8, 3)
    packed = rsel[3]
    for b in range(3):
        value = jnp.where(column == 0, spin[b][0], jnp.where(column == 1, spin[b][1], spin[b][2]))
        value = jnp.where(comp8 < 9, value, m[3 + b])
        packed = packed + rsel[b] * value
    lines = fbuf.shape[1]
    me = z * 2 + p
    fbuf[me] = packed[0:lines, :]

    f_copies = []
    steps = sorted(
        ((d, c) for d in range(n) for c in (0, 1) if (d, c) != (0, 0)),
        key=lambda s: (-min(s[0], n - s[0]), s[1]),
    )
    for d, c in steps:
        device = {"blk": lax.rem(z + d, n), "pair": p if c == 0 else other}
        copy = pltpu.make_async_remote_copy(
            src_ref=fbuf.at[me],
            dst_ref=fbuf.at[me],
            send_sem=f_send.at[2 * d + c],
            recv_sem=f_recv.at[2 * d + c],
            device_id=device,
            device_id_type=MESH,
        )
        copy.start()
        f_copies.append(copy)
    give_s.start()
    give_s.wait_recv()
    out_single[theirs, :] = sbuf[1].astype(BF16)
    for d, c in reversed(steps):
        source = lax.rem(z - d + n, n) * 2 + (p if c == 0 else other)
        pltpu.make_async_remote_copy(
            src_ref=fbuf.at[source],
            dst_ref=fbuf.at[source],
            send_sem=f_send.at[2 * d + c],
            recv_sem=f_recv.at[2 * d + c],
            device_id={"pair": other},
            device_id_type=MESH,
        ).wait_recv()

    gap = (lax.broadcasted_iota(jnp.int32, (SUB, LANES), 0) - part8) & (SUB - 1)
    for t in range(2 * n // groups):
        for line_number in range(2):
            tile = fbuf[t * groups : (t + 1) * groups, line_number, :]
            out = tile
            for s in range(1, groups):
                out = jnp.where(gap == s, roll(roll(tile, s, 0), -half * s, 1), out)
            height = 8 if line_number == 0 else 4
            out_frames[8 * line_number : 8 * line_number + height, t * LANES : (t + 1) * LANES] = out[:height]

    for copy in sends + x_copies + f_copies:
        copy.wait_send()
    give.wait_send()
    give_s.wait_send()


def body(n, nx, *args):
    (
        single,
        pair,
        frames,
        chain,
        mask,
        w_q,
        w_kv,
        w_qp,
        w_kvp,
        w_pb,
        head_w,
        chain_b,
        w_out,
        gain,
        w_bb,
    ) = args
    rows, half = single.shape[0], pair.shape[2]
    heads = w_pb.shape[1]
    ch = w_q.shape[1] // heads
    pq = w_qp.shape[1] // (3 * heads)
    nv = w_kvp.shape[1] // (3 * heads) - pq
    order, children = gather_plan(n, 6 if n >= 16 else 2, 0.9, 0.72, 0.4)
    deltas = sorted({d for kids in children.values() for _, d in kids})
    deltas = sorted(set(deltas) | {-d for d in deltas})
    deltas = [d for i, d in enumerate(deltas) if d % n not in {e % n for e in deltas[:i]}]
    chunk = min(8, n)
    cfg = (n, nx, heads, ch, pq, nv, half, chunk, order, children, deltas)
    hots, masks = constants(heads, ch, pq, nv)
    hots = [jnp.asarray(h, BF16) for h in hots]
    masks = jnp.asarray(masks, F32)
    vmem = pl.BlockSpec(memory_space=pltpu.VMEM)
    smem = pl.BlockSpec(memory_space=pltpu.SMEM)
    hbm = pl.BlockSpec(memory_space=pl.ANY)
    specs = [vmem, hbm, vmem, vmem, vmem, vmem, vmem, vmem, vmem, vmem, smem, smem]
    specs += [vmem] * (3 + len(hots) + 1)
    marks = 3 * pq + 2
    span = chunk * half
    width = w_out.shape[2]
    scratch = [
        pltpu.VMEM((rows, n, half, LANES), BF16),
        pltpu.VMEM((n, 2, half, LANES), F32),
        pltpu.VMEM((16, rows), F32),
        pltpu.VMEM((rows, 16), F32),
        pltpu.VMEM((rows, SUB, n * half), F32),
        pltpu.VMEM((rows, marks, SUB, LANES), F32),
        pltpu.VMEM((rows * SUB, LANES), F32),
        pltpu.VMEM((LANES // SUB, SUB, span), F32),
        pltpu.VMEM((rows, SUB, span), F32),
        pltpu.VMEM((rows, SUB, span), F32),
        pltpu.VMEM((rows, SUB, LANES), F32),
        pltpu.VMEM((rows, 2, SUB, LANES), F32),
        pltpu.VMEM((half, 2, SUB, LANES), F32),
        pltpu.VMEM((nx, half, width), F32),
        pltpu.VMEM((2 * n, 2, LANES), F32),
        pltpu.VMEM((2, half, width), F32),
        pltpu.VMEM((2 * LANES, width), BF16),
        pltpu.VMEM((12, half, LANES), F32),
        pltpu.VMEM((4, SUB, LANES), F32),
        pltpu.SemaphoreType.DMA((n,)),
        pltpu.SemaphoreType.DMA((n,)),
        pltpu.SemaphoreType.DMA((n,)),
        pltpu.SemaphoreType.DMA((2,)),
        pltpu.SemaphoreType.DMA((max(nx - 1, 1),)),
        pltpu.SemaphoreType.DMA((max(nx - 1, 1),)),
        pltpu.SemaphoreType.DMA((2,)),
        pltpu.SemaphoreType.DMA((2 * n,)),
        pltpu.SemaphoreType.DMA((2 * n,)),
    ]
    return pl.pallas_call(
        functools.partial(kernel, cfg),
        out_shape=(
            jax.ShapeDtypeStruct(single.shape, BF16),
            jax.ShapeDtypeStruct((12, n * rows), F32),
        ),
        in_specs=specs,
        out_specs=(vmem, vmem),
        scratch_shapes=scratch,
        compiler_params=pltpu.CompilerParams(collective_id=0, has_side_effects=True),
        name="layer",
    )(
        single,
        pair,
        frames,
        chain.reshape(1, rows),
        mask.reshape(1, rows),
        w_q,
        w_kv,
        w_qp,
        w_kvp,
        w_pb,
        head_w,
        chain_b,
        w_out,
        gain.reshape(1, -1),
        w_bb,
        *hots,
        masks,
    )


def solution(mesh):
    placed = (
        P(("groups", "blk"), None),
        P(("groups", "blk"), None, "pair", None),
        P(None, ("groups", "blk")),
        P(("groups", "blk")),
        P(("groups", "blk")),
        P(None, "head"),
        P(None, "head"),
        P(None, "head"),
        P(None, "head"),
        P(None, "head"),
        P("head"),
        P("head"),
        P("head", None, None),
        P(),
        P(),
    )
    return jax.shard_map(
        functools.partial(body, mesh.shape["blk"], mesh.shape["head"]),
        mesh=mesh,
        in_specs=placed,
        out_specs=(P(("groups", "blk"), None), P(None, "groups")),
        check_vma=False,
    )
```

```python
import functools
import math

import jax
import jax.numpy as jnp
import numpy as np
from jax import lax
from jax.experimental import pallas as pl
from jax.experimental.pallas import tpu as pltpu
from jax.sharding import PartitionSpec as P

MESH = pl.DeviceIdType.MESH
HIGH = lax.Precision.HIGHEST
F32 = jnp.float32
BF16 = jnp.bfloat16
LW = math.sqrt(1.0 / 3.0)
MASK_PENALTY = 100000.0
KEY_PATH = 9
LANES = 128
SUB = 8
NT = (((1,), (1,)), ((), ()))

CHAIN_LANE = 7
MASK_LANE = 15
ONE_LANE = 120
TOP_LANE = 121


def gather_plan(n, stride, fixed, hop, weight):
    low, high = -((n - 1) // 2), n // 2
    when, parent = {0: 0.0}, {}
    anchors = [0]
    for sign in (1, -1):
        for k in range(1, n):
            o = sign * k * stride
            if not (low <= o <= high) or abs(o) > n // 2 - 2:
                break
            anchors.append(o)
            parent[o] = (o - sign * stride, sign * stride)
            when[o] = when[o - sign * stride] + fixed + hop * stride
    for o in range(low, high + 1):
        if o in when:
            continue
        best = min(
            anchors,
            key=lambda a: (when[a] + fixed + (hop + weight) * abs(o - a), abs(a)),
        )
        parent[o] = (best, o - best)
        when[o] = when[best] + fixed + hop * abs(o - best)
    order = sorted(when, key=lambda o: (o not in anchors, when[o], abs(o), o))
    anchors = [o for o in order if o in anchors]
    children = {}
    for o, (p, delta) in parent.items():
        children.setdefault(p, []).append((o, delta))
    for p in children:
        children[p].sort(key=lambda c: (c[0] not in anchors, -abs(c[1])))
    return order, anchors, children


def constants(heads, ch, pq, pv):
    key_lane = lambda h, c: ((h * ch + c) // 4) * 8 + 3 + (h * ch + c) % 4
    kp_lane = lambda h, p, a: (p * 3 + a) * 8 + h
    v_lane = lambda h, c: h * ch + c
    vp_lane = lambda h, p, a: heads * ch + a * heads * pv + h * pv + p
    kv = np.zeros((heads * 2 * ch, 2 * LANES), np.float32)
    kp = np.zeros((heads * (pq + pv) * 3, 6 * LANES), np.float32)
    fr = np.zeros((16, 8 * LANES), np.float32)
    q = np.zeros((heads * ch, LANES), np.float32)
    qp = np.zeros((heads * pq * 3, 3 * LANES), np.float32)
    pa = np.zeros((LANES, LANES), np.float32)
    masks = np.zeros((3, SUB, LANES), np.float32)
    perm = np.zeros((2 * LANES, heads * (ch + 4 * pv)), np.float32)
    small = ch + 4 * pv
    for h in range(heads):
        for c in range(ch):
            kv[h * 2 * ch + c, key_lane(h, c)] = 1
            kv[h * 2 * ch + ch + c, LANES + v_lane(h, c)] = 1
            q[h * ch + c, key_lane(h, c)] = 1
            masks[0, h, key_lane(h, c)] = 1
            masks[2, h, v_lane(h, c)] = 1
            perm[v_lane(h, c), h * small + c] = 1
        for p in range(pq):
            for a in range(3):
                lane = kp_lane(h, p, a)
                masks[1, h, lane] = 1
                pa[lane, p * 3 + a] = 1
                for b in range(3):
                    kp[(h * (pq + pv) + p) * 3 + b, 2 * b * LANES + lane] = 1
                    qp[(h * pq + p) * 3 + b, b * LANES + lane] = 1
                    fr[3 * a + b, 2 * b * LANES + lane] = 1
                fr[9 + a, 6 * LANES + lane] = 1
        for p in range(pv):
            for a in range(3):
                lane = vp_lane(h, p, a)
                masks[2, h, lane] = 1
                perm[lane, h * small + ch + p * 3 + a] = 1
                for b in range(3):
                    kp[(h * (pq + pv) + pq + p) * 3 + b, (2 * b + 1) * LANES + lane] = 1
                    fr[3 * a + b, (2 * b + 1) * LANES + lane] = 1
                fr[9 + a, 7 * LANES + lane] = 1
            perm[LANES + vp_lane(h, p, 0), h * small + ch + 3 * pv + p] = 1
    masks[1, :heads, CHAIN_LANE] = 1
    masks[1, :heads, MASK_LANE] = 1
    pa[CHAIN_LANE, 12] = 1
    pa[MASK_LANE, 13] = 1
    fr[12, 6 * LANES + CHAIN_LANE] = 1
    fr[13, 6 * LANES + MASK_LANE] = 1
    fr[14, 7 * LANES + ONE_LANE] = 1
    return (kv, kp, fr, q, qp, pa, perm), masks.reshape(3 * SUB, LANES)


def pieces3(x):
    a = x.astype(BF16)
    r = x - a.astype(F32)
    b = r.astype(BF16)
    c = (r - b.astype(F32)).astype(BF16)
    return a, b, c


def select(x, onehot):
    m = x.shape[0]
    y = jnp.dot(jnp.concatenate(pieces3(x), axis=0), onehot, preferred_element_type=F32)
    return y[:m] + y[m : 2 * m] + y[2 * m :]


def roll(x, shift, axis):
    shift %= x.shape[axis]
    return x if shift == 0 else pltpu.roll(x, shift, axis)


def kernel(
    cfg,
    pair,
    *refs,
):
    n_loads = cfg[-1]
    sources, (out_single, out_frames) = refs[:n_loads], refs[n_loads : n_loads + 2]
    held = refs[n_loads + 2 : 2 * n_loads + 2]
    run(cfg[:-1], pair, sources, held, out_single, out_frames, *refs[2 * n_loads + 2 :])


def run(
    cfg,
    pair,
    sources,
    held,
    out_single,
    out_frames,
    load_sem,
    pv,
    buf,
    stack,
    ft,
    bias,
    qpb,
    qblk,
    kt,
    dots,
    wts,
    alpha,
    acc,
    mbuf,
    xbuf,
    fbuf,
    sbuf,
    wp,
    rb,
    rsel,
    pair_sem,
    send_sem,
    recv_sem,
    m_sem,
    x_sem,
    s_sem,
    f_sem,
):
    n, nx, heads, ch, pq, nv, half, chunk, order, anchors, children, deltas = cfg
    rows = 2 * half
    z = lax.axis_index("blk")
    x = lax.axis_index("head")
    p = lax.axis_index("pair")
    other = 1 - p
    slot_of = {o: i for i, o in enumerate(order)}

    group_of = {o: i for i, o in enumerate(anchors)}
    for i, o in enumerate(order[len(anchors) :], len(anchors)):
        group_of[o] = len(anchors) + i // chunk

    def block(o):
        return lax.rem(z - o + 2 * n, n)

    barrier = pltpu.get_barrier_semaphore()
    signals = 0
    for d in deltas:
        pl.semaphore_signal(
            barrier, inc=1, device_id={"blk": lax.rem(z + d + n, n)}, device_id_type=MESH
        )
        signals += 1
    for d in range(1, nx):
        pl.semaphore_signal(
            barrier, inc=1, device_id={"head": lax.rem(x + d, nx)}, device_id_type=MESH
        )
        signals += 1
    pl.semaphore_signal(barrier, inc=1, device_id={"pair": other}, device_id_type=MESH)
    signals += 1

    loads = [
        pltpu.make_async_copy(source, place, load_sem.at[k])
        for k, (source, place) in enumerate(zip(sources, held))
    ]
    for copy in loads:
        copy.start()
    (frames, chain, mask, single, w_kv, w_kvp, c_fr, c_kp, c_kv) = held[:KEY_PATH]
    (w_q, w_qp, w_pb, head_w, chain_b, gain, w_bb, w_out, c_q, c_qp, c_pa, c_perm, c_masks) = held[
        KEY_PATH:
    ]

    for copy in loads[:KEY_PATH]:
        copy.wait()
    for o in order:
        pltpu.make_async_copy(pair.at[:, block(o)], pv.at[:, slot_of[o]], pair_sem).start()

    stack[...] = jnp.zeros_like(stack)
    stack[0:12, :] = frames[...]
    stack[12:13, :] = chain[...].astype(F32)
    stack[13:14, :] = mask[...].astype(F32)
    stack[14:15, :] = jnp.ones((1, rows), F32)
    eye = (
        lax.broadcasted_iota(jnp.int32, (rows, rows), 0)
        == lax.broadcasted_iota(jnp.int32, (rows, rows), 1)
    ).astype(F32)
    ft[...] = lax.dot_general(eye, stack[...], NT, precision=HIGH, preferred_element_type=F32)
    mine = pl.ds(pl.multiple_of(p * half, half), half)
    theirs = pl.ds(pl.multiple_of(other * half, half), half)
    ks = single[mine, :]
    key_value = lax.dot_general(ks, w_kv[...], NT, preferred_element_type=F32)
    key_local = lax.dot_general(ks, w_kvp[...], NT, preferred_element_type=F32)
    turn = select(ft[mine, :], c_fr[...])
    local = select(key_local, c_kp[...])
    width = 2 * LANES
    line = select(key_value, c_kv[...]) + turn[:, 3 * width :]
    for b in range(3):
        line += turn[:, b * width : (b + 1) * width] * local[:, b * width : (b + 1) * width]
    buf[0, 0] = line[:, :LANES]
    buf[0, 1] = line[:, LANES:]

    def relay(o):
        for child, delta in children.get(o, []):
            pltpu.make_async_remote_copy(
                src_ref=buf.at[slot_of[o]],
                dst_ref=buf.at[slot_of[child]],
                send_sem=send_sem,
                recv_sem=recv_sem.at[group_of[child]],
                device_id={"blk": lax.rem(z + delta + n, n)},
                device_id_type=MESH,
            ).start()

    def arrive(first, last, group):
        pltpu.make_async_remote_copy(
            src_ref=buf.at[first:last],
            dst_ref=buf.at[first:last],
            send_sem=send_sem,
            recv_sem=recv_sem.at[group],
            device_id={"blk": lax.rem(z + 1, n)},
            device_id_type=MESH,
        ).wait_recv()

    pl.semaphore_wait(barrier, signals)
    relay(0)

    for copy in loads[KEY_PATH:]:
        copy.wait()
    full = ft[...]
    query = lax.dot_general(single[...], w_q[...], NT, preferred_element_type=F32)
    query = select(query, c_q[...]) * (LW / math.sqrt(ch))
    q_local = select(
        lax.dot_general(single[...], w_qp[...], NT, preferred_element_type=F32), c_qp[...]
    )
    q_turn = select(full, c_fr[...])
    q_line = q_turn[:, 3 * width : 3 * width + LANES]
    for b in range(3):
        q_line += (
            q_turn[:, b * width : b * width + LANES] * q_local[:, b * LANES : (b + 1) * LANES]
        )
    head_keys = c_masks[0:SUB, :]
    head_points = c_masks[SUB : 2 * SUB, :]
    head_values = c_masks[2 * SUB : 3 * SUB, :]
    qblk[...] = (query[:, None, :] * head_keys[None]).reshape(rows * SUB, LANES)
    spread = select((q_line[:, None, :] * head_points[None]).reshape(rows * SUB, LANES), c_pa[...])
    spread = spread.reshape(rows, SUB, LANES)
    marks = 3 * pq + 2
    for k in range(marks):
        qpb[:, k] = jnp.broadcast_to(spread[:, :, k : k + 1], (rows, SUB, LANES))

    diagonal = lax.broadcasted_iota(jnp.int32, (SUB, heads), 0) == lax.broadcasted_iota(
        jnp.int32, (SUB, heads), 1
    )

    def down(row):
        column = jnp.sum(jnp.where(diagonal, row, 0.0), axis=1, keepdims=True)
        return jnp.broadcast_to(column, (SUB, LANES))

    raw = down(head_w[...])
    cross = down(chain_b[...]) * LW
    soft = jnp.maximum(raw, 0.0) + jnp.log1p(jnp.exp(-jnp.abs(raw)))
    near = soft * (LW * math.sqrt(2.0 / (9.0 * pq)) / 2.0)

    w_bias = jnp.dot(diagonal.astype(BF16), w_pb[...], preferred_element_type=F32).astype(BF16)

    pltpu.make_async_copy(pair, pv, pair_sem).wait()

    keys = n * half

    def bias_of(i, _):
        bias[i] = LW * lax.dot_general(
            w_bias, pv[i].reshape(keys, LANES), NT, preferred_element_type=F32
        )
        return 0

    lax.fori_loop(0, rows, bias_of, 0, unroll=8)

    short = w_out.shape[1] - LANES
    w_short = w_out[:, 0:short, :].reshape(heads * short, w_out.shape[2])
    wp[...] = jnp.dot(c_perm[...], w_short, preferred_element_type=F32).astype(BF16)
    mine_ft = ft[mine, :]
    for k in range(12):
        rb[k] = jnp.broadcast_to(mine_ft[:, k : k + 1], (half, LANES))
    lane = lax.broadcasted_iota(jnp.int32, (rows, LANES), 1)
    repeat = ((lane & (half - 1)) + p * half == lax.broadcasted_iota(jnp.int32, (rows, LANES), 0)).astype(BF16)
    wide = select(stack[...], repeat)
    lane8 = lax.broadcasted_iota(jnp.int32, (SUB, LANES), 1)
    part8 = lax.div(lane8, half)
    comp8 = lax.broadcasted_iota(jnp.int32, (SUB, LANES), 0) * (LANES // half) + part8
    for b in range(4):
        picked = jnp.zeros((SUB, LANES), F32)
        for k in range(12):
            source = (k - k % 3 + b if k < 9 else 3 * (k - 9) + b) if b < 3 else k
            if b == 3 and k < 9:
                continue
            picked = jnp.where(comp8 == k, wide[source : source + 1, :], picked)
        rsel[b] = picked
    eye_b = (
        lax.broadcasted_iota(jnp.int32, (SUB, w_bb.shape[0]), 0)
        == lax.broadcasted_iota(jnp.int32, (SUB, w_bb.shape[0]), 1)
    ).astype(BF16)
    w_motion = jnp.dot(eye_b, w_bb[...], preferred_element_type=F32).astype(BF16)

    for i, o in enumerate(anchors):
        if o != 0:
            arrive(i, i + 1, group_of[o])
            relay(o)

    span = chunk * half
    acc[...] = jnp.zeros_like(acc)
    alpha[...] = jnp.full(alpha.shape, -1e30, F32)
    for c in range(n // chunk):
        slots = slice(c * chunk, (c + 1) * chunk)
        first, last = max(len(anchors), c * chunk), (c + 1) * chunk
        if first < last:
            arrive(first, last, len(anchors) + c)
        kc = buf[slots, 0].reshape(span, LANES)
        vc = buf[slots, 1].reshape(span, LANES)
        kt[...] = kc.T.reshape(LANES // SUB, SUB, span)
        dots[...] = lax.dot_general(
            qblk[...], kc, NT, precision=HIGH, preferred_element_type=F32
        ).reshape(rows, SUB, span)
        chain_j = kt[0, 7:8, :]
        mask_j = kt[1, 7:8, :]

        def one_row(i, _):
            far = jnp.zeros((SUB, span), F32)
            for k in range(3 * pq):
                gap = qpb[i, k][:, :span] - kt[k]
                far += gap * gap
            differ = jnp.where(qpb[i, 3 * pq][:, :span] != chain_j, cross[:, :span], 0.0)
            absent = 1.0 - qpb[i, 3 * pq + 1][:, :span] * mask_j
            logits = (
                dots[i]
                + bias[i, :, c * span : (c + 1) * span]
                - near[:, :span] * far
                + differ
                - MASK_PENALTY * absent
            )
            old = alpha[i]
            top = jnp.maximum(old, jnp.max(logits, axis=1, keepdims=True))
            w = jnp.exp(logits - top[:, :span])
            wts[i] = w
            alpha[i] = top
            scale = jnp.exp(old - top)
            acc[i, 1] = acc[i, 1] * scale
            acc[i, 0] = acc[i, 0] * scale + jnp.dot(
                w.astype(BF16),
                pv[i, slots].reshape(span, LANES),
                preferred_element_type=F32,
            )
            return 0

        lax.fori_loop(0, rows, one_row, 0, unroll=16)
        acc[:, 1] += jnp.dot(
            wts[...].reshape(rows * SUB, span), vc, precision=HIGH, preferred_element_type=F32
        ).reshape(rows, SUB, LANES)

    lane3 = lax.broadcasted_iota(jnp.int32, (rows, SUB, LANES), 2)
    acc[:, 1] = jnp.where(lane3 == TOP_LANE, alpha[...], acc[:, 1])
    give = pltpu.make_async_remote_copy(
        src_ref=acc.at[theirs],
        dst_ref=mbuf,
        send_sem=m_sem.at[0],
        recv_sem=m_sem.at[1],
        device_id={"pair": other},
        device_id_type=MESH,
    )
    give.start()
    give.wait_recv()
    own_p, own_b = acc[mine, 0], acc[mine, 1]
    far_p, far_b = mbuf[:, 0], mbuf[:, 1]
    own_top, far_top = own_b[:, :, TOP_LANE : TOP_LANE + 1], far_b[:, :, TOP_LANE : TOP_LANE + 1]
    top = jnp.maximum(own_top, far_top)
    own_scale, far_scale = jnp.exp(own_top - top), jnp.exp(far_top - top)
    both_b = own_b * own_scale + far_b * far_scale
    total = both_b[:, :, ONE_LANE : ONE_LANE + 1]
    both_b = both_b / total * head_values[None]
    paired = (own_p * own_scale + far_p * far_scale) / total
    mbuf[:, 0] = paired
    sums = jnp.sum(both_b, axis=1)
    first = heads * ch
    third = heads * nv
    moved = [roll(sums, -a * third, 1) - rb[9 + a] for a in range(3)]
    pointed = [sum(rb[3 * a + b] * moved[a] for a in range(3)) for b in range(3)]
    norms = jnp.sqrt(pointed[0] * pointed[0] + pointed[1] * pointed[1] + pointed[2] * pointed[2] + 1.0)
    lane16 = lax.broadcasted_iota(jnp.int32, (half, LANES), 1)
    joined = sums
    for b in range(3):
        joined = jnp.where(
            (lane16 >= first + b * third) & (lane16 < first + (b + 1) * third),
            roll(pointed[b], b * third, 1),
            joined,
        )
    norms = jnp.where((lane16 >= first) & (lane16 < first + third), norms, 0.0)
    features = jnp.concatenate([joined, norms], axis=1).astype(BF16)
    update = jnp.dot(features, wp[...], preferred_element_type=F32)
    for h in range(heads):
        update += jnp.dot(
            mbuf[:, 0, h, :].astype(BF16), w_out[h, short:, :], preferred_element_type=F32
        )

    xbuf[x] = update
    for d in range(1, nx):
        pltpu.make_async_remote_copy(
            src_ref=xbuf.at[x],
            dst_ref=xbuf.at[x],
            send_sem=x_sem.at[0],
            recv_sem=x_sem.at[1],
            device_id={"head": lax.rem(x + d, nx)},
            device_id_type=MESH,
        ).start()
    x_all = pltpu.make_async_remote_copy(
        src_ref=xbuf.at[0 : nx - 1],
        dst_ref=xbuf.at[0 : nx - 1],
        send_sem=x_sem.at[0],
        recv_sem=x_sem.at[1],
        device_id={"head": lax.rem(x + 1, nx)},
        device_id_type=MESH,
    )
    if nx > 1:
        x_all.wait_recv()
    update = xbuf[0]
    for k in range(1, nx):
        update = update + xbuf[k]
    mixed = single[mine, :].astype(F32) + update
    count = mixed.shape[1]
    gains = jnp.concatenate([gain[k : k + 1, :] for k in range(count // LANES)], axis=1)
    centre = jnp.sum(mixed, axis=1, keepdims=True) * (1.0 / count)
    apart = mixed - centre
    variance = jnp.sum(apart * apart, axis=1, keepdims=True) * (1.0 / count)
    result = (apart * lax.rsqrt(variance + 1e-05) * gains).astype(BF16)
    out_single[mine, :] = result
    sbuf[0] = result.astype(F32)
    give_s = pltpu.make_async_remote_copy(
        src_ref=sbuf.at[0],
        dst_ref=sbuf.at[1],
        send_sem=s_sem.at[0],
        recv_sem=s_sem.at[1],
        device_id={"pair": other},
        device_id_type=MESH,
    )

    groups = LANES // half
    motion = lax.dot_general(
        w_motion,
        jnp.concatenate([result] * groups, axis=0),
        NT,
        preferred_element_type=F32,
    )
    m = [jnp.broadcast_to(motion[k : k + 1, :], (SUB, LANES)) for k in range(6)]
    qa = 1.0 / jnp.sqrt(1.0 + m[0] * m[0] + m[1] * m[1] + m[2] * m[2])
    qb, qc, qd = m[0] * qa, m[1] * qa, m[2] * qa
    aa, bb, cc, dd = qa * qa, qb * qb, qc * qc, qd * qd
    ab, ac, ad = qa * qb, qa * qc, qa * qd
    bc, bd, cd = qb * qc, qb * qd, qc * qd
    spin = [
        [aa + bb - cc - dd, 2.0 * (bc - ad), 2.0 * (bd + ac)],
        [2.0 * (bc + ad), aa - bb + cc - dd, 2.0 * (cd - ab)],
        [2.0 * (bd - ac), 2.0 * (cd + ab), aa - bb - cc + dd],
    ]
    column = lax.rem(comp8, 3)
    packed = rsel[3]
    for b in range(3):
        value = jnp.where(column == 0, spin[b][0], jnp.where(column == 1, spin[b][1], spin[b][2]))
        value = jnp.where(comp8 < 9, value, m[3 + b])
        packed = packed + rsel[b] * value
    lines = fbuf.shape[1]
    me = z * 2 + p
    fbuf[me] = packed[0:lines, :]

    steps = sorted(
        ((d, c) for d in range(n) for c in (0, 1) if (d, c) != (0, 0)),
        key=lambda s: (-min(s[0], n - s[0]), s[1]),
    )
    for d, c in steps:
        device = {"blk": lax.rem(z + d, n), "pair": p if c == 0 else other}
        pltpu.make_async_remote_copy(
            src_ref=fbuf.at[me],
            dst_ref=fbuf.at[me],
            send_sem=f_sem.at[0],
            recv_sem=f_sem.at[1],
            device_id=device,
            device_id_type=MESH,
        ).start()
    give_s.start()
    give_s.wait_recv()
    out_single[theirs, :] = sbuf[1].astype(BF16)
    f_all = pltpu.make_async_remote_copy(
        src_ref=fbuf.at[0 : 2 * n - 1],
        dst_ref=fbuf.at[0 : 2 * n - 1],
        send_sem=f_sem.at[0],
        recv_sem=f_sem.at[1],
        device_id={"pair": other},
        device_id_type=MESH,
    )
    f_all.wait_recv()

    gap = (lax.broadcasted_iota(jnp.int32, (SUB, LANES), 0) - part8) & (SUB - 1)
    for t in range(2 * n // groups):
        for line_number in range(2):
            tile = fbuf[t * groups : (t + 1) * groups, line_number, :]
            out = tile
            for s in range(1, groups):
                out = jnp.where(gap == s, roll(roll(tile, s, 0), -half * s, 1), out)
            height = 8 if line_number == 0 else 4
            out_frames[8 * line_number : 8 * line_number + height, t * LANES : (t + 1) * LANES] = out[:height]

    pltpu.make_async_remote_copy(
        src_ref=buf.at[0 : n - 1],
        dst_ref=buf.at[0 : n - 1],
        send_sem=send_sem,
        recv_sem=recv_sem.at[0],
        device_id={"blk": lax.rem(z + 1, n)},
        device_id_type=MESH,
    ).wait_send()
    if nx > 1:
        x_all.wait_send()
    f_all.wait_send()
    give.wait_send()
    give_s.wait_send()


def body(n, nx, *args):
    (
        single,
        pair,
        frames,
        chain,
        mask,
        w_q,
        w_kv,
        w_qp,
        w_kvp,
        w_pb,
        head_w,
        chain_b,
        w_out,
        gain,
        w_bb,
    ) = args
    rows, half = single.shape[0], pair.shape[2]
    heads = w_pb.shape[1]
    ch = w_q.shape[1] // heads
    pq = w_qp.shape[1] // (3 * heads)
    nv = w_kvp.shape[1] // (3 * heads) - pq
    order, anchors, children = gather_plan(n, 6 if n >= 16 else 2, 0.9, 0.72, 0.4)
    deltas = sorted({d for kids in children.values() for _, d in kids})
    deltas = sorted(set(deltas) | {-d for d in deltas})
    deltas = [d for i, d in enumerate(deltas) if d % n not in {e % n for e in deltas[:i]}]
    chunk = min(8, n)
    cfg = (n, nx, heads, ch, pq, nv, half, chunk, order, anchors, children, deltas)
    hots, masks = constants(heads, ch, pq, nv)
    hots = [jnp.asarray(h, BF16) for h in hots]
    masks = jnp.asarray(masks, F32)
    vmem = pl.BlockSpec(memory_space=pltpu.VMEM)
    hbm = pl.BlockSpec(memory_space=pl.ANY)
    loads = [
        frames,
        chain.reshape(1, rows),
        mask.reshape(1, rows),
        single,
        w_kv.T,
        w_kvp.T,
        hots[2],
        hots[1],
        hots[0],
        w_q.T,
        w_qp.T,
        w_pb.T,
        head_w.reshape(1, heads),
        chain_b.reshape(1, heads),
        gain.reshape(-1, LANES),
        w_bb.T,
        w_out,
        hots[3],
        hots[4],
        hots[5],
        hots[6],
        masks,
    ]
    cfg += (len(loads),)
    specs = [hbm] + [hbm] * len(loads)
    marks = 3 * pq + 2
    span = chunk * half
    width = w_out.shape[2]
    scratch = [pltpu.VMEM(a.shape, a.dtype) for a in loads] + [
        pltpu.SemaphoreType.DMA((len(loads),)),
        pltpu.VMEM((rows, n, half, LANES), BF16),
        pltpu.VMEM((n, 2, half, LANES), F32),
        pltpu.VMEM((16, rows), F32),
        pltpu.VMEM((rows, 16), F32),
        pltpu.VMEM((rows, SUB, n * half), F32),
        pltpu.VMEM((rows, marks, SUB, LANES), F32),
        pltpu.VMEM((rows * SUB, LANES), F32),
        pltpu.VMEM((LANES // SUB, SUB, span), F32),
        pltpu.VMEM((rows, SUB, span), F32),
        pltpu.VMEM((rows, SUB, span), F32),
        pltpu.VMEM((rows, SUB, LANES), F32),
        pltpu.VMEM((rows, 2, SUB, LANES), F32),
        pltpu.VMEM((half, 2, SUB, LANES), F32),
        pltpu.VMEM((nx, half, width), F32),
        pltpu.VMEM((2 * n, 2, LANES), F32),
        pltpu.VMEM((2, half, width), F32),
        pltpu.VMEM((2 * LANES, width), BF16),
        pltpu.VMEM((12, half, LANES), F32),
        pltpu.VMEM((4, SUB, LANES), F32),
        pltpu.SemaphoreType.DMA,
        pltpu.SemaphoreType.DMA,
        pltpu.SemaphoreType.DMA((len(anchors) + -(-n // chunk),)),
        pltpu.SemaphoreType.DMA((2,)),
        pltpu.SemaphoreType.DMA((2,)),
        pltpu.SemaphoreType.DMA((2,)),
        pltpu.SemaphoreType.DMA((2,)),
    ]
    return pl.pallas_call(
        functools.partial(kernel, cfg),
        out_shape=(
            jax.ShapeDtypeStruct(single.shape, BF16),
            jax.ShapeDtypeStruct((12, n * rows), F32),
        ),
        in_specs=specs,
        out_specs=(vmem, vmem),
        scratch_shapes=scratch,
        compiler_params=pltpu.CompilerParams(collective_id=0, has_side_effects=True),
        name="layer",
    )(pair, *loads)


def solution(mesh):
    placed = (
        P(("groups", "blk"), None),
        P(("groups", "blk"), None, "pair", None),
        P(None, ("groups", "blk")),
        P(("groups", "blk")),
        P(("groups", "blk")),
        P(None, "head"),
        P(None, "head"),
        P(None, "head"),
        P(None, "head"),
        P(None, "head"),
        P("head"),
        P("head"),
        P("head", None, None),
        P(),
        P(),
    )
    return jax.shard_map(
        functools.partial(body, mesh.shape["blk"], mesh.shape["head"]),
        mesh=mesh,
        in_specs=placed,
        out_specs=(P(("groups", "blk"), None), P(None, "groups")),
        check_vma=False,
    )
```

```python
import functools
import math

import jax
import jax.numpy as jnp
import numpy as np
from jax import lax
from jax.experimental import pallas as pl
from jax.experimental.pallas import tpu as pltpu
from jax.sharding import PartitionSpec as P

MESH = pl.DeviceIdType.MESH
HIGH = lax.Precision.HIGHEST
F32 = jnp.float32
BF16 = jnp.bfloat16
LW = math.sqrt(1.0 / 3.0)
MASK_PENALTY = 100000.0
KEY_PATH = 9
PIECES = 7
QUARTER = 4
THIRD = 32
LANES = 128
SUB = 8
NT = (((1,), (1,)), ((), ()))

CHAIN_LANE = 7
MASK_LANE = 15
ONE_LANE = 120
TOP_LANE = 121


def gather_plan(n, stride, chunk, fixed, hop, weight):
    low, high = -((n - 1) // 2), n // 2
    when, parent = {0: 0.0}, {}
    anchors = [0]
    for sign in (1, -1):
        for k in range(1, n):
            o = sign * k * stride
            if not (low <= o <= high) or abs(o) > n // 2 - 2:
                break
            anchors.append(o)
            parent[o] = (o - sign * stride, sign * stride)
            when[o] = when[o - sign * stride] + fixed + hop * stride
    for o in range(low, high + 1):
        if o in when:
            continue
        best = min(
            anchors,
            key=lambda a: (when[a] + fixed + (hop + weight) * abs(o - a), abs(a)),
        )
        parent[o] = (best, o - best)
        when[o] = when[best] + fixed + hop * abs(o - best)
    order = sorted(when, key=lambda o: (when[o], abs(o), o))
    order = [
        o
        for c in range(0, n, chunk)
        for o in sorted(order[c : c + chunk], key=lambda o: (o not in anchors, when[o]))
    ]
    anchors = sorted(anchors, key=lambda o: (when[o], -o))
    children = {}
    for o, (p, delta) in parent.items():
        children.setdefault(p, []).append((o, delta))
    for p in children:
        children[p].sort(key=lambda c: (c[0] not in anchors, -abs(c[1])))
    return order, anchors, children


def constants(heads, ch, pq, pv):
    key_lane = lambda h, c: ((h * ch + c) // 4) * 8 + 3 + (h * ch + c) % 4
    kp_lane = lambda h, p, a: (p * 3 + a) * 8 + h
    v_lane = lambda h, c: h * ch + c
    vp_lane = lambda h, p, a: heads * ch + a * heads * pv + h * pv + p
    kv = np.zeros((heads * 2 * ch, 2 * LANES), np.float32)
    kp = np.zeros((heads * (pq + pv) * 3, 6 * LANES), np.float32)
    fr = np.zeros((16, 8 * LANES), np.float32)
    q = np.zeros((heads * ch, LANES), np.float32)
    qp = np.zeros((heads * pq * 3, 3 * LANES), np.float32)
    pa = np.zeros((LANES, LANES), np.float32)
    masks = np.zeros((3, SUB, LANES), np.float32)
    perm = np.zeros((2 * LANES, heads * (ch + 4 * pv)), np.float32)
    small = ch + 4 * pv
    for h in range(heads):
        for c in range(ch):
            kv[h * 2 * ch + c, key_lane(h, c)] = 1
            kv[h * 2 * ch + ch + c, LANES + v_lane(h, c)] = 1
            q[h * ch + c, key_lane(h, c)] = 1
            masks[0, h, key_lane(h, c)] = 1
            masks[2, h, v_lane(h, c)] = 1
            perm[v_lane(h, c), h * small + c] = 1
        for p in range(pq):
            for a in range(3):
                lane = kp_lane(h, p, a)
                masks[1, h, lane] = 1
                pa[lane, p * 3 + a] = 1
                for b in range(3):
                    kp[(h * (pq + pv) + p) * 3 + b, 2 * b * LANES + lane] = 1
                    qp[(h * pq + p) * 3 + b, b * LANES + lane] = 1
                    fr[3 * a + b, 2 * b * LANES + lane] = 1
                fr[9 + a, 6 * LANES + lane] = 1
        for p in range(pv):
            for a in range(3):
                lane = vp_lane(h, p, a)
                masks[2, h, lane] = 1
                perm[lane, h * small + ch + p * 3 + a] = 1
                line = 0 if lane >= 3 * THIRD else 1
                for b in range(3):
                    kp[(h * (pq + pv) + pq + p) * 3 + b, (2 * b + line) * LANES + lane] = 1
                    fr[3 * a + b, (2 * b + line) * LANES + lane] = 1
                fr[9 + a, (6 + line) * LANES + lane] = 1
            perm[LANES + vp_lane(h, p, 0), h * small + ch + 3 * pv + p] = 1
    masks[1, :heads, CHAIN_LANE] = 1
    masks[1, :heads, MASK_LANE] = 1
    pa[CHAIN_LANE, 12] = 1
    pa[MASK_LANE, 13] = 1
    fr[12, 6 * LANES + CHAIN_LANE] = 1
    fr[13, 6 * LANES + MASK_LANE] = 1
    return (kv, kp, fr, q, qp, pa, perm), masks.reshape(3 * SUB, LANES)


def pieces3(x):
    a = x.astype(BF16)
    r = x - a.astype(F32)
    b = r.astype(BF16)
    c = (r - b.astype(F32)).astype(BF16)
    return a, b, c


def select(x, onehot):
    m = x.shape[0]
    y = jnp.dot(jnp.concatenate(pieces3(x), axis=0), onehot, preferred_element_type=F32)
    return y[:m] + y[m : 2 * m] + y[2 * m :]


def roll(x, shift, axis):
    shift %= x.shape[axis]
    return x if shift == 0 else pltpu.roll(x, shift, axis)


def kernel(
    cfg,
    pair,
    *refs,
):
    n_loads = cfg[-1]
    sources, (out_single, out_frames) = refs[:n_loads], refs[n_loads : n_loads + 2]
    held = refs[n_loads + 2 : 2 * n_loads + 2]
    run(cfg[:-1], pair, sources, held, out_single, out_frames, *refs[2 * n_loads + 2 :])


def run(
    cfg,
    pair,
    sources,
    held,
    out_single,
    out_frames,
    load_sem,
    pv,
    buf,
    rbuf,
    stack,
    ft,
    bias,
    qpb,
    qblk,
    kt,
    dots,
    wts,
    alpha,
    acc,
    mbuf,
    xbuf,
    fbuf,
    sbuf,
    wp,
    rb,
    rsel,
    pair_sem,
    send_sem,
    recv_sem,
    m_sem,
    x_sem,
    s_sem,
    f_sem,
):
    n, nx, heads, ch, pq, nv, half, chunk, order, anchors, children, deltas = cfg
    rows = 2 * half
    z = lax.axis_index("blk")
    x = lax.axis_index("head")
    p = lax.axis_index("pair")
    other = 1 - p
    slot_of = {o: i for i, o in enumerate(order)}

    group_of = {o: len(anchors) + i // chunk for i, o in enumerate(order)}
    group_of.update({o: i for i, o in enumerate(anchors)})
    hub_slot = {o: i for i, o in enumerate(anchors)}

    def block(o):
        return lax.rem(z - o + 2 * n, n)

    lane16 = lax.broadcasted_iota(jnp.int32, (half, LANES), 1)

    loads = [
        pltpu.make_async_copy(source, place, load_sem.at[k])
        for k, (source, place) in enumerate(zip(sources, held))
    ]
    for copy in loads[:KEY_PATH]:
        copy.start()

    barrier = pltpu.get_barrier_semaphore()
    signals = 0
    for d in deltas:
        for core in (p, other):
            pl.semaphore_signal(
                barrier,
                inc=1,
                device_id={"blk": lax.rem(z + d + n, n), "pair": core},
                device_id_type=MESH,
            )
            signals += 1
    for d in range(1, nx):
        pl.semaphore_signal(
            barrier, inc=1, device_id={"head": lax.rem(x + d, nx)}, device_id_type=MESH
        )
        signals += 1
    pl.semaphore_signal(barrier, inc=1, device_id={"pair": other}, device_id_type=MESH)
    signals += 1

    for copy in loads[KEY_PATH:]:
        copy.start()
    (frames, chain, mask, single, w_kv, w_kvp, c_fr, c_kp, c_kv) = held[:KEY_PATH]
    (w_q, w_qp, w_pb, head_w, chain_b, gain, w_bb, w_out, c_q, c_qp, c_pa, c_perm, c_masks) = held[
        KEY_PATH:
    ]

    for copy in loads[:KEY_PATH]:
        copy.wait()
    for o in order:
        pltpu.make_async_copy(pair.at[:, block(o)], pv.at[:, slot_of[o]], pair_sem).start()

    stack[...] = jnp.zeros_like(stack)
    stack[0:12, :] = frames[...]
    stack[12:13, :] = chain[...].astype(F32)
    stack[13:14, :] = mask[...].astype(F32)
    eye = (
        lax.broadcasted_iota(jnp.int32, (rows, rows), 0)
        == lax.broadcasted_iota(jnp.int32, (rows, rows), 1)
    ).astype(F32)
    ft[...] = lax.dot_general(eye, stack[...], NT, precision=HIGH, preferred_element_type=F32)
    mine = pl.ds(pl.multiple_of(p * half, half), half)
    theirs = pl.ds(pl.multiple_of(other * half, half), half)
    ks = single[mine, :]
    key_value = lax.dot_general(ks, w_kv[...], NT, preferred_element_type=F32)
    key_local = lax.dot_general(ks, w_kvp[...], NT, preferred_element_type=F32)
    turn = select(ft[mine, :], c_fr[...])
    local = select(key_local, c_kp[...])
    width = 2 * LANES
    line = select(key_value, c_kv[...]) + turn[:, 3 * width :]
    for b in range(3):
        line += turn[:, b * width : (b + 1) * width] * local[:, b * width : (b + 1) * width]
    near_line = line[:, :LANES]
    for k in range(4):
        buf[k] = near_line[QUARTER * k : QUARTER * (k + 1)]
    far_line = line[:, LANES:]
    last_rows = far_line[3 * QUARTER :]
    lane4 = lax.broadcasted_iota(jnp.int32, (QUARTER, LANES), 1)
    for k in range(3):
        moved_rows = roll(last_rows, 3 * THIRD - k * THIRD, 1)
        buf[4 + k] = jnp.where(
            lane4 < 3 * THIRD, far_line[QUARTER * k : QUARTER * (k + 1)], moved_rows
        )

    def send(src, place, group, delta, core, sem):
        pltpu.make_async_remote_copy(
            src_ref=src,
            dst_ref=place,
            send_sem=send_sem.at[sem],
            recv_sem=recv_sem.at[group],
            device_id={"blk": lax.rem(z + delta + n, n), "pair": core},
            device_id_type=MESH,
        ).start()

    def held_block(ref, first, last=None):
        last = first + 1 if last is None else last
        return ref.at[first * PIECES : last * PIECES]

    def relay(o):
        for child, delta in children.get(o, []):
            send(held_block(buf, slot_of[o]), held_block(buf, slot_of[child]), group_of[child], delta, p, 0)

    hub_group = {o: len(anchors) + n // chunk + i for i, o in enumerate(anchors)}

    def hub_relay(o):
        src = held_block(rbuf, hub_slot[o])
        for child, delta in children.get(o, []):
            if child in anchors:
                send(src, held_block(rbuf, hub_slot[child]), hub_group[child], delta, 1, 1)
            else:
                send(src, held_block(buf, slot_of[child]), group_of[child], delta, 0, 1)
        send(src, held_block(buf, slot_of[o]), group_of[o], 0, 0, 1)

    def first_sends():
        for child, delta in children[0]:
            if child in anchors:
                send(held_block(buf, 0), held_block(rbuf, hub_slot[child]), hub_group[child], delta, 1, 0)
            else:
                send(held_block(buf, 0), held_block(buf, slot_of[child]), group_of[child], delta, 0, 0)

    def take(ref, first, last, group):
        pltpu.make_async_remote_copy(
            src_ref=held_block(ref, first, last),
            dst_ref=held_block(ref, first, last),
            send_sem=send_sem.at[0],
            recv_sem=recv_sem.at[group],
            device_id={"blk": lax.rem(z + 1, n)},
            device_id_type=MESH,
        ).wait_recv()

    pl.semaphore_wait(barrier, signals)

    @pl.when(p == 1)
    def _():
        relay(0)

    @pl.when(p == 0)
    def _():
        first_sends()


    for copy in loads[KEY_PATH:]:
        copy.wait()
    full = ft[...]
    query = lax.dot_general(single[...], w_q[...], NT, preferred_element_type=F32)
    query = select(query, c_q[...]) * (LW / math.sqrt(ch))
    q_local = select(
        lax.dot_general(single[...], w_qp[...], NT, preferred_element_type=F32), c_qp[...]
    )
    q_turn = select(full, c_fr[...])
    q_line = q_turn[:, 3 * width : 3 * width + LANES]
    for b in range(3):
        q_line += (
            q_turn[:, b * width : b * width + LANES] * q_local[:, b * LANES : (b + 1) * LANES]
        )
    head_keys = c_masks[0:SUB, :]
    head_points = c_masks[SUB : 2 * SUB, :]
    head_values = c_masks[2 * SUB : 3 * SUB, :]
    wide_query = (query[:, None, :] * head_keys[None]).reshape(rows * SUB, LANES)
    coarse = wide_query.astype(BF16)
    qblk[0] = coarse
    qblk[1] = (wide_query - coarse.astype(F32)).astype(BF16)
    spread = select((q_line[:, None, :] * head_points[None]).reshape(rows * SUB, LANES), c_pa[...])
    spread = spread.reshape(rows, SUB, LANES)
    marks = 3 * pq + 2
    for k in range(marks):
        qpb[:, k] = jnp.broadcast_to(spread[:, :, k : k + 1], (rows, SUB, LANES))

    diagonal = lax.broadcasted_iota(jnp.int32, (SUB, heads), 0) == lax.broadcasted_iota(
        jnp.int32, (SUB, heads), 1
    )

    def down(row):
        column = jnp.sum(jnp.where(diagonal, row, 0.0), axis=1, keepdims=True)
        return jnp.broadcast_to(column, (SUB, LANES))

    raw = down(head_w[...])
    cross = down(chain_b[...]) * LW
    soft = jnp.maximum(raw, 0.0) + jnp.log1p(jnp.exp(-jnp.abs(raw)))
    near = soft * (LW * math.sqrt(2.0 / (9.0 * pq)) / 2.0)

    w_bias = jnp.dot(diagonal.astype(BF16), w_pb[...], preferred_element_type=F32).astype(BF16)

    pltpu.make_async_copy(pair, pv, pair_sem).wait()

    keys = n * half

    def bias_of(i, _):
        bias[i] = LW * lax.dot_general(
            w_bias, pv[i].reshape(keys, LANES), NT, preferred_element_type=F32
        )
        return 0

    lax.fori_loop(0, rows, bias_of, 0, unroll=8)

    short = w_out.shape[1] - LANES
    w_short = w_out[:, 0:short, :].reshape(heads * short, w_out.shape[2])
    wp[...] = jnp.dot(c_perm[...], w_short, preferred_element_type=F32).astype(BF16)
    mine_ft = ft[mine, :]
    for k in range(12):
        rb[k] = jnp.broadcast_to(mine_ft[:, k : k + 1], (half, LANES))
    lane = lax.broadcasted_iota(jnp.int32, (rows, LANES), 1)
    repeat = ((lane & (half - 1)) + p * half == lax.broadcasted_iota(jnp.int32, (rows, LANES), 0)).astype(BF16)
    wide = select(stack[...], repeat)
    lane8 = lax.broadcasted_iota(jnp.int32, (SUB, LANES), 1)
    part8 = lax.div(lane8, half)
    comp8 = lax.broadcasted_iota(jnp.int32, (SUB, LANES), 0) * (LANES // half) + part8
    for b in range(4):
        picked = jnp.zeros((SUB, LANES), F32)
        for k in range(12):
            source = (k - k % 3 + b if k < 9 else 3 * (k - 9) + b) if b < 3 else k
            if b == 3 and k < 9:
                continue
            picked = jnp.where(comp8 == k, wide[source : source + 1, :], picked)
        rsel[b] = picked
    eye_b = (
        lax.broadcasted_iota(jnp.int32, (SUB, w_bb.shape[0]), 0)
        == lax.broadcasted_iota(jnp.int32, (SUB, w_bb.shape[0]), 1)
    ).astype(BF16)
    w_motion = jnp.dot(eye_b, w_bb[...], preferred_element_type=F32).astype(BF16)

    def unpacked(slot):
        piece = [buf[slot * PIECES + k] for k in range(PIECES)]
        near_line = jnp.concatenate(piece[:4], axis=0)
        tail = jnp.zeros((QUARTER, LANES), F32)
        lane4 = lax.broadcasted_iota(jnp.int32, (QUARTER, LANES), 1)
        for k in range(3):
            tail = jnp.where(
                (lane4 >= k * THIRD) & (lane4 < (k + 1) * THIRD), roll(piece[4 + k], k * THIRD - 3 * THIRD, 1), tail
            )
        far_line = jnp.concatenate(piece[4:] + [tail], axis=0)
        far_line = jnp.where(lane16 < 3 * THIRD, far_line, near_line)
        return near_line, jnp.where(lane16 == ONE_LANE, 1.0, far_line)

    span = chunk * half
    acc[...] = jnp.zeros_like(acc)
    alpha[...] = jnp.full(alpha.shape, -1e30, F32)
    def pass_on(these):
        @pl.when(p == 1)
        def _():
            for reach in sorted({abs(o) for o in these}):
                level = [o for o in these if abs(o) == reach]
                for o in level:
                    take(buf, slot_of[o], slot_of[o] + 1, group_of[o])
                    relay(o)
                for o in level:
                    take(rbuf, hub_slot[o], hub_slot[o] + 1, hub_group[o])
                    hub_relay(o)

        @pl.when(p == 0)
        def _():
            for o in these:
                take(buf, slot_of[o], slot_of[o] + 1, group_of[o])

    late = [o for o in anchors if o not in order[:chunk] and abs(o) == max(abs(a) for a in anchors)]
    pass_on([o for o in anchors if o != 0 and o not in late])
    for c in range(n // chunk):
        if c == min(2, n // chunk - 1):
            pass_on(late)
        slots = slice(c * chunk, (c + 1) * chunk)
        first = c * chunk + sum(o in anchors for o in order[slots])
        last = (c + 1) * chunk
        if first < last:
            take(buf, first, last, len(anchors) + c)
        lines = [unpacked(slot) for slot in range(c * chunk, (c + 1) * chunk)]
        kc = jnp.concatenate([a for a, _ in lines], axis=0)
        vc = jnp.concatenate([b for _, b in lines], axis=0)
        kt[...] = kc.T.reshape(LANES // SUB, SUB, span)
        k_coarse = kc.astype(BF16)
        k_fine = (kc - k_coarse.astype(F32)).astype(BF16)
        products = [
            lax.dot_general(a, b, NT, preferred_element_type=F32)
            for a, b in ((qblk[0], k_coarse), (qblk[0], k_fine), (qblk[1], k_coarse))
        ]
        dots[...] = (products[0] + products[1] + products[2]).reshape(rows, SUB, span)
        chain_j = kt[0, 7:8, :]
        mask_j = kt[1, 7:8, :]

        def one_row(i, _):
            far = jnp.zeros((SUB, span), F32)
            for k in range(3 * pq):
                gap = qpb[i, k][:, :span] - kt[k]
                far += gap * gap
            differ = jnp.where(qpb[i, 3 * pq][:, :span] != chain_j, cross[:, :span], 0.0)
            absent = 1.0 - qpb[i, 3 * pq + 1][:, :span] * mask_j
            logits = (
                dots[i]
                + bias[i, :, c * span : (c + 1) * span]
                - near[:, :span] * far
                + differ
                - MASK_PENALTY * absent
            )
            old = alpha[i]
            top = jnp.maximum(old, jnp.max(logits, axis=1, keepdims=True))
            w = jnp.exp(logits - top[:, :span])
            wts[i] = w
            alpha[i] = top
            scale = jnp.exp(old - top)
            acc[i, 1] = acc[i, 1] * scale
            acc[i, 0] = acc[i, 0] * scale + jnp.dot(
                w.astype(BF16),
                pv[i, slots].reshape(span, LANES),
                preferred_element_type=F32,
            )
            return 0

        lax.fori_loop(0, rows, one_row, 0, unroll=rows)
        acc[:, 1] += jnp.dot(
            wts[...].reshape(rows * SUB, span), vc, precision=HIGH, preferred_element_type=F32
        ).reshape(rows, SUB, LANES)

    lane3 = lax.broadcasted_iota(jnp.int32, (rows, SUB, LANES), 2)
    acc[:, 1] = jnp.where(lane3 == TOP_LANE, alpha[...], acc[:, 1])
    give = pltpu.make_async_remote_copy(
        src_ref=acc.at[theirs],
        dst_ref=mbuf,
        send_sem=m_sem.at[0],
        recv_sem=m_sem.at[1],
        device_id={"pair": other},
        device_id_type=MESH,
    )
    give.start()
    give.wait_recv()
    own_p, own_b = acc[mine, 0], acc[mine, 1]
    far_p, far_b = mbuf[:, 0], mbuf[:, 1]
    own_top, far_top = own_b[:, :, TOP_LANE : TOP_LANE + 1], far_b[:, :, TOP_LANE : TOP_LANE + 1]
    top = jnp.maximum(own_top, far_top)
    own_scale, far_scale = jnp.exp(own_top - top), jnp.exp(far_top - top)
    both_b = own_b * own_scale + far_b * far_scale
    total = both_b[:, :, ONE_LANE : ONE_LANE + 1]
    both_b = both_b / total * head_values[None]
    paired = (own_p * own_scale + far_p * far_scale) / total
    mbuf[:, 0] = paired
    sums = jnp.sum(both_b, axis=1)
    first = heads * ch
    third = heads * nv
    moved = [roll(sums, -a * third, 1) - rb[9 + a] for a in range(3)]
    pointed = [sum(rb[3 * a + b] * moved[a] for a in range(3)) for b in range(3)]
    norms = jnp.sqrt(pointed[0] * pointed[0] + pointed[1] * pointed[1] + pointed[2] * pointed[2] + 1.0)
    joined = sums
    for b in range(3):
        joined = jnp.where(
            (lane16 >= first + b * third) & (lane16 < first + (b + 1) * third),
            roll(pointed[b], b * third, 1),
            joined,
        )
    norms = jnp.where((lane16 >= first) & (lane16 < first + third), norms, 0.0)
    features = jnp.concatenate([joined, norms], axis=1).astype(BF16)
    update = jnp.dot(features, wp[...], preferred_element_type=F32)
    for h in range(heads):
        update += jnp.dot(
            mbuf[:, 0, h, :].astype(BF16), w_out[h, short:, :], preferred_element_type=F32
        )

    xbuf[x] = update
    for d in range(1, nx):
        pltpu.make_async_remote_copy(
            src_ref=xbuf.at[x],
            dst_ref=xbuf.at[x],
            send_sem=x_sem.at[0],
            recv_sem=x_sem.at[1],
            device_id={"head": lax.rem(x + d, nx)},
            device_id_type=MESH,
        ).start()
    x_all = pltpu.make_async_remote_copy(
        src_ref=xbuf.at[0 : nx - 1],
        dst_ref=xbuf.at[0 : nx - 1],
        send_sem=x_sem.at[0],
        recv_sem=x_sem.at[1],
        device_id={"head": lax.rem(x + 1, nx)},
        device_id_type=MESH,
    )
    if nx > 1:
        x_all.wait_recv()
    update = xbuf[0]
    for k in range(1, nx):
        update = update + xbuf[k]
    mixed = single[mine, :].astype(F32) + update
    count = mixed.shape[1]
    gains = jnp.concatenate([gain[k : k + 1, :] for k in range(count // LANES)], axis=1)
    centre = jnp.sum(mixed, axis=1, keepdims=True) * (1.0 / count)
    apart = mixed - centre
    variance = jnp.sum(apart * apart, axis=1, keepdims=True) * (1.0 / count)
    result = (apart * lax.rsqrt(variance + 1e-05) * gains).astype(BF16)
    out_single[mine, :] = result
    sbuf[0] = result.astype(F32)
    give_s = pltpu.make_async_remote_copy(
        src_ref=sbuf.at[0],
        dst_ref=sbuf.at[1],
        send_sem=s_sem.at[0],
        recv_sem=s_sem.at[1],
        device_id={"pair": other},
        device_id_type=MESH,
    )

    groups = LANES // half
    motion = lax.dot_general(
        w_motion,
        jnp.concatenate([result] * groups, axis=0),
        NT,
        preferred_element_type=F32,
    )
    m = [jnp.broadcast_to(motion[k : k + 1, :], (SUB, LANES)) for k in range(6)]
    qa = 1.0 / jnp.sqrt(1.0 + m[0] * m[0] + m[1] * m[1] + m[2] * m[2])
    qb, qc, qd = m[0] * qa, m[1] * qa, m[2] * qa
    aa, bb, cc, dd = qa * qa, qb * qb, qc * qc, qd * qd
    ab, ac, ad = qa * qb, qa * qc, qa * qd
    bc, bd, cd = qb * qc, qb * qd, qc * qd
    spin = [
        [aa + bb - cc - dd, 2.0 * (bc - ad), 2.0 * (bd + ac)],
        [2.0 * (bc + ad), aa - bb + cc - dd, 2.0 * (cd - ab)],
        [2.0 * (bd - ac), 2.0 * (cd + ab), aa - bb - cc + dd],
    ]
    column = lax.rem(comp8, 3)
    packed = rsel[3]
    for b in range(3):
        value = jnp.where(column == 0, spin[b][0], jnp.where(column == 1, spin[b][1], spin[b][2]))
        value = jnp.where(comp8 < 9, value, m[3 + b])
        packed = packed + rsel[b] * value
    lines = fbuf.shape[1]
    me = z * 2 + p
    fbuf[me] = packed[0:lines, :]

    steps = sorted(
        ((d, c) for d in range(n) for c in (0, 1) if (d, c) != (0, 0)),
        key=lambda s: (-min(s[0], n - s[0]), s[1]),
    )
    for d, c in steps:
        device = {"blk": lax.rem(z + d, n), "pair": p if c == 0 else other}
        pltpu.make_async_remote_copy(
            src_ref=fbuf.at[me],
            dst_ref=fbuf.at[me],
            send_sem=f_sem.at[0],
            recv_sem=f_sem.at[1],
            device_id=device,
            device_id_type=MESH,
        ).start()
    give_s.start()
    give_s.wait_recv()
    out_single[theirs, :] = sbuf[1].astype(BF16)
    f_all = pltpu.make_async_remote_copy(
        src_ref=fbuf.at[0 : 2 * n - 1],
        dst_ref=fbuf.at[0 : 2 * n - 1],
        send_sem=f_sem.at[0],
        recv_sem=f_sem.at[1],
        device_id={"pair": other},
        device_id_type=MESH,
    )
    f_all.wait_recv()

    gap = (lax.broadcasted_iota(jnp.int32, (SUB, LANES), 0) - part8) & (SUB - 1)
    for t in range(2 * n // groups):
        for line_number in range(2):
            tile = fbuf[t * groups : (t + 1) * groups, line_number, :]
            out = tile
            for s in range(1, groups):
                out = jnp.where(gap == s, roll(roll(tile, s, 0), -half * s, 1), out)
            height = 8 if line_number == 0 else 4
            out_frames[8 * line_number : 8 * line_number + height, t * LANES : (t + 1) * LANES] = out[:height]

    def sent(count, sem):
        pltpu.make_async_remote_copy(
            src_ref=held_block(buf, 0, count),
            dst_ref=held_block(buf, 0, count),
            send_sem=send_sem.at[sem],
            recv_sem=recv_sem.at[0],
            device_id={"blk": lax.rem(z + 1, n)},
            device_id_type=MESH,
        ).wait_send()

    @pl.when(p == 1)
    def _():
        sent(n - 1, 0)
        sent(n - 1 - len(children[0]) + len(anchors) - 1, 1)

    @pl.when(p == 0)
    def _():
        sent(len(children[0]), 0)

    if nx > 1:
        x_all.wait_send()
    f_all.wait_send()
    give.wait_send()
    give_s.wait_send()


def body(n, nx, *args):
    (
        single,
        pair,
        frames,
        chain,
        mask,
        w_q,
        w_kv,
        w_qp,
        w_kvp,
        w_pb,
        head_w,
        chain_b,
        w_out,
        gain,
        w_bb,
    ) = args
    rows, half = single.shape[0], pair.shape[2]
    heads = w_pb.shape[1]
    ch = w_q.shape[1] // heads
    pq = w_qp.shape[1] // (3 * heads)
    nv = w_kvp.shape[1] // (3 * heads) - pq
    chunk = min(8, n)
    order, anchors, children = gather_plan(n, 4 if n >= 16 else 2, chunk, 0.9, 0.72, 1.0)
    deltas = sorted({d for kids in children.values() for _, d in kids})
    deltas = sorted(set(deltas) | {-d for d in deltas})
    deltas = [d for i, d in enumerate(deltas) if d % n not in {e % n for e in deltas[:i]}]
    cfg = (n, nx, heads, ch, pq, nv, half, chunk, order, anchors, children, deltas)
    hots, masks = constants(heads, ch, pq, nv)
    hots = [jnp.asarray(h, BF16) for h in hots]
    masks = jnp.asarray(masks, F32)
    vmem = pl.BlockSpec(memory_space=pltpu.VMEM)
    hbm = pl.BlockSpec(memory_space=pl.ANY)
    loads = [
        frames,
        chain.reshape(1, rows),
        mask.reshape(1, rows),
        single,
        w_kv.T,
        w_kvp.T,
        hots[2],
        hots[1],
        hots[0],
        w_q.T,
        w_qp.T,
        w_pb.T,
        head_w.reshape(1, heads),
        chain_b.reshape(1, heads),
        gain.reshape(-1, LANES),
        w_bb.T,
        w_out,
        hots[3],
        hots[4],
        hots[5],
        hots[6],
        masks,
    ]
    cfg += (len(loads),)
    specs = [hbm] + [hbm] * len(loads)
    marks = 3 * pq + 2
    span = chunk * half
    width = w_out.shape[2]
    scratch = [pltpu.VMEM(a.shape, a.dtype) for a in loads] + [
        pltpu.SemaphoreType.DMA((len(loads),)),
        pltpu.VMEM((rows, n, half, LANES), BF16),
        pltpu.VMEM((n * PIECES, QUARTER, LANES), F32),
        pltpu.VMEM((len(anchors) * PIECES, QUARTER, LANES), F32),
        pltpu.VMEM((16, rows), F32),
        pltpu.VMEM((rows, 16), F32),
        pltpu.VMEM((rows, SUB, n * half), F32),
        pltpu.VMEM((rows, marks, SUB, LANES), F32),
        pltpu.VMEM((2, rows * SUB, LANES), BF16),
        pltpu.VMEM((LANES // SUB, SUB, span), F32),
        pltpu.VMEM((rows, SUB, span), F32),
        pltpu.VMEM((rows, SUB, span), F32),
        pltpu.VMEM((rows, SUB, LANES), F32),
        pltpu.VMEM((rows, 2, SUB, LANES), F32),
        pltpu.VMEM((half, 2, SUB, LANES), F32),
        pltpu.VMEM((nx, half, width), F32),
        pltpu.VMEM((2 * n, 2, LANES), F32),
        pltpu.VMEM((2, half, width), F32),
        pltpu.VMEM((2 * LANES, width), BF16),
        pltpu.VMEM((12, half, LANES), F32),
        pltpu.VMEM((4, SUB, LANES), F32),
        pltpu.SemaphoreType.DMA,
        pltpu.SemaphoreType.DMA((2,)),
        pltpu.SemaphoreType.DMA((2 * len(anchors) + n // chunk,)),
        pltpu.SemaphoreType.DMA((2,)),
        pltpu.SemaphoreType.DMA((2,)),
        pltpu.SemaphoreType.DMA((2,)),
        pltpu.SemaphoreType.DMA((2,)),
    ]
    return pl.pallas_call(
        functools.partial(kernel, cfg),
        out_shape=(
            jax.ShapeDtypeStruct(single.shape, BF16),
            jax.ShapeDtypeStruct((12, n * rows), F32),
        ),
        in_specs=specs,
        out_specs=(vmem, vmem),
        scratch_shapes=scratch,
        compiler_params=pltpu.CompilerParams(collective_id=0, has_side_effects=True),
        name="layer",
    )(pair, *loads)


def solution(mesh):
    placed = (
        P(("groups", "blk"), None),
        P(("groups", "blk"), None, "pair", None),
        P(None, ("groups", "blk")),
        P(("groups", "blk")),
        P(("groups", "blk")),
        P(None, "head"),
        P(None, "head"),
        P(None, "head"),
        P(None, "head"),
        P(None, "head"),
        P("head"),
        P("head"),
        P("head", None, None),
        P(),
        P(),
    )
    return jax.shard_map(
        functools.partial(body, mesh.shape["blk"], mesh.shape["head"]),
        mesh=mesh,
        in_specs=placed,
        out_specs=(P(("groups", "blk"), None), P(None, "groups")),
        check_vma=False,
    )
```

```python
import functools
import math

import jax
import jax.numpy as jnp
import numpy as np
from jax import lax
from jax.experimental import pallas as pl
from jax.experimental.pallas import tpu as pltpu
from jax.sharding import PartitionSpec as P

MESH = pl.DeviceIdType.MESH
HIGH = lax.Precision.HIGHEST
F32 = jnp.float32
BF16 = jnp.bfloat16
LW = math.sqrt(1.0 / 3.0)
MASK_PENALTY = 100000.0
KEY_PATH = 9
PIECES = 7
QUARTER = 4
THIRD = 32
LANES = 128
SUB = 8
NT = (((1,), (1,)), ((), ()))

CHAIN_LANE = 7
MASK_LANE = 15
ONE_LANE = 120
TOP_LANE = 121


def gather_plan(n, stride, chunk, fixed, hop, weight):
    low, high = -((n - 1) // 2), n // 2
    when, parent = {0: 0.0}, {}
    anchors = [0]
    for sign in (1, -1):
        for k in range(1, n):
            o = sign * k * stride
            if not (low <= o <= high) or abs(o) > n // 2 - 2:
                break
            anchors.append(o)
            parent[o] = (o - sign * stride, sign * stride)
            when[o] = when[o - sign * stride] + fixed + hop * stride
    for o in range(low, high + 1):
        if o in when:
            continue
        best = min(
            anchors,
            key=lambda a: (when[a] + fixed + (hop + weight) * abs(o - a), abs(a)),
        )
        parent[o] = (best, o - best)
        when[o] = when[best] + fixed + hop * abs(o - best)
    order = sorted(when, key=lambda o: (when[o], abs(o), o))
    order = [
        o
        for c in range(0, n, chunk)
        for o in sorted(order[c : c + chunk], key=lambda o: (o not in anchors, when[o]))
    ]
    anchors = sorted(anchors, key=lambda o: (when[o], -o))
    children = {}
    for o, (p, delta) in parent.items():
        children.setdefault(p, []).append((o, delta))
    for p in children:
        children[p].sort(key=lambda c: (c[0] not in anchors, -abs(c[1])))
    return order, anchors, children


def constants(heads, ch, pq, pv):
    key_lane = lambda h, c: ((h * ch + c) // 4) * 8 + 3 + (h * ch + c) % 4
    kp_lane = lambda h, p, a: (p * 3 + a) * 8 + h
    v_lane = lambda h, c: h * ch + c
    vp_lane = lambda h, p, a: heads * ch + a * heads * pv + h * pv + p
    kv = np.zeros((heads * 2 * ch, 2 * LANES), np.float32)
    kp = np.zeros((heads * (pq + pv) * 3, 6 * LANES), np.float32)
    fr = np.zeros((16, 8 * LANES), np.float32)
    q = np.zeros((heads * ch, LANES), np.float32)
    qp = np.zeros((heads * pq * 3, 3 * LANES), np.float32)
    pa = np.zeros((LANES, LANES), np.float32)
    masks = np.zeros((3, SUB, LANES), np.float32)
    perm = np.zeros((2 * LANES, heads * (ch + 4 * pv)), np.float32)
    small = ch + 4 * pv
    for h in range(heads):
        for c in range(ch):
            kv[h * 2 * ch + c, key_lane(h, c)] = 1
            kv[h * 2 * ch + ch + c, LANES + v_lane(h, c)] = 1
            q[h * ch + c, key_lane(h, c)] = 1
            masks[0, h, key_lane(h, c)] = 1
            masks[2, h, v_lane(h, c)] = 1
            perm[v_lane(h, c), h * small + c] = 1
        for p in range(pq):
            for a in range(3):
                lane = kp_lane(h, p, a)
                masks[1, h, lane] = 1
                pa[lane, p * 3 + a] = 1
                for b in range(3):
                    kp[(h * (pq + pv) + p) * 3 + b, 2 * b * LANES + lane] = 1
                    qp[(h * pq + p) * 3 + b, b * LANES + lane] = 1
                    fr[3 * a + b, 2 * b * LANES + lane] = 1
                fr[9 + a, 6 * LANES + lane] = 1
        for p in range(pv):
            for a in range(3):
                lane = vp_lane(h, p, a)
                masks[2, h, lane] = 1
                perm[lane, h * small + ch + p * 3 + a] = 1
                line = 0 if lane >= 3 * THIRD else 1
                for b in range(3):
                    kp[(h * (pq + pv) + pq + p) * 3 + b, (2 * b + line) * LANES + lane] = 1
                    fr[3 * a + b, (2 * b + line) * LANES + lane] = 1
                fr[9 + a, (6 + line) * LANES + lane] = 1
            perm[LANES + vp_lane(h, p, 0), h * small + ch + 3 * pv + p] = 1
    masks[1, :heads, CHAIN_LANE] = 1
    masks[1, :heads, MASK_LANE] = 1
    pa[CHAIN_LANE, 12] = 1
    pa[MASK_LANE, 13] = 1
    fr[12, 6 * LANES + CHAIN_LANE] = 1
    fr[13, 6 * LANES + MASK_LANE] = 1
    return (kv, kp, fr, q, qp, pa, perm), masks.reshape(3 * SUB, LANES)


def pieces3(x):
    a = x.astype(BF16)
    r = x - a.astype(F32)
    b = r.astype(BF16)
    c = (r - b.astype(F32)).astype(BF16)
    return a, b, c


def select(x, onehot):
    m = x.shape[0]
    y = jnp.dot(jnp.concatenate(pieces3(x), axis=0), onehot, preferred_element_type=F32)
    return y[:m] + y[m : 2 * m] + y[2 * m :]


def roll(x, shift, axis):
    shift %= x.shape[axis]
    return x if shift == 0 else pltpu.roll(x, shift, axis)


def kernel(
    cfg,
    pair,
    *refs,
):
    n_loads = cfg[-1]
    sources, (out_single, out_frames) = refs[:n_loads], refs[n_loads : n_loads + 2]
    held = refs[n_loads + 2 : 2 * n_loads + 2]
    run(cfg[:-1], pair, sources, held, out_single, out_frames, *refs[2 * n_loads + 2 :])


def run(
    cfg,
    pair,
    sources,
    held,
    out_single,
    out_frames,
    load_sem,
    pv,
    buf,
    rbuf,
    stack,
    ft,
    bias,
    qpb,
    qblk,
    kt,
    dots,
    wts,
    alpha,
    acc,
    mbuf,
    xbuf,
    fbuf,
    sbuf,
    wp,
    rb,
    rsel,
    pair_sem,
    send_sem,
    recv_sem,
    m_sem,
    x_sem,
    s_sem,
    f_sem,
):
    n, nx, heads, ch, pq, nv, half, chunk, order, anchors, children, deltas = cfg
    rows = 2 * half
    z = lax.axis_index("blk")
    x = lax.axis_index("head")
    p = lax.axis_index("pair")
    other = 1 - p
    slot_of = {o: i for i, o in enumerate(order)}

    group_of = {o: len(anchors) + i // chunk for i, o in enumerate(order)}
    group_of.update({o: i for i, o in enumerate(anchors)})
    hub_slot = {o: i for i, o in enumerate(anchors)}

    def block(o):
        return lax.rem(z - o + 2 * n, n)

    lane16 = lax.broadcasted_iota(jnp.int32, (half, LANES), 1)

    loads = [
        pltpu.make_async_copy(source, place, load_sem.at[k])
        for k, (source, place) in enumerate(zip(sources, held))
    ]
    for copy in loads[:KEY_PATH]:
        copy.start()

    barrier = pltpu.get_barrier_semaphore()
    signals = 0
    for d in deltas:
        for core in (p, other):
            pl.semaphore_signal(
                barrier,
                inc=1,
                device_id={"blk": lax.rem(z + d + n, n), "pair": core},
                device_id_type=MESH,
            )
            signals += 1
    for d in range(1, nx):
        pl.semaphore_signal(
            barrier, inc=1, device_id={"head": lax.rem(x + d, nx)}, device_id_type=MESH
        )
        signals += 1
    pl.semaphore_signal(barrier, inc=1, device_id={"pair": other}, device_id_type=MESH)
    signals += 1

    for copy in loads[KEY_PATH:]:
        copy.start()
    (frames, chain, mask, single, w_kv, w_kvp, c_fr, c_kp, c_kv) = held[:KEY_PATH]
    (w_q, w_qp, w_pb, head_w, chain_b, gain, w_bb, w_out, c_q, c_qp, c_pa, c_perm, c_masks) = held[
        KEY_PATH:
    ]

    for copy in loads[:KEY_PATH]:
        copy.wait()
    for o in order:
        pltpu.make_async_copy(pair.at[:, block(o)], pv.at[:, slot_of[o]], pair_sem).start()

    stack[...] = jnp.zeros_like(stack)
    stack[0:12, :] = frames[...]
    stack[12:13, :] = chain[...].astype(F32)
    stack[13:14, :] = mask[...].astype(F32)
    eye = (
        lax.broadcasted_iota(jnp.int32, (rows, rows), 0)
        == lax.broadcasted_iota(jnp.int32, (rows, rows), 1)
    ).astype(F32)
    ft[...] = lax.dot_general(eye, stack[...], NT, precision=HIGH, preferred_element_type=F32)
    mine = pl.ds(pl.multiple_of(p * half, half), half)
    theirs = pl.ds(pl.multiple_of(other * half, half), half)
    ks = single[mine, :]
    key_value = lax.dot_general(ks, w_kv[...], NT, preferred_element_type=F32)
    key_local = lax.dot_general(ks, w_kvp[...], NT, preferred_element_type=F32)
    turn = select(ft[mine, :], c_fr[...])
    local = select(key_local, c_kp[...])
    width = 2 * LANES
    line = select(key_value, c_kv[...]) + turn[:, 3 * width :]
    for b in range(3):
        line += turn[:, b * width : (b + 1) * width] * local[:, b * width : (b + 1) * width]
    near_line = line[:, :LANES]
    for k in range(4):
        buf[k] = near_line[QUARTER * k : QUARTER * (k + 1)]
    far_line = line[:, LANES:]
    last_rows = far_line[3 * QUARTER :]
    lane4 = lax.broadcasted_iota(jnp.int32, (QUARTER, LANES), 1)
    for k in range(3):
        moved_rows = roll(last_rows, 3 * THIRD - k * THIRD, 1)
        buf[4 + k] = jnp.where(
            lane4 < 3 * THIRD, far_line[QUARTER * k : QUARTER * (k + 1)], moved_rows
        )

    def send(src, place, group, delta, core, sem):
        pltpu.make_async_remote_copy(
            src_ref=src,
            dst_ref=place,
            send_sem=send_sem.at[sem],
            recv_sem=recv_sem.at[group],
            device_id={"blk": lax.rem(z + delta + n, n), "pair": core},
            device_id_type=MESH,
        ).start()

    def held_block(ref, first, last=None):
        last = first + 1 if last is None else last
        return ref.at[first * PIECES : last * PIECES]

    def relay(o):
        for child, delta in children.get(o, []):
            send(held_block(buf, slot_of[o]), held_block(buf, slot_of[child]), group_of[child], delta, p, 0)

    hub_group = {o: len(anchors) + n // chunk + i for i, o in enumerate(anchors)}

    def hub_relay(o):
        src = held_block(rbuf, hub_slot[o])
        for child, delta in children.get(o, []):
            if child in anchors:
                send(src, held_block(rbuf, hub_slot[child]), hub_group[child], delta, 1, 1)
            else:
                send(src, held_block(buf, slot_of[child]), group_of[child], delta, 0, 1)
        send(src, held_block(buf, slot_of[o]), group_of[o], 0, 0, 1)

    def first_sends():
        for child, delta in children[0]:
            if child in anchors:
                send(held_block(buf, 0), held_block(rbuf, hub_slot[child]), hub_group[child], delta, 1, 0)
            else:
                send(held_block(buf, 0), held_block(buf, slot_of[child]), group_of[child], delta, 0, 0)

    def take(ref, first, last, group):
        pltpu.make_async_remote_copy(
            src_ref=held_block(ref, first, last),
            dst_ref=held_block(ref, first, last),
            send_sem=send_sem.at[0],
            recv_sem=recv_sem.at[group],
            device_id={"blk": lax.rem(z + 1, n)},
            device_id_type=MESH,
        ).wait_recv()

    pl.semaphore_wait(barrier, signals)

    @pl.when(p == 1)
    def _():
        relay(0)

    @pl.when(p == 0)
    def _():
        first_sends()


    for copy in loads[KEY_PATH:]:
        copy.wait()
    full = ft[...]
    query = lax.dot_general(single[...], w_q[...], NT, preferred_element_type=F32)
    query = select(query, c_q[...]) * (LW / math.sqrt(ch))
    q_local = select(
        lax.dot_general(single[...], w_qp[...], NT, preferred_element_type=F32), c_qp[...]
    )
    q_turn = select(full, c_fr[...])
    q_line = q_turn[:, 3 * width : 3 * width + LANES]
    for b in range(3):
        q_line += (
            q_turn[:, b * width : b * width + LANES] * q_local[:, b * LANES : (b + 1) * LANES]
        )
    head_keys = c_masks[0:SUB, :]
    head_points = c_masks[SUB : 2 * SUB, :]
    head_values = c_masks[2 * SUB : 3 * SUB, :]
    wide_query = (query[:, None, :] * head_keys[None]).reshape(rows * SUB, LANES)
    coarse = wide_query.astype(BF16)
    qblk[0] = coarse
    qblk[1] = (wide_query - coarse.astype(F32)).astype(BF16)
    spread = select((q_line[:, None, :] * head_points[None]).reshape(rows * SUB, LANES), c_pa[...])
    spread = spread.reshape(rows, SUB, LANES)
    marks = 3 * pq + 2
    for k in range(marks):
        qpb[:, k] = jnp.broadcast_to(spread[:, :, k : k + 1], (rows, SUB, LANES))

    diagonal = lax.broadcasted_iota(jnp.int32, (SUB, heads), 0) == lax.broadcasted_iota(
        jnp.int32, (SUB, heads), 1
    )

    def down(row):
        column = jnp.sum(jnp.where(diagonal, row, 0.0), axis=1, keepdims=True)
        return jnp.broadcast_to(column, (SUB, LANES))

    raw = down(head_w[...])
    cross = down(chain_b[...]) * LW
    soft = jnp.maximum(raw, 0.0) + jnp.log1p(jnp.exp(-jnp.abs(raw)))
    near = soft * (LW * math.sqrt(2.0 / (9.0 * pq)) / 2.0)

    w_bias = jnp.dot(diagonal.astype(BF16), w_pb[...], preferred_element_type=F32).astype(BF16)

    pltpu.make_async_copy(pair, pv, pair_sem).wait()

    keys = n * half

    def bias_of(i, _):
        bias[i] = LW * lax.dot_general(
            w_bias, pv[i].reshape(keys, LANES), NT, preferred_element_type=F32
        )
        return 0

    lax.fori_loop(0, rows, bias_of, 0, unroll=8)

    short = w_out.shape[1] - LANES
    w_short = w_out[:, 0:short, :].reshape(heads * short, w_out.shape[2])
    wp[...] = jnp.dot(c_perm[...], w_short, preferred_element_type=F32).astype(BF16)
    mine_ft = ft[mine, :]
    for k in range(12):
        rb[k] = jnp.broadcast_to(mine_ft[:, k : k + 1], (half, LANES))
    lane = lax.broadcasted_iota(jnp.int32, (rows, LANES), 1)
    repeat = ((lane & (half - 1)) + p * half == lax.broadcasted_iota(jnp.int32, (rows, LANES), 0)).astype(BF16)
    wide = select(stack[...], repeat)
    lane8 = lax.broadcasted_iota(jnp.int32, (SUB, LANES), 1)
    part8 = lax.div(lane8, half)
    comp8 = lax.broadcasted_iota(jnp.int32, (SUB, LANES), 0) * (LANES // half) + part8
    for b in range(4):
        picked = jnp.zeros((SUB, LANES), F32)
        for k in range(12):
            source = (k - k % 3 + b if k < 9 else 3 * (k - 9) + b) if b < 3 else k
            if b == 3 and k < 9:
                continue
            picked = jnp.where(comp8 == k, wide[source : source + 1, :], picked)
        rsel[b] = picked
    eye_b = (
        lax.broadcasted_iota(jnp.int32, (SUB, w_bb.shape[0]), 0)
        == lax.broadcasted_iota(jnp.int32, (SUB, w_bb.shape[0]), 1)
    ).astype(BF16)
    w_motion = jnp.dot(eye_b, w_bb[...], preferred_element_type=F32).astype(BF16)

    def unpacked(slot):
        piece = [buf[slot * PIECES + k] for k in range(PIECES)]
        near_line = jnp.concatenate(piece[:4], axis=0)
        tail = jnp.zeros((QUARTER, LANES), F32)
        lane4 = lax.broadcasted_iota(jnp.int32, (QUARTER, LANES), 1)
        for k in range(3):
            tail = jnp.where(
                (lane4 >= k * THIRD) & (lane4 < (k + 1) * THIRD), roll(piece[4 + k], k * THIRD - 3 * THIRD, 1), tail
            )
        far_line = jnp.concatenate(piece[4:] + [tail], axis=0)
        far_line = jnp.where(lane16 < 3 * THIRD, far_line, near_line)
        return near_line, jnp.where(lane16 == ONE_LANE, 1.0, far_line)

    span = chunk * half
    acc[...] = jnp.zeros_like(acc)
    alpha[...] = jnp.full(alpha.shape, -1e30, F32)
    def pass_on(these):
        @pl.when(p == 1)
        def _():
            for reach in sorted({abs(o) for o in these}):
                level = [o for o in these if abs(o) == reach]
                for o in level:
                    take(buf, slot_of[o], slot_of[o] + 1, group_of[o])
                    relay(o)
                for o in level:
                    take(rbuf, hub_slot[o], hub_slot[o] + 1, hub_group[o])
                    hub_relay(o)

        @pl.when(p == 0)
        def _():
            for o in these:
                take(buf, slot_of[o], slot_of[o] + 1, group_of[o])

    late = [o for o in anchors if o not in order[:chunk] and abs(o) == max(abs(a) for a in anchors)]
    pass_on([o for o in anchors if o != 0 and o not in late])
    for c in range(n // chunk):
        if c == min(2, n // chunk - 1):
            pass_on(late)
        slots = slice(c * chunk, (c + 1) * chunk)
        first = c * chunk + sum(o in anchors for o in order[slots])
        last = (c + 1) * chunk
        if first < last:
            take(buf, first, last, len(anchors) + c)
        lines = [unpacked(slot) for slot in range(c * chunk, (c + 1) * chunk)]
        kc = jnp.concatenate([a for a, _ in lines], axis=0)
        vc = jnp.concatenate([b for _, b in lines], axis=0)
        kt[...] = kc.T.reshape(LANES // SUB, SUB, span)
        k_coarse = kc.astype(BF16)
        k_fine = (kc - k_coarse.astype(F32)).astype(BF16)
        products = [
            lax.dot_general(a, b, NT, preferred_element_type=F32)
            for a, b in ((qblk[0], k_coarse), (qblk[0], k_fine), (qblk[1], k_coarse))
        ]
        dots[...] = (products[0] + products[1] + products[2]).reshape(rows, SUB, span)
        chain_j = kt[0, 7:8, :]
        mask_j = kt[1, 7:8, :]

        def one_row(i, _):
            far = jnp.zeros((SUB, span), F32)
            for k in range(3 * pq):
                gap = qpb[i, k][:, :span] - kt[k]
                far += gap * gap
            differ = jnp.where(qpb[i, 3 * pq][:, :span] != chain_j, cross[:, :span], 0.0)
            absent = 1.0 - qpb[i, 3 * pq + 1][:, :span] * mask_j
            logits = (
                dots[i]
                + bias[i, :, c * span : (c + 1) * span]
                - near[:, :span] * far
                + differ
                - MASK_PENALTY * absent
            )
            old = alpha[i]
            top = jnp.maximum(old, jnp.max(logits, axis=1, keepdims=True))
            w = jnp.exp(logits - top[:, :span])
            wts[i] = w
            alpha[i] = top
            scale = jnp.exp(old - top)
            acc[i, 1] = acc[i, 1] * scale
            acc[i, 0] = acc[i, 0] * scale + jnp.dot(
                w.astype(BF16),
                pv[i, slots].reshape(span, LANES),
                preferred_element_type=F32,
            )
            return 0

        lax.fori_loop(0, rows, one_row, 0, unroll=rows)
        acc[:, 1] += jnp.dot(
            wts[...].reshape(rows * SUB, span), vc, precision=HIGH, preferred_element_type=F32
        ).reshape(rows, SUB, LANES)

    lane3 = lax.broadcasted_iota(jnp.int32, (rows, SUB, LANES), 2)
    acc[:, 1] = jnp.where(lane3 == TOP_LANE, alpha[...], acc[:, 1])
    give = pltpu.make_async_remote_copy(
        src_ref=acc.at[theirs],
        dst_ref=mbuf,
        send_sem=m_sem.at[0],
        recv_sem=m_sem.at[1],
        device_id={"pair": other},
        device_id_type=MESH,
    )
    give.start()
    give.wait_recv()
    own_p, own_b = acc[mine, 0], acc[mine, 1]
    far_p, far_b = mbuf[:, 0], mbuf[:, 1]
    own_top, far_top = own_b[:, :, TOP_LANE : TOP_LANE + 1], far_b[:, :, TOP_LANE : TOP_LANE + 1]
    top = jnp.maximum(own_top, far_top)
    own_scale, far_scale = jnp.exp(own_top - top), jnp.exp(far_top - top)
    both_b = own_b * own_scale + far_b * far_scale
    total = both_b[:, :, ONE_LANE : ONE_LANE + 1]
    both_b = both_b / total * head_values[None]
    paired = (own_p * own_scale + far_p * far_scale) / total
    mbuf[:, 0] = paired
    sums = jnp.sum(both_b, axis=1)
    first = heads * ch
    third = heads * nv
    moved = [roll(sums, -a * third, 1) - rb[9 + a] for a in range(3)]
    pointed = [sum(rb[3 * a + b] * moved[a] for a in range(3)) for b in range(3)]
    norms = jnp.sqrt(pointed[0] * pointed[0] + pointed[1] * pointed[1] + pointed[2] * pointed[2] + 1.0)
    joined = sums
    for b in range(3):
        joined = jnp.where(
            (lane16 >= first + b * third) & (lane16 < first + (b + 1) * third),
            roll(pointed[b], b * third, 1),
            joined,
        )
    norms = jnp.where((lane16 >= first) & (lane16 < first + third), norms, 0.0)
    features = jnp.concatenate([joined, norms], axis=1).astype(BF16)
    update = jnp.dot(features, wp[...], preferred_element_type=F32)
    for h in range(heads):
        update += jnp.dot(
            mbuf[:, 0, h, :].astype(BF16), w_out[h, short:, :], preferred_element_type=F32
        )

    xbuf[x] = update
    for d in range(1, nx):
        pltpu.make_async_remote_copy(
            src_ref=xbuf.at[x],
            dst_ref=xbuf.at[x],
            send_sem=x_sem.at[0],
            recv_sem=x_sem.at[1],
            device_id={"head": lax.rem(x + d, nx)},
            device_id_type=MESH,
        ).start()
    x_all = pltpu.make_async_remote_copy(
        src_ref=xbuf.at[0 : nx - 1],
        dst_ref=xbuf.at[0 : nx - 1],
        send_sem=x_sem.at[0],
        recv_sem=x_sem.at[1],
        device_id={"head": lax.rem(x + 1, nx)},
        device_id_type=MESH,
    )
    if nx > 1:
        x_all.wait_recv()
    update = xbuf[0]
    for k in range(1, nx):
        update = update + xbuf[k]
    mixed = single[mine, :].astype(F32) + update
    count = mixed.shape[1]
    gains = jnp.concatenate([gain[k : k + 1, :] for k in range(count // LANES)], axis=1)
    centre = jnp.sum(mixed, axis=1, keepdims=True) * (1.0 / count)
    apart = mixed - centre
    variance = jnp.sum(apart * apart, axis=1, keepdims=True) * (1.0 / count)
    result = (apart * lax.rsqrt(variance + 1e-05) * gains).astype(BF16)
    out_single[mine, :] = result
    sbuf[0] = result.astype(F32)
    give_s = pltpu.make_async_remote_copy(
        src_ref=sbuf.at[0],
        dst_ref=sbuf.at[1],
        send_sem=s_sem.at[0],
        recv_sem=s_sem.at[1],
        device_id={"pair": other},
        device_id_type=MESH,
    )

    groups = LANES // half
    motion = lax.dot_general(
        w_motion,
        jnp.concatenate([result] * groups, axis=0),
        NT,
        preferred_element_type=F32,
    )
    m = [jnp.broadcast_to(motion[k : k + 1, :], (SUB, LANES)) for k in range(6)]
    qa = 1.0 / jnp.sqrt(1.0 + m[0] * m[0] + m[1] * m[1] + m[2] * m[2])
    qb, qc, qd = m[0] * qa, m[1] * qa, m[2] * qa
    aa, bb, cc, dd = qa * qa, qb * qb, qc * qc, qd * qd
    ab, ac, ad = qa * qb, qa * qc, qa * qd
    bc, bd, cd = qb * qc, qb * qd, qc * qd
    spin = [
        [aa + bb - cc - dd, 2.0 * (bc - ad), 2.0 * (bd + ac)],
        [2.0 * (bc + ad), aa - bb + cc - dd, 2.0 * (cd - ab)],
        [2.0 * (bd - ac), 2.0 * (cd + ab), aa - bb - cc + dd],
    ]
    column = lax.rem(comp8, 3)
    packed = rsel[3]
    for b in range(3):
        value = jnp.where(column == 0, spin[b][0], jnp.where(column == 1, spin[b][1], spin[b][2]))
        value = jnp.where(comp8 < 9, value, m[3 + b])
        packed = packed + rsel[b] * value
    lines = fbuf.shape[1]
    me = z * 2 + p
    fbuf[me] = packed[0:lines, :]

    steps = sorted(
        ((d, c) for d in range(n) for c in (0, 1) if (d, c) != (0, 0)),
        key=lambda s: (-min(s[0], n - s[0]), s[1]),
    )
    for d, c in steps:
        device = {"blk": lax.rem(z + d, n), "pair": p if c == 0 else other}
        pltpu.make_async_remote_copy(
            src_ref=fbuf.at[me],
            dst_ref=fbuf.at[me],
            send_sem=f_sem.at[0],
            recv_sem=f_sem.at[1],
            device_id=device,
            device_id_type=MESH,
        ).start()
    give_s.start()
    give_s.wait_recv()
    out_single[theirs, :] = sbuf[1].astype(BF16)
    f_all = pltpu.make_async_remote_copy(
        src_ref=fbuf.at[0 : 2 * n - 1],
        dst_ref=fbuf.at[0 : 2 * n - 1],
        send_sem=f_sem.at[0],
        recv_sem=f_sem.at[1],
        device_id={"pair": other},
        device_id_type=MESH,
    )
    f_all.wait_recv()

    gap = (lax.broadcasted_iota(jnp.int32, (SUB, LANES), 0) - part8) & (SUB - 1)
    for t in range(2 * n // groups):
        for line_number in range(2):
            tile = fbuf[t * groups : (t + 1) * groups, line_number, :]
            out = tile
            for s in range(1, groups):
                out = jnp.where(gap == s, roll(roll(tile, s, 0), -half * s, 1), out)
            height = 8 if line_number == 0 else 4
            out_frames[8 * line_number : 8 * line_number + height, t * LANES : (t + 1) * LANES] = out[:height]

    def sent(count, sem):
        pltpu.make_async_remote_copy(
            src_ref=held_block(buf, 0, count),
            dst_ref=held_block(buf, 0, count),
            send_sem=send_sem.at[sem],
            recv_sem=recv_sem.at[0],
            device_id={"blk": lax.rem(z + 1, n)},
            device_id_type=MESH,
        ).wait_send()

    @pl.when(p == 1)
    def _():
        sent(n - 1, 0)
        sent(n - 1 - len(children[0]) + len(anchors) - 1, 1)

    @pl.when(p == 0)
    def _():
        sent(len(children[0]), 0)

    if nx > 1:
        x_all.wait_send()
    f_all.wait_send()
    give.wait_send()
    give_s.wait_send()


def hand_over(single_in, frames_in, single_out, frames_out):
    single_out[...] = single_in[...]
    frames_out[...] = frames_in[...]


def body(n, nx, *args):
    (
        single,
        pair,
        frames,
        chain,
        mask,
        w_q,
        w_kv,
        w_qp,
        w_kvp,
        w_pb,
        head_w,
        chain_b,
        w_out,
        gain,
        w_bb,
    ) = args
    rows, half = single.shape[0], pair.shape[2]
    heads = w_pb.shape[1]
    ch = w_q.shape[1] // heads
    pq = w_qp.shape[1] // (3 * heads)
    nv = w_kvp.shape[1] // (3 * heads) - pq
    chunk = min(8, n)
    order, anchors, children = gather_plan(n, 4 if n >= 16 else 2, chunk, 0.9, 0.72, 1.0)
    deltas = sorted({d for kids in children.values() for _, d in kids})
    deltas = sorted(set(deltas) | {-d for d in deltas})
    deltas = [d for i, d in enumerate(deltas) if d % n not in {e % n for e in deltas[:i]}]
    cfg = (n, nx, heads, ch, pq, nv, half, chunk, order, anchors, children, deltas)
    hots, masks = constants(heads, ch, pq, nv)
    hots = [jnp.asarray(h, BF16) for h in hots]
    masks = jnp.asarray(masks, F32)
    vmem = pl.BlockSpec(memory_space=pltpu.VMEM)
    hbm = pl.BlockSpec(memory_space=pl.ANY)
    loads = [
        frames,
        chain.reshape(1, rows),
        mask.reshape(1, rows),
        single,
        w_kv.T,
        w_kvp.T,
        hots[2],
        hots[1],
        hots[0],
        w_q.T,
        w_qp.T,
        w_pb.T,
        head_w.reshape(1, heads),
        chain_b.reshape(1, heads),
        gain.reshape(-1, LANES),
        w_bb.T,
        w_out,
        hots[3],
        hots[4],
        hots[5],
        hots[6],
        masks,
    ]
    cfg += (len(loads),)
    specs = [hbm] + [hbm] * len(loads)
    marks = 3 * pq + 2
    span = chunk * half
    width = w_out.shape[2]
    scratch = [pltpu.VMEM(a.shape, a.dtype) for a in loads] + [
        pltpu.SemaphoreType.DMA((len(loads),)),
        pltpu.VMEM((rows, n, half, LANES), BF16),
        pltpu.VMEM((n * PIECES, QUARTER, LANES), F32),
        pltpu.VMEM((len(anchors) * PIECES, QUARTER, LANES), F32),
        pltpu.VMEM((16, rows), F32),
        pltpu.VMEM((rows, 16), F32),
        pltpu.VMEM((rows, SUB, n * half), F32),
        pltpu.VMEM((rows, marks, SUB, LANES), F32),
        pltpu.VMEM((2, rows * SUB, LANES), BF16),
        pltpu.VMEM((LANES // SUB, SUB, span), F32),
        pltpu.VMEM((rows, SUB, span), F32),
        pltpu.VMEM((rows, SUB, span), F32),
        pltpu.VMEM((rows, SUB, LANES), F32),
        pltpu.VMEM((rows, 2, SUB, LANES), F32),
        pltpu.VMEM((half, 2, SUB, LANES), F32),
        pltpu.VMEM((nx, half, width), F32),
        pltpu.VMEM((2 * n, 2, LANES), F32),
        pltpu.VMEM((2, half, width), F32),
        pltpu.VMEM((2 * LANES, width), BF16),
        pltpu.VMEM((12, half, LANES), F32),
        pltpu.VMEM((4, SUB, LANES), F32),
        pltpu.SemaphoreType.DMA,
        pltpu.SemaphoreType.DMA((2,)),
        pltpu.SemaphoreType.DMA((2 * len(anchors) + n // chunk,)),
        pltpu.SemaphoreType.DMA((2,)),
        pltpu.SemaphoreType.DMA((2,)),
        pltpu.SemaphoreType.DMA((2,)),
        pltpu.SemaphoreType.DMA((2,)),
    ]
    results = pl.pallas_call(
        functools.partial(kernel, cfg),
        out_shape=(
            jax.ShapeDtypeStruct(single.shape, BF16),
            jax.ShapeDtypeStruct((12, n * rows), F32),
        ),
        in_specs=specs,
        out_specs=(vmem, vmem),
        scratch_shapes=scratch,
        compiler_params=pltpu.CompilerParams(collective_id=0, has_side_effects=True),
        name="layer",
    )(pair, *loads)
    return pl.pallas_call(
        hand_over,
        out_shape=(
            jax.ShapeDtypeStruct(single.shape, BF16),
            jax.ShapeDtypeStruct((12, n * rows), F32),
        ),
        in_specs=[vmem, vmem],
        out_specs=(vmem, vmem),
        name="results",
    )(*results)


def solution(mesh):
    placed = (
        P(("groups", "blk"), None),
        P(("groups", "blk"), None, "pair", None),
        P(None, ("groups", "blk")),
        P(("groups", "blk")),
        P(("groups", "blk")),
        P(None, "head"),
        P(None, "head"),
        P(None, "head"),
        P(None, "head"),
        P(None, "head"),
        P("head"),
        P("head"),
        P("head", None, None),
        P(),
        P(),
    )
    return jax.shard_map(
        functools.partial(body, mesh.shape["blk"], mesh.shape["head"]),
        mesh=mesh,
        in_specs=placed,
        out_specs=(P(("groups", "blk"), None), P(None, "groups")),
        check_vma=False,
    )
```

```python
import functools
import math

import jax
import jax.numpy as jnp
import numpy as np
from jax import lax
from jax.experimental import pallas as pl
from jax.experimental.pallas import tpu as pltpu
from jax.sharding import PartitionSpec as P

MESH = pl.DeviceIdType.MESH
HIGH = lax.Precision.HIGHEST
F32 = jnp.float32
BF16 = jnp.bfloat16
LW = math.sqrt(1.0 / 3.0)
MASK_PENALTY = 100000.0
KEY_PATH = 9
PIECES = 7
QUARTER = 4
THIRD = 32
LANES = 128
SUB = 8
NT = (((1,), (1,)), ((), ()))

CHAIN_LANE = 7
MASK_LANE = 15
ONE_LANE = 120
TOP_LANE = 121


def gather_plan(n, stride, chunk, fixed, hop, weight):
    low, high = -((n - 1) // 2), n // 2
    when, parent = {0: 0.0}, {}
    anchors = [0]
    for sign in (1, -1):
        for k in range(1, n):
            o = sign * k * stride
            if not (low <= o <= high) or abs(o) > n // 2 - 2:
                break
            anchors.append(o)
            parent[o] = (o - sign * stride, sign * stride)
            when[o] = when[o - sign * stride] + fixed + hop * stride
    for o in range(low, high + 1):
        if o in when:
            continue
        best = min(
            anchors,
            key=lambda a: (when[a] + fixed + (hop + weight) * abs(o - a), abs(a)),
        )
        parent[o] = (best, o - best)
        when[o] = when[best] + fixed + hop * abs(o - best)
    order = sorted(when, key=lambda o: (when[o], abs(o), o))
    order = [
        o
        for c in range(0, n, chunk)
        for o in sorted(order[c : c + chunk], key=lambda o: (o not in anchors, when[o]))
    ]
    anchors = sorted(anchors, key=lambda o: (when[o], -o))
    children = {}
    for o, (p, delta) in parent.items():
        children.setdefault(p, []).append((o, delta))
    for p in children:
        children[p].sort(key=lambda c: (c[0] not in anchors, -abs(c[1])))
    return order, anchors, children


def constants(heads, ch, pq, pv):
    key_lane = lambda h, c: ((h * ch + c) // 4) * 8 + 3 + (h * ch + c) % 4
    kp_lane = lambda h, p, a: (p * 3 + a) * 8 + h
    v_lane = lambda h, c: h * ch + c
    vp_lane = lambda h, p, a: heads * ch + a * heads * pv + h * pv + p
    kv = np.zeros((heads * 2 * ch, 2 * LANES), np.float32)
    kp = np.zeros((heads * (pq + pv) * 3, 6 * LANES), np.float32)
    fr = np.zeros((16, 8 * LANES), np.float32)
    q = np.zeros((heads * ch, LANES), np.float32)
    qp = np.zeros((heads * pq * 3, 3 * LANES), np.float32)
    pa = np.zeros((LANES, LANES), np.float32)
    masks = np.zeros((3, SUB, LANES), np.float32)
    perm = np.zeros((2 * LANES, heads * (ch + 4 * pv)), np.float32)
    small = ch + 4 * pv
    for h in range(heads):
        for c in range(ch):
            kv[h * 2 * ch + c, key_lane(h, c)] = 1
            kv[h * 2 * ch + ch + c, LANES + v_lane(h, c)] = 1
            q[h * ch + c, key_lane(h, c)] = 1
            masks[0, h, key_lane(h, c)] = 1
            masks[2, h, v_lane(h, c)] = 1
            perm[v_lane(h, c), h * small + c] = 1
        for p in range(pq):
            for a in range(3):
                lane = kp_lane(h, p, a)
                masks[1, h, lane] = 1
                pa[lane, p * 3 + a] = 1
                for b in range(3):
                    kp[(h * (pq + pv) + p) * 3 + b, 2 * b * LANES + lane] = 1
                    qp[(h * pq + p) * 3 + b, b * LANES + lane] = 1
                    fr[3 * a + b, 2 * b * LANES + lane] = 1
                fr[9 + a, 6 * LANES + lane] = 1
        for p in range(pv):
            for a in range(3):
                lane = vp_lane(h, p, a)
                masks[2, h, lane] = 1
                perm[lane, h * small + ch + p * 3 + a] = 1
                line = 0 if lane >= 3 * THIRD else 1
                for b in range(3):
                    kp[(h * (pq + pv) + pq + p) * 3 + b, (2 * b + line) * LANES + lane] = 1
                    fr[3 * a + b, (2 * b + line) * LANES + lane] = 1
                fr[9 + a, (6 + line) * LANES + lane] = 1
            perm[LANES + vp_lane(h, p, 0), h * small + ch + 3 * pv + p] = 1
    masks[1, :heads, CHAIN_LANE] = 1
    masks[1, :heads, MASK_LANE] = 1
    pa[CHAIN_LANE, 12] = 1
    pa[MASK_LANE, 13] = 1
    fr[12, 6 * LANES + CHAIN_LANE] = 1
    fr[13, 6 * LANES + MASK_LANE] = 1
    return (kv, kp, fr, q, qp, pa, perm), masks.reshape(3 * SUB, LANES)


def pieces3(x):
    a = x.astype(BF16)
    r = x - a.astype(F32)
    b = r.astype(BF16)
    c = (r - b.astype(F32)).astype(BF16)
    return a, b, c


def select(x, onehot):
    m = x.shape[0]
    y = jnp.dot(jnp.concatenate(pieces3(x), axis=0), onehot, preferred_element_type=F32)
    return y[:m] + y[m : 2 * m] + y[2 * m :]


def roll(x, shift, axis):
    shift %= x.shape[axis]
    return x if shift == 0 else pltpu.roll(x, shift, axis)


def kernel(
    cfg,
    pair,
    *refs,
):
    n_loads = cfg[-1]
    sources, (out_single, out_frames) = refs[:n_loads], refs[n_loads : n_loads + 2]
    held = refs[n_loads + 2 : 2 * n_loads + 2]
    run(cfg[:-1], pair, sources, held, out_single, out_frames, *refs[2 * n_loads + 2 :])


def run(
    cfg,
    pair,
    sources,
    held,
    out_single,
    out_frames,
    load_sem,
    pv,
    buf,
    rbuf,
    stack,
    ft,
    bias,
    qpb,
    qblk,
    kt,
    dots,
    wts,
    alpha,
    acc,
    mbuf,
    xbuf,
    fbuf,
    sbuf,
    wp,
    rb,
    rsel,
    pair_sem,
    send_sem,
    recv_sem,
    m_sem,
    x_sem,
    s_sem,
    f_sem,
):
    n, nx, heads, ch, pq, nv, half, chunk, order, anchors, children, deltas = cfg
    rows = 2 * half
    z = lax.axis_index("blk")
    x = lax.axis_index("head")
    p = lax.axis_index("pair")
    other = 1 - p
    slot_of = {o: i for i, o in enumerate(order)}

    group_of = {o: len(anchors) + i // chunk for i, o in enumerate(order)}
    group_of.update({o: i for i, o in enumerate(anchors)})
    hub_slot = {o: i for i, o in enumerate(anchors)}

    def block(o):
        return lax.rem(z - o + 2 * n, n)

    lane16 = lax.broadcasted_iota(jnp.int32, (half, LANES), 1)

    barrier = pltpu.get_barrier_semaphore()
    near_first = sorted(deltas, key=abs)
    for d in near_first[-2:]:
        for core in (p, other):
            pl.semaphore_signal(
                barrier,
                inc=1,
                device_id={"blk": lax.rem(z + d + n, n), "pair": core},
                device_id_type=MESH,
            )

    loads = [
        pltpu.make_async_copy(source, place, load_sem.at[k])
        for k, (source, place) in enumerate(zip(sources, held))
    ]
    for copy in loads[:KEY_PATH]:
        copy.start()

    def greet(d, core):
        pl.semaphore_signal(
            barrier,
            inc=1,
            device_id={"blk": lax.rem(z + d + n, n), "pair": core},
            device_id_type=MESH,
        )

    for d in near_first[:-2]:
        for core in (p, other):
            greet(d, core)
    for d in range(1, nx):
        pl.semaphore_signal(
            barrier, inc=1, device_id={"head": lax.rem(x + d, nx)}, device_id_type=MESH
        )
    pl.semaphore_signal(barrier, inc=1, device_id={"pair": other}, device_id_type=MESH)
    signals = 2 * len(deltas) + nx
    for copy in loads[KEY_PATH:]:
        copy.start()
    (frames, chain, mask, single, w_kv, w_kvp, c_fr, c_kp, c_kv) = held[:KEY_PATH]
    (w_q, w_qp, w_pb, head_w, chain_b, gain, w_bb, w_out, c_q, c_qp, c_pa, c_perm, c_masks) = held[
        KEY_PATH:
    ]

    for copy in loads[:KEY_PATH]:
        copy.wait()
    for o in order:
        pltpu.make_async_copy(pair.at[:, block(o)], pv.at[:, slot_of[o]], pair_sem).start()

    stack[...] = jnp.zeros_like(stack)
    stack[0:12, :] = frames[...]
    stack[12:13, :] = chain[...].astype(F32)
    stack[13:14, :] = mask[...].astype(F32)
    eye = (
        lax.broadcasted_iota(jnp.int32, (rows, rows), 0)
        == lax.broadcasted_iota(jnp.int32, (rows, rows), 1)
    ).astype(F32)
    ft[...] = lax.dot_general(eye, stack[...], NT, precision=HIGH, preferred_element_type=F32)
    mine = pl.ds(pl.multiple_of(p * half, half), half)
    theirs = pl.ds(pl.multiple_of(other * half, half), half)
    ks = single[mine, :]
    key_value = lax.dot_general(ks, w_kv[...], NT, preferred_element_type=F32)
    key_local = lax.dot_general(ks, w_kvp[...], NT, preferred_element_type=F32)
    turn = select(ft[mine, :], c_fr[...])
    local = select(key_local, c_kp[...])
    width = 2 * LANES
    line = select(key_value, c_kv[...]) + turn[:, 3 * width :]
    for b in range(3):
        line += turn[:, b * width : (b + 1) * width] * local[:, b * width : (b + 1) * width]
    near_line = line[:, :LANES]
    for k in range(4):
        buf[k] = near_line[QUARTER * k : QUARTER * (k + 1)]
    far_line = line[:, LANES:]
    last_rows = far_line[3 * QUARTER :]
    lane4 = lax.broadcasted_iota(jnp.int32, (QUARTER, LANES), 1)
    for k in range(3):
        moved_rows = roll(last_rows, 3 * THIRD - k * THIRD, 1)
        buf[4 + k] = jnp.where(
            lane4 < 3 * THIRD, far_line[QUARTER * k : QUARTER * (k + 1)], moved_rows
        )

    def send(src, place, group, delta, core, sem):
        pltpu.make_async_remote_copy(
            src_ref=src,
            dst_ref=place,
            send_sem=send_sem.at[sem],
            recv_sem=recv_sem.at[group],
            device_id={"blk": lax.rem(z + delta + n, n), "pair": core},
            device_id_type=MESH,
        ).start()

    def held_block(ref, first, last=None):
        last = first + 1 if last is None else last
        return ref.at[first * PIECES : last * PIECES]

    def relay(o):
        for child, delta in children.get(o, []):
            send(held_block(buf, slot_of[o]), held_block(buf, slot_of[child]), group_of[child], delta, p, 0)

    hub_group = {o: len(anchors) + n // chunk + i for i, o in enumerate(anchors)}

    def hub_relay(o):
        src = held_block(rbuf, hub_slot[o])
        for child, delta in children.get(o, []):
            if child in anchors:
                send(src, held_block(rbuf, hub_slot[child]), hub_group[child], delta, 1, 1)
            else:
                send(src, held_block(buf, slot_of[child]), group_of[child], delta, 0, 1)
        send(src, held_block(buf, slot_of[o]), group_of[o], 0, 0, 1)

    def first_sends():
        for child, delta in children[0]:
            if child in anchors:
                send(held_block(buf, 0), held_block(rbuf, hub_slot[child]), hub_group[child], delta, 1, 0)
            else:
                send(held_block(buf, 0), held_block(buf, slot_of[child]), group_of[child], delta, 0, 0)

    def take(ref, first, last, group):
        pltpu.make_async_remote_copy(
            src_ref=held_block(ref, first, last),
            dst_ref=held_block(ref, first, last),
            send_sem=send_sem.at[0],
            recv_sem=recv_sem.at[group],
            device_id={"blk": lax.rem(z + 1, n)},
            device_id_type=MESH,
        ).wait_recv()

    pl.semaphore_wait(barrier, signals)

    @pl.when(p == 1)
    def _():
        relay(0)

    @pl.when(p == 0)
    def _():
        first_sends()


    for copy in loads[KEY_PATH:]:
        copy.wait()
    full = ft[...]
    query = lax.dot_general(single[...], w_q[...], NT, preferred_element_type=F32)
    query = select(query, c_q[...]) * (LW / math.sqrt(ch))
    q_local = select(
        lax.dot_general(single[...], w_qp[...], NT, preferred_element_type=F32), c_qp[...]
    )
    q_turn = select(full, c_fr[...])
    q_line = q_turn[:, 3 * width : 3 * width + LANES]
    for b in range(3):
        q_line += (
            q_turn[:, b * width : b * width + LANES] * q_local[:, b * LANES : (b + 1) * LANES]
        )
    head_keys = c_masks[0:SUB, :]
    head_points = c_masks[SUB : 2 * SUB, :]
    head_values = c_masks[2 * SUB : 3 * SUB, :]
    wide_query = (query[:, None, :] * head_keys[None]).reshape(rows * SUB, LANES)
    coarse = wide_query.astype(BF16)
    qblk[0] = coarse
    qblk[1] = (wide_query - coarse.astype(F32)).astype(BF16)
    spread = select((q_line[:, None, :] * head_points[None]).reshape(rows * SUB, LANES), c_pa[...])
    spread = spread.reshape(rows, SUB, LANES)
    marks = 3 * pq + 2
    for k in range(marks):
        qpb[:, k] = jnp.broadcast_to(spread[:, :, k : k + 1], (rows, SUB, LANES))

    diagonal = lax.broadcasted_iota(jnp.int32, (SUB, heads), 0) == lax.broadcasted_iota(
        jnp.int32, (SUB, heads), 1
    )

    def down(row):
        column = jnp.sum(jnp.where(diagonal, row, 0.0), axis=1, keepdims=True)
        return jnp.broadcast_to(column, (SUB, LANES))

    raw = down(head_w[...])
    cross = down(chain_b[...]) * LW
    soft = jnp.maximum(raw, 0.0) + jnp.log1p(jnp.exp(-jnp.abs(raw)))
    near = soft * (LW * math.sqrt(2.0 / (9.0 * pq)) / 2.0)

    w_bias = jnp.dot(diagonal.astype(BF16), w_pb[...], preferred_element_type=F32).astype(BF16)

    pltpu.make_async_copy(pair, pv, pair_sem).wait()

    keys = n * half

    def bias_of(i, _):
        bias[i] = LW * lax.dot_general(
            w_bias, pv[i].reshape(keys, LANES), NT, preferred_element_type=F32
        )
        return 0

    lax.fori_loop(0, rows, bias_of, 0, unroll=8)

    short = w_out.shape[1] - LANES
    w_short = w_out[:, 0:short, :].reshape(heads * short, w_out.shape[2])
    wp[...] = jnp.dot(c_perm[...], w_short, preferred_element_type=F32).astype(BF16)
    mine_ft = ft[mine, :]
    for k in range(12):
        rb[k] = jnp.broadcast_to(mine_ft[:, k : k + 1], (half, LANES))
    lane = lax.broadcasted_iota(jnp.int32, (rows, LANES), 1)
    repeat = ((lane & (half - 1)) + p * half == lax.broadcasted_iota(jnp.int32, (rows, LANES), 0)).astype(BF16)
    wide = select(stack[...], repeat)
    lane8 = lax.broadcasted_iota(jnp.int32, (SUB, LANES), 1)
    part8 = lax.div(lane8, half)
    comp8 = lax.broadcasted_iota(jnp.int32, (SUB, LANES), 0) * (LANES // half) + part8
    for b in range(4):
        picked = jnp.zeros((SUB, LANES), F32)
        for k in range(12):
            source = (k - k % 3 + b if k < 9 else 3 * (k - 9) + b) if b < 3 else k
            if b == 3 and k < 9:
                continue
            picked = jnp.where(comp8 == k, wide[source : source + 1, :], picked)
        rsel[b] = picked
    eye_b = (
        lax.broadcasted_iota(jnp.int32, (SUB, w_bb.shape[0]), 0)
        == lax.broadcasted_iota(jnp.int32, (SUB, w_bb.shape[0]), 1)
    ).astype(BF16)
    w_motion = jnp.dot(eye_b, w_bb[...], preferred_element_type=F32).astype(BF16)

    def unpacked(slot):
        piece = [buf[slot * PIECES + k] for k in range(PIECES)]
        near_line = jnp.concatenate(piece[:4], axis=0)
        tail = jnp.zeros((QUARTER, LANES), F32)
        lane4 = lax.broadcasted_iota(jnp.int32, (QUARTER, LANES), 1)
        for k in range(3):
            tail = jnp.where(
                (lane4 >= k * THIRD) & (lane4 < (k + 1) * THIRD), roll(piece[4 + k], k * THIRD - 3 * THIRD, 1), tail
            )
        far_line = jnp.concatenate(piece[4:] + [tail], axis=0)
        far_line = jnp.where(lane16 < 3 * THIRD, far_line, near_line)
        return near_line, jnp.where(lane16 == ONE_LANE, 1.0, far_line)

    span = chunk * half
    acc[...] = jnp.zeros_like(acc)
    alpha[...] = jnp.full(alpha.shape, -1e30, F32)
    def pass_on(these):
        @pl.when(p == 1)
        def _():
            for reach in sorted({abs(o) for o in these}):
                level = [o for o in these if abs(o) == reach]
                for o in level:
                    take(buf, slot_of[o], slot_of[o] + 1, group_of[o])
                    relay(o)
                for o in level:
                    take(rbuf, hub_slot[o], hub_slot[o] + 1, hub_group[o])
                    hub_relay(o)

        @pl.when(p == 0)
        def _():
            for o in these:
                take(buf, slot_of[o], slot_of[o] + 1, group_of[o])

    late = [o for o in anchors if o not in order[:chunk] and abs(o) == max(abs(a) for a in anchors)]
    pass_on([o for o in anchors if o != 0 and o not in late])
    for c in range(n // chunk):
        if c == min(2, n // chunk - 1):
            pass_on(late)
        slots = slice(c * chunk, (c + 1) * chunk)
        first = c * chunk + sum(o in anchors for o in order[slots])
        last = (c + 1) * chunk
        if first < last:
            take(buf, first, last, len(anchors) + c)
        lines = [unpacked(slot) for slot in range(c * chunk, (c + 1) * chunk)]
        kc = jnp.concatenate([a for a, _ in lines], axis=0)
        vc = jnp.concatenate([b for _, b in lines], axis=0)
        kt[...] = kc.T.reshape(LANES // SUB, SUB, span)
        k_coarse = kc.astype(BF16)
        k_fine = (kc - k_coarse.astype(F32)).astype(BF16)
        products = [
            lax.dot_general(a, b, NT, preferred_element_type=F32)
            for a, b in ((qblk[0], k_coarse), (qblk[0], k_fine), (qblk[1], k_coarse))
        ]
        dots[...] = (products[0] + products[1] + products[2]).reshape(rows, SUB, span)
        chain_j = kt[0, 7:8, :]
        mask_j = kt[1, 7:8, :]

        def one_row(i, _):
            far = jnp.zeros((SUB, span), F32)
            for k in range(3 * pq):
                gap = qpb[i, k][:, :span] - kt[k]
                far += gap * gap
            differ = jnp.where(qpb[i, 3 * pq][:, :span] != chain_j, cross[:, :span], 0.0)
            absent = 1.0 - qpb[i, 3 * pq + 1][:, :span] * mask_j
            logits = (
                dots[i]
                + bias[i, :, c * span : (c + 1) * span]
                - near[:, :span] * far
                + differ
                - MASK_PENALTY * absent
            )
            old = alpha[i]
            top = jnp.maximum(old, jnp.max(logits, axis=1, keepdims=True))
            w = jnp.exp(logits - top[:, :span])
            wts[i] = w
            alpha[i] = top
            scale = jnp.exp(old - top)
            acc[i, 1] = acc[i, 1] * scale
            acc[i, 0] = acc[i, 0] * scale + jnp.dot(
                w.astype(BF16),
                pv[i, slots].reshape(span, LANES),
                preferred_element_type=F32,
            )
            return 0

        lax.fori_loop(0, rows, one_row, 0, unroll=rows)
        acc[:, 1] += jnp.dot(
            wts[...].reshape(rows * SUB, span), vc, precision=HIGH, preferred_element_type=F32
        ).reshape(rows, SUB, LANES)

    lane3 = lax.broadcasted_iota(jnp.int32, (rows, SUB, LANES), 2)
    acc[:, 1] = jnp.where(lane3 == TOP_LANE, alpha[...], acc[:, 1])
    give = pltpu.make_async_remote_copy(
        src_ref=acc.at[theirs],
        dst_ref=mbuf,
        send_sem=m_sem.at[0],
        recv_sem=m_sem.at[1],
        device_id={"pair": other},
        device_id_type=MESH,
    )
    give.start()
    give.wait_recv()
    own_p, own_b = acc[mine, 0], acc[mine, 1]
    far_p, far_b = mbuf[:, 0], mbuf[:, 1]
    own_top, far_top = own_b[:, :, TOP_LANE : TOP_LANE + 1], far_b[:, :, TOP_LANE : TOP_LANE + 1]
    top = jnp.maximum(own_top, far_top)
    own_scale, far_scale = jnp.exp(own_top - top), jnp.exp(far_top - top)
    both_b = own_b * own_scale + far_b * far_scale
    total = both_b[:, :, ONE_LANE : ONE_LANE + 1]
    both_b = both_b / total * head_values[None]
    paired = (own_p * own_scale + far_p * far_scale) / total
    mbuf[:, 0] = paired
    sums = jnp.sum(both_b, axis=1)
    first = heads * ch
    third = heads * nv
    moved = [roll(sums, -a * third, 1) - rb[9 + a] for a in range(3)]
    pointed = [sum(rb[3 * a + b] * moved[a] for a in range(3)) for b in range(3)]
    norms = jnp.sqrt(pointed[0] * pointed[0] + pointed[1] * pointed[1] + pointed[2] * pointed[2] + 1.0)
    joined = sums
    for b in range(3):
        joined = jnp.where(
            (lane16 >= first + b * third) & (lane16 < first + (b + 1) * third),
            roll(pointed[b], b * third, 1),
            joined,
        )
    norms = jnp.where((lane16 >= first) & (lane16 < first + third), norms, 0.0)
    features = jnp.concatenate([joined, norms], axis=1).astype(BF16)
    update = jnp.dot(features, wp[...], preferred_element_type=F32)
    for h in range(heads):
        update += jnp.dot(
            mbuf[:, 0, h, :].astype(BF16), w_out[h, short:, :], preferred_element_type=F32
        )

    xbuf[x] = update
    for d in sorted(range(1, nx), key=lambda d: -min(d, nx - d)):
        pltpu.make_async_remote_copy(
            src_ref=xbuf.at[x],
            dst_ref=xbuf.at[x],
            send_sem=x_sem.at[0],
            recv_sem=x_sem.at[1],
            device_id={"head": lax.rem(x + d, nx)},
            device_id_type=MESH,
        ).start()
    x_all = pltpu.make_async_remote_copy(
        src_ref=xbuf.at[0 : nx - 1],
        dst_ref=xbuf.at[0 : nx - 1],
        send_sem=x_sem.at[0],
        recv_sem=x_sem.at[1],
        device_id={"head": lax.rem(x + 1, nx)},
        device_id_type=MESH,
    )
    if nx > 1:
        x_all.wait_recv()
    update = xbuf[0]
    for k in range(1, nx):
        update = update + xbuf[k]
    mixed = single[mine, :].astype(F32) + update
    count = mixed.shape[1]
    gains = jnp.concatenate([gain[k : k + 1, :] for k in range(count // LANES)], axis=1)
    centre = jnp.sum(mixed, axis=1, keepdims=True) * (1.0 / count)
    apart = mixed - centre
    variance = jnp.sum(apart * apart, axis=1, keepdims=True) * (1.0 / count)
    result = (apart * lax.rsqrt(variance + 1e-05) * gains).astype(BF16)
    out_single[mine, :] = result
    sbuf[0] = result.astype(F32)
    give_s = pltpu.make_async_remote_copy(
        src_ref=sbuf.at[0],
        dst_ref=sbuf.at[1],
        send_sem=s_sem.at[0],
        recv_sem=s_sem.at[1],
        device_id={"pair": other},
        device_id_type=MESH,
    )

    groups = LANES // half
    motion = lax.dot_general(
        w_motion,
        jnp.concatenate([result] * groups, axis=0),
        NT,
        preferred_element_type=F32,
    )
    m = [jnp.broadcast_to(motion[k : k + 1, :], (SUB, LANES)) for k in range(6)]
    qa = 1.0 / jnp.sqrt(1.0 + m[0] * m[0] + m[1] * m[1] + m[2] * m[2])
    qb, qc, qd = m[0] * qa, m[1] * qa, m[2] * qa
    aa, bb, cc, dd = qa * qa, qb * qb, qc * qc, qd * qd
    ab, ac, ad = qa * qb, qa * qc, qa * qd
    bc, bd, cd = qb * qc, qb * qd, qc * qd
    spin = [
        [aa + bb - cc - dd, 2.0 * (bc - ad), 2.0 * (bd + ac)],
        [2.0 * (bc + ad), aa - bb + cc - dd, 2.0 * (cd - ab)],
        [2.0 * (bd - ac), 2.0 * (cd + ab), aa - bb - cc + dd],
    ]
    column = lax.rem(comp8, 3)
    packed = rsel[3]
    for b in range(3):
        value = jnp.where(column == 0, spin[b][0], jnp.where(column == 1, spin[b][1], spin[b][2]))
        value = jnp.where(comp8 < 9, value, m[3 + b])
        packed = packed + rsel[b] * value
    lines = fbuf.shape[1]
    me = z * 2 + p
    fbuf[me] = packed[0:lines, :]

    steps = sorted(
        ((d, c) for d in range(n) for c in (0, 1) if (d, c) != (0, 0)),
        key=lambda s: (-min(s[0], n - s[0]), s[1]),
    )
    for d, c in steps:
        device = {"blk": lax.rem(z + d, n), "pair": p if c == 0 else other}
        pltpu.make_async_remote_copy(
            src_ref=fbuf.at[me],
            dst_ref=fbuf.at[me],
            send_sem=f_sem.at[0],
            recv_sem=f_sem.at[1],
            device_id=device,
            device_id_type=MESH,
        ).start()
    give_s.start()
    give_s.wait_recv()
    out_single[theirs, :] = sbuf[1].astype(BF16)
    f_all = pltpu.make_async_remote_copy(
        src_ref=fbuf.at[0 : 2 * n - 1],
        dst_ref=fbuf.at[0 : 2 * n - 1],
        send_sem=f_sem.at[0],
        recv_sem=f_sem.at[1],
        device_id={"pair": other},
        device_id_type=MESH,
    )
    f_all.wait_recv()

    gap = (lax.broadcasted_iota(jnp.int32, (SUB, LANES), 0) - part8) & (SUB - 1)
    for t in range(2 * n // groups):
        for line_number in range(2):
            tile = fbuf[t * groups : (t + 1) * groups, line_number, :]
            out = tile
            for s in range(1, groups):
                out = jnp.where(gap == s, roll(roll(tile, s, 0), -half * s, 1), out)
            height = 8 if line_number == 0 else 4
            out_frames[8 * line_number : 8 * line_number + height, t * LANES : (t + 1) * LANES] = out[:height]

    def sent(count, sem):
        pltpu.make_async_remote_copy(
            src_ref=held_block(buf, 0, count),
            dst_ref=held_block(buf, 0, count),
            send_sem=send_sem.at[sem],
            recv_sem=recv_sem.at[0],
            device_id={"blk": lax.rem(z + 1, n)},
            device_id_type=MESH,
        ).wait_send()

    @pl.when(p == 1)
    def _():
        sent(n - 1, 0)
        sent(n - 1 - len(children[0]) + len(anchors) - 1, 1)

    @pl.when(p == 0)
    def _():
        sent(len(children[0]), 0)

    if nx > 1:
        x_all.wait_send()
    f_all.wait_send()
    give.wait_send()
    give_s.wait_send()


def hand_over(single_in, frames_in, single_out, frames_out):
    single_out[...] = single_in[...]
    frames_out[...] = frames_in[...]


def body(n, nx, *args):
    (
        single,
        pair,
        frames,
        chain,
        mask,
        w_q,
        w_kv,
        w_qp,
        w_kvp,
        w_pb,
        head_w,
        chain_b,
        w_out,
        gain,
        w_bb,
    ) = args
    rows, half = single.shape[0], pair.shape[2]
    heads = w_pb.shape[1]
    ch = w_q.shape[1] // heads
    pq = w_qp.shape[1] // (3 * heads)
    nv = w_kvp.shape[1] // (3 * heads) - pq
    chunk = min(8, n)
    order, anchors, children = gather_plan(n, 4 if n >= 16 else 2, chunk, 0.9, 0.72, 1.0)
    deltas = sorted({d for kids in children.values() for _, d in kids})
    deltas = sorted(set(deltas) | {-d for d in deltas})
    deltas = [d for i, d in enumerate(deltas) if d % n not in {e % n for e in deltas[:i]}]
    cfg = (n, nx, heads, ch, pq, nv, half, chunk, order, anchors, children, deltas)
    hots, masks = constants(heads, ch, pq, nv)
    hots = [jnp.asarray(h, BF16) for h in hots]
    masks = jnp.asarray(masks, F32)
    vmem = pl.BlockSpec(memory_space=pltpu.VMEM)
    hbm = pl.BlockSpec(memory_space=pl.ANY)
    loads = [
        frames,
        chain.reshape(1, rows),
        mask.reshape(1, rows),
        single,
        w_kv.T,
        w_kvp.T,
        hots[2],
        hots[1],
        hots[0],
        w_q.T,
        w_qp.T,
        w_pb.T,
        head_w.reshape(1, heads),
        chain_b.reshape(1, heads),
        gain.reshape(-1, LANES),
        w_bb.T,
        w_out,
        hots[3],
        hots[4],
        hots[5],
        hots[6],
        masks,
    ]
    cfg += (len(loads),)
    specs = [hbm] + [hbm] * len(loads)
    marks = 3 * pq + 2
    span = chunk * half
    width = w_out.shape[2]
    scratch = [pltpu.VMEM(a.shape, a.dtype) for a in loads] + [
        pltpu.SemaphoreType.DMA((len(loads),)),
        pltpu.VMEM((rows, n, half, LANES), BF16),
        pltpu.VMEM((n * PIECES, QUARTER, LANES), F32),
        pltpu.VMEM((len(anchors) * PIECES, QUARTER, LANES), F32),
        pltpu.VMEM((16, rows), F32),
        pltpu.VMEM((rows, 16), F32),
        pltpu.VMEM((rows, SUB, n * half), F32),
        pltpu.VMEM((rows, marks, SUB, LANES), F32),
        pltpu.VMEM((2, rows * SUB, LANES), BF16),
        pltpu.VMEM((LANES // SUB, SUB, span), F32),
        pltpu.VMEM((rows, SUB, span), F32),
        pltpu.VMEM((rows, SUB, span), F32),
        pltpu.VMEM((rows, SUB, LANES), F32),
        pltpu.VMEM((rows, 2, SUB, LANES), F32),
        pltpu.VMEM((half, 2, SUB, LANES), F32),
        pltpu.VMEM((nx, half, width), F32),
        pltpu.VMEM((2 * n, 2, LANES), F32),
        pltpu.VMEM((2, half, width), F32),
        pltpu.VMEM((2 * LANES, width), BF16),
        pltpu.VMEM((12, half, LANES), F32),
        pltpu.VMEM((4, SUB, LANES), F32),
        pltpu.SemaphoreType.DMA,
        pltpu.SemaphoreType.DMA((2,)),
        pltpu.SemaphoreType.DMA((2 * len(anchors) + n // chunk,)),
        pltpu.SemaphoreType.DMA((2,)),
        pltpu.SemaphoreType.DMA((2,)),
        pltpu.SemaphoreType.DMA((2,)),
        pltpu.SemaphoreType.DMA((2,)),
    ]
    results = pl.pallas_call(
        functools.partial(kernel, cfg),
        out_shape=(
            jax.ShapeDtypeStruct(single.shape, BF16),
            jax.ShapeDtypeStruct((12, n * rows), F32),
        ),
        in_specs=specs,
        out_specs=(vmem, vmem),
        scratch_shapes=scratch,
        compiler_params=pltpu.CompilerParams(collective_id=0, has_side_effects=True),
        name="layer",
    )(pair, *loads)
    return pl.pallas_call(
        hand_over,
        out_shape=(
            jax.ShapeDtypeStruct(single.shape, BF16),
            jax.ShapeDtypeStruct((12, n * rows), F32),
        ),
        in_specs=[vmem, vmem],
        out_specs=(vmem, vmem),
        name="results",
    )(*results)


def solution(mesh):
    placed = (
        P(("groups", "blk"), None),
        P(("groups", "blk"), None, "pair", None),
        P(None, ("groups", "blk")),
        P(("groups", "blk")),
        P(("groups", "blk")),
        P(None, "head"),
        P(None, "head"),
        P(None, "head"),
        P(None, "head"),
        P(None, "head"),
        P("head"),
        P("head"),
        P("head", None, None),
        P(),
        P(),
    )
    return jax.shard_map(
        functools.partial(body, mesh.shape["blk"], mesh.shape["head"]),
        mesh=mesh,
        in_specs=placed,
        out_specs=(P(("groups", "blk"), None), P(None, "groups")),
        check_vma=False,
    )
```

```python
import functools
import math

import jax
import jax.numpy as jnp
import numpy as np
from jax import lax
from jax.experimental import pallas as pl
from jax.experimental.pallas import tpu as pltpu
from jax.sharding import PartitionSpec as P

MESH = pl.DeviceIdType.MESH
HIGH = lax.Precision.HIGHEST
F32 = jnp.float32
BF16 = jnp.bfloat16
LW = math.sqrt(1.0 / 3.0)
MASK_PENALTY = 100000.0
KEY_PATH = 9
PIECES = 7
QUARTER = 4
THIRD = 32
LANES = 128
SUB = 8
NT = (((1,), (1,)), ((), ()))

CHAIN_LANE = 7
MASK_LANE = 15
ONE_LANE = 120
TOP_LANE = 121


def gather_plan(n, stride, chunk, fixed, hop, weight):
    low, high = -((n - 1) // 2), n // 2
    when, parent = {0: 0.0}, {}
    anchors = [0]
    for sign in (1, -1):
        for k in range(1, n):
            o = sign * k * stride
            if not (low <= o <= high) or abs(o) > n // 2 - 2:
                break
            anchors.append(o)
            parent[o] = (o - sign * stride, sign * stride)
            when[o] = when[o - sign * stride] + fixed + hop * stride
    for o in range(low, high + 1):
        if o in when:
            continue
        best = min(
            anchors,
            key=lambda a: (when[a] + fixed + (hop + weight) * abs(o - a), abs(a)),
        )
        parent[o] = (best, o - best)
        when[o] = when[best] + fixed + hop * abs(o - best)
    order = sorted(when, key=lambda o: (when[o], abs(o), o))
    order = [
        o
        for c in range(0, n, chunk)
        for o in sorted(order[c : c + chunk], key=lambda o: (o not in anchors, when[o]))
    ]
    anchors = sorted(anchors, key=lambda o: (when[o], -o))
    children = {}
    for o, (p, delta) in parent.items():
        children.setdefault(p, []).append((o, delta))
    for p in children:
        children[p].sort(key=lambda c: (c[0] not in anchors, -abs(c[1])))
    return order, anchors, children


def constants(heads, ch, pq, pv):
    key_lane = lambda h, c: ((h * ch + c) // 4) * 8 + 3 + (h * ch + c) % 4
    kp_lane = lambda h, p, a: (p * 3 + a) * 8 + h
    v_lane = lambda h, c: h * ch + c
    vp_lane = lambda h, p, a: heads * ch + a * heads * pv + h * pv + p
    kv = np.zeros((heads * 2 * ch, 2 * LANES), np.float32)
    kp = np.zeros((heads * (pq + pv) * 3, 6 * LANES), np.float32)
    fr = np.zeros((16, 8 * LANES), np.float32)
    q = np.zeros((heads * ch, LANES), np.float32)
    qp = np.zeros((heads * pq * 3, 3 * LANES), np.float32)
    pa = np.zeros((LANES, LANES), np.float32)
    masks = np.zeros((3, SUB, LANES), np.float32)
    perm = np.zeros((2 * LANES, heads * (ch + 4 * pv)), np.float32)
    small = ch + 4 * pv
    for h in range(heads):
        for c in range(ch):
            kv[h * 2 * ch + c, key_lane(h, c)] = 1
            kv[h * 2 * ch + ch + c, LANES + v_lane(h, c)] = 1
            q[h * ch + c, key_lane(h, c)] = 1
            masks[0, h, key_lane(h, c)] = 1
            masks[2, h, v_lane(h, c)] = 1
            perm[v_lane(h, c), h * small + c] = 1
        for p in range(pq):
            for a in range(3):
                lane = kp_lane(h, p, a)
                masks[1, h, lane] = 1
                pa[lane, p * 3 + a] = 1
                for b in range(3):
                    kp[(h * (pq + pv) + p) * 3 + b, 2 * b * LANES + lane] = 1
                    qp[(h * pq + p) * 3 + b, b * LANES + lane] = 1
                    fr[3 * a + b, 2 * b * LANES + lane] = 1
                fr[9 + a, 6 * LANES + lane] = 1
        for p in range(pv):
            for a in range(3):
                lane = vp_lane(h, p, a)
                masks[2, h, lane] = 1
                perm[lane, h * small + ch + p * 3 + a] = 1
                line = 0 if lane >= 3 * THIRD else 1
                for b in range(3):
                    kp[(h * (pq + pv) + pq + p) * 3 + b, (2 * b + line) * LANES + lane] = 1
                    fr[3 * a + b, (2 * b + line) * LANES + lane] = 1
                fr[9 + a, (6 + line) * LANES + lane] = 1
            perm[LANES + vp_lane(h, p, 0), h * small + ch + 3 * pv + p] = 1
    masks[1, :heads, CHAIN_LANE] = 1
    masks[1, :heads, MASK_LANE] = 1
    pa[CHAIN_LANE, 12] = 1
    pa[MASK_LANE, 13] = 1
    fr[12, 6 * LANES + CHAIN_LANE] = 1
    fr[13, 6 * LANES + MASK_LANE] = 1
    return (kv, kp, fr, q, qp, pa, perm), masks.reshape(3 * SUB, LANES)


def pieces3(x):
    a = x.astype(BF16)
    r = x - a.astype(F32)
    b = r.astype(BF16)
    c = (r - b.astype(F32)).astype(BF16)
    return a, b, c


def select(x, onehot):
    m = x.shape[0]
    y = jnp.dot(jnp.concatenate(pieces3(x), axis=0), onehot, preferred_element_type=F32)
    return y[:m] + y[m : 2 * m] + y[2 * m :]


def roll(x, shift, axis):
    shift %= x.shape[axis]
    return x if shift == 0 else pltpu.roll(x, shift, axis)


def kernel(
    cfg,
    pair,
    *refs,
):
    n_loads = cfg[-1]
    sources, (out_single, out_frames) = refs[:n_loads], refs[n_loads : n_loads + 2]
    held = refs[n_loads + 2 : 2 * n_loads + 2]
    run(cfg[:-1], pair, sources, held, out_single, out_frames, *refs[2 * n_loads + 2 :])


def run(
    cfg,
    pair,
    sources,
    held,
    out_single,
    out_frames,
    load_sem,
    pv,
    buf,
    rbuf,
    stack,
    ft,
    bias,
    qpb,
    qblk,
    kt,
    dots,
    wts,
    alpha,
    acc,
    mbuf,
    xbuf,
    fbuf,
    sbuf,
    wp,
    rb,
    rsel,
    pair_sem,
    send_sem,
    recv_sem,
    m_sem,
    x_sem,
    s_sem,
    f_sem,
):
    n, nx, heads, ch, pq, nv, half, chunk, order, anchors, children, deltas = cfg
    rows = 2 * half
    z = lax.axis_index("blk")
    x = lax.axis_index("head")
    p = lax.axis_index("pair")
    other = 1 - p
    slot_of = {o: i for i, o in enumerate(order)}

    group_of = {o: len(anchors) + i // chunk for i, o in enumerate(order)}
    group_of.update({o: i for i, o in enumerate(anchors)})
    hub_slot = {o: i for i, o in enumerate(anchors)}

    def block(o):
        return lax.rem(z - o + 2 * n, n)

    lane16 = lax.broadcasted_iota(jnp.int32, (half, LANES), 1)

    loads = [
        pltpu.make_async_copy(source, place, load_sem.at[k])
        for k, (source, place) in enumerate(zip(sources, held))
    ]
    for copy in loads[:KEY_PATH]:
        copy.start()

    barrier = pltpu.get_barrier_semaphore()
    signals = 0
    for d in deltas:
        for core in (p, other):
            pl.semaphore_signal(
                barrier,
                inc=1,
                device_id={"blk": lax.rem(z + d + n, n), "pair": core},
                device_id_type=MESH,
            )
            signals += 1
    for d in range(1, nx):
        pl.semaphore_signal(
            barrier, inc=1, device_id={"head": lax.rem(x + d, nx)}, device_id_type=MESH
        )
        signals += 1
    pl.semaphore_signal(barrier, inc=1, device_id={"pair": other}, device_id_type=MESH)
    signals += 1

    for copy in loads[KEY_PATH:]:
        copy.start()
    (frames, chain, mask, single, w_kv, w_kvp, c_fr, c_kp, c_kv) = held[:KEY_PATH]
    (w_q, w_qp, w_pb, head_w, chain_b, gain, w_bb, w_out, c_q, c_qp, c_pa, c_perm, c_masks) = held[
        KEY_PATH:
    ]

    for copy in loads[:KEY_PATH]:
        copy.wait()
    for o in order:
        pltpu.make_async_copy(pair.at[:, block(o)], pv.at[:, slot_of[o]], pair_sem).start()

    stack[...] = jnp.zeros_like(stack)
    stack[0:12, :] = frames[...]
    stack[12:13, :] = chain[...].astype(F32)
    stack[13:14, :] = mask[...].astype(F32)
    eye = (
        lax.broadcasted_iota(jnp.int32, (rows, rows), 0)
        == lax.broadcasted_iota(jnp.int32, (rows, rows), 1)
    ).astype(F32)
    ft[...] = lax.dot_general(eye, stack[...], NT, precision=HIGH, preferred_element_type=F32)
    mine = pl.ds(pl.multiple_of(p * half, half), half)
    theirs = pl.ds(pl.multiple_of(other * half, half), half)
    ks = single[mine, :]
    key_value = lax.dot_general(ks, w_kv[...], NT, preferred_element_type=F32)
    key_local = lax.dot_general(ks, w_kvp[...], NT, preferred_element_type=F32)
    turn = select(ft[mine, :], c_fr[...])
    local = select(key_local, c_kp[...])
    width = 2 * LANES
    line = select(key_value, c_kv[...]) + turn[:, 3 * width :]
    for b in range(3):
        line += turn[:, b * width : (b + 1) * width] * local[:, b * width : (b + 1) * width]
    near_line = line[:, :LANES]
    for k in range(4):
        buf[k] = near_line[QUARTER * k : QUARTER * (k + 1)]
    far_line = line[:, LANES:]
    last_rows = far_line[3 * QUARTER :]
    lane4 = lax.broadcasted_iota(jnp.int32, (QUARTER, LANES), 1)
    for k in range(3):
        moved_rows = roll(last_rows, 3 * THIRD - k * THIRD, 1)
        buf[4 + k] = jnp.where(
            lane4 < 3 * THIRD, far_line[QUARTER * k : QUARTER * (k + 1)], moved_rows
        )

    def send(src, place, group, delta, core, sem):
        pltpu.make_async_remote_copy(
            src_ref=src,
            dst_ref=place,
            send_sem=send_sem.at[sem],
            recv_sem=recv_sem.at[group],
            device_id={"blk": lax.rem(z + delta + n, n), "pair": core},
            device_id_type=MESH,
        ).start()

    def held_block(ref, first, last=None):
        last = first + 1 if last is None else last
        return ref.at[first * PIECES : last * PIECES]

    def relay(o):
        for child, delta in children.get(o, []):
            send(held_block(buf, slot_of[o]), held_block(buf, slot_of[child]), group_of[child], delta, p, 0)

    hub_group = {o: len(anchors) + n // chunk + i for i, o in enumerate(anchors)}

    def hub_relay(o):
        src = held_block(rbuf, hub_slot[o])
        for child, delta in children.get(o, []):
            if child in anchors:
                send(src, held_block(rbuf, hub_slot[child]), hub_group[child], delta, 1, 1)
            else:
                send(src, held_block(buf, slot_of[child]), group_of[child], delta, 0, 1)
        send(src, held_block(buf, slot_of[o]), group_of[o], 0, 0, 1)

    def first_sends():
        for child, delta in children[0]:
            if child in anchors:
                send(held_block(buf, 0), held_block(rbuf, hub_slot[child]), hub_group[child], delta, 1, 0)
            else:
                send(held_block(buf, 0), held_block(buf, slot_of[child]), group_of[child], delta, 0, 0)

    def take(ref, first, last, group):
        pltpu.make_async_remote_copy(
            src_ref=held_block(ref, first, last),
            dst_ref=held_block(ref, first, last),
            send_sem=send_sem.at[0],
            recv_sem=recv_sem.at[group],
            device_id={"blk": lax.rem(z + 1, n)},
            device_id_type=MESH,
        ).wait_recv()

    pl.semaphore_wait(barrier, signals)

    @pl.when(p == 1)
    def _():
        relay(0)

    @pl.when(p == 0)
    def _():
        first_sends()


    for copy in loads[KEY_PATH:]:
        copy.wait()
    full = ft[...]
    query = lax.dot_general(single[...], w_q[...], NT, preferred_element_type=F32)
    query = select(query, c_q[...]) * (LW / math.sqrt(ch))
    q_local = select(
        lax.dot_general(single[...], w_qp[...], NT, preferred_element_type=F32), c_qp[...]
    )
    q_turn = select(full, c_fr[...])
    q_line = q_turn[:, 3 * width : 3 * width + LANES]
    for b in range(3):
        q_line += (
            q_turn[:, b * width : b * width + LANES] * q_local[:, b * LANES : (b + 1) * LANES]
        )
    head_keys = c_masks[0:SUB, :]
    head_points = c_masks[SUB : 2 * SUB, :]
    head_values = c_masks[2 * SUB : 3 * SUB, :]
    wide_query = (query[:, None, :] * head_keys[None]).reshape(rows * SUB, LANES)
    coarse = wide_query.astype(BF16)
    qblk[0] = coarse
    qblk[1] = (wide_query - coarse.astype(F32)).astype(BF16)
    spread = select((q_line[:, None, :] * head_points[None]).reshape(rows * SUB, LANES), c_pa[...])
    spread = spread.reshape(rows, SUB, LANES)
    marks = 3 * pq + 2
    for k in range(marks):
        qpb[:, k] = jnp.broadcast_to(spread[:, :, k : k + 1], (rows, SUB, LANES))

    diagonal = lax.broadcasted_iota(jnp.int32, (SUB, heads), 0) == lax.broadcasted_iota(
        jnp.int32, (SUB, heads), 1
    )

    def down(row):
        column = jnp.sum(jnp.where(diagonal, row, 0.0), axis=1, keepdims=True)
        return jnp.broadcast_to(column, (SUB, LANES))

    raw = down(head_w[...])
    cross = down(chain_b[...]) * LW
    soft = jnp.maximum(raw, 0.0) + jnp.log1p(jnp.exp(-jnp.abs(raw)))
    near = soft * (LW * math.sqrt(2.0 / (9.0 * pq)) / 2.0)

    w_bias = jnp.dot(diagonal.astype(BF16), w_pb[...], preferred_element_type=F32).astype(BF16)

    pltpu.make_async_copy(pair, pv, pair_sem).wait()

    keys = n * half

    def bias_of(i, _):
        bias[i] = LW * lax.dot_general(
            w_bias, pv[i].reshape(keys, LANES), NT, preferred_element_type=F32
        )
        return 0

    lax.fori_loop(0, rows, bias_of, 0, unroll=8)

    short = w_out.shape[1] - LANES
    w_short = w_out[:, 0:short, :].reshape(heads * short, w_out.shape[2])
    wp[...] = jnp.dot(c_perm[...], w_short, preferred_element_type=F32).astype(BF16)
    mine_ft = ft[mine, :]
    for k in range(12):
        rb[k] = jnp.broadcast_to(mine_ft[:, k : k + 1], (half, LANES))
    lane = lax.broadcasted_iota(jnp.int32, (rows, LANES), 1)
    repeat = ((lane & (half - 1)) + p * half == lax.broadcasted_iota(jnp.int32, (rows, LANES), 0)).astype(BF16)
    wide = select(stack[...], repeat)
    lane8 = lax.broadcasted_iota(jnp.int32, (SUB, LANES), 1)
    part8 = lax.div(lane8, half)
    comp8 = lax.broadcasted_iota(jnp.int32, (SUB, LANES), 0) * (LANES // half) + part8
    for b in range(4):
        picked = jnp.zeros((SUB, LANES), F32)
        for k in range(12):
            source = (k - k % 3 + b if k < 9 else 3 * (k - 9) + b) if b < 3 else k
            if b == 3 and k < 9:
                continue
            picked = jnp.where(comp8 == k, wide[source : source + 1, :], picked)
        rsel[b] = picked
    eye_b = (
        lax.broadcasted_iota(jnp.int32, (SUB, w_bb.shape[0]), 0)
        == lax.broadcasted_iota(jnp.int32, (SUB, w_bb.shape[0]), 1)
    ).astype(BF16)
    w_motion = jnp.dot(eye_b, w_bb[...], preferred_element_type=F32).astype(BF16)

    def unpacked(slot):
        piece = [buf[slot * PIECES + k] for k in range(PIECES)]
        near_line = jnp.concatenate(piece[:4], axis=0)
        tail = jnp.zeros((QUARTER, LANES), F32)
        lane4 = lax.broadcasted_iota(jnp.int32, (QUARTER, LANES), 1)
        for k in range(3):
            tail = jnp.where(
                (lane4 >= k * THIRD) & (lane4 < (k + 1) * THIRD), roll(piece[4 + k], k * THIRD - 3 * THIRD, 1), tail
            )
        far_line = jnp.concatenate(piece[4:] + [tail], axis=0)
        far_line = jnp.where(lane16 < 3 * THIRD, far_line, near_line)
        return near_line, jnp.where(lane16 == ONE_LANE, 1.0, far_line)

    span = chunk * half
    acc[...] = jnp.zeros_like(acc)
    alpha[...] = jnp.full(alpha.shape, -1e30, F32)
    def pass_on(these):
        @pl.when(p == 1)
        def _():
            for reach in sorted({abs(o) for o in these}):
                level = [o for o in these if abs(o) == reach]
                for o in level:
                    take(buf, slot_of[o], slot_of[o] + 1, group_of[o])
                    relay(o)
                for o in level:
                    take(rbuf, hub_slot[o], hub_slot[o] + 1, hub_group[o])
                    hub_relay(o)

        @pl.when(p == 0)
        def _():
            for o in these:
                take(buf, slot_of[o], slot_of[o] + 1, group_of[o])

    late = [o for o in anchors if o not in order[:chunk] and abs(o) == max(abs(a) for a in anchors)]
    pass_on([o for o in anchors if o != 0 and o not in late])
    for c in range(n // chunk):
        if c == min(2, n // chunk - 1):
            pass_on(late)
        slots = slice(c * chunk, (c + 1) * chunk)
        first = c * chunk + sum(o in anchors for o in order[slots])
        last = (c + 1) * chunk
        if first < last:
            take(buf, first, last, len(anchors) + c)
        lines = [unpacked(slot) for slot in range(c * chunk, (c + 1) * chunk)]
        kc = jnp.concatenate([a for a, _ in lines], axis=0)
        vc = jnp.concatenate([b for _, b in lines], axis=0)
        kt[...] = kc.T.reshape(LANES // SUB, SUB, span)
        k_coarse = kc.astype(BF16)
        k_fine = (kc - k_coarse.astype(F32)).astype(BF16)
        products = [
            lax.dot_general(a, b, NT, preferred_element_type=F32)
            for a, b in ((qblk[0], k_coarse), (qblk[0], k_fine), (qblk[1], k_coarse))
        ]
        dots[...] = (products[0] + products[1] + products[2]).reshape(rows, SUB, span)
        chain_j = kt[0, 7:8, :]
        mask_j = kt[1, 7:8, :]

        def one_row(i, _):
            far = jnp.zeros((SUB, span), F32)
            for k in range(3 * pq):
                gap = qpb[i, k][:, :span] - kt[k]
                far += gap * gap
            differ = jnp.where(qpb[i, 3 * pq][:, :span] != chain_j, cross[:, :span], 0.0)
            absent = 1.0 - qpb[i, 3 * pq + 1][:, :span] * mask_j
            logits = (
                dots[i]
                + bias[i, :, c * span : (c + 1) * span]
                - near[:, :span] * far
                + differ
                - MASK_PENALTY * absent
            )
            old = alpha[i]
            top = jnp.maximum(old, jnp.max(logits, axis=1, keepdims=True))
            w = jnp.exp(logits - top[:, :span])
            wts[i] = w
            alpha[i] = top
            scale = jnp.exp(old - top)
            acc[i, 1] = acc[i, 1] * scale
            acc[i, 0] = acc[i, 0] * scale + jnp.dot(
                w.astype(BF16),
                pv[i, slots].reshape(span, LANES),
                preferred_element_type=F32,
            )
            return 0

        lax.fori_loop(0, rows, one_row, 0, unroll=rows)
        w_all = wts[...].reshape(rows * SUB, span)
        w_coarse = w_all.astype(BF16)
        w_fine = (w_all - w_coarse.astype(F32)).astype(BF16)
        v_first, v_second, v_third = pieces3(vc)
        value_sums = [
            jnp.dot(a, b, preferred_element_type=F32)
            for a, b in (
                (w_coarse, v_third),
                (w_fine, v_second),
                (w_coarse, v_second),
                (w_fine, v_first),
                (w_coarse, v_first),
            )
        ]
        acc[:, 1] += sum(value_sums[1:], value_sums[0]).reshape(rows, SUB, LANES)

    lane3 = lax.broadcasted_iota(jnp.int32, (rows, SUB, LANES), 2)
    acc[:, 1] = jnp.where(lane3 == TOP_LANE, alpha[...], acc[:, 1])
    give = pltpu.make_async_remote_copy(
        src_ref=acc.at[theirs],
        dst_ref=mbuf,
        send_sem=m_sem.at[0],
        recv_sem=m_sem.at[1],
        device_id={"pair": other},
        device_id_type=MESH,
    )
    give.start()
    give.wait_recv()
    own_p, own_b = acc[mine, 0], acc[mine, 1]
    far_p, far_b = mbuf[:, 0], mbuf[:, 1]
    own_top, far_top = own_b[:, :, TOP_LANE : TOP_LANE + 1], far_b[:, :, TOP_LANE : TOP_LANE + 1]
    top = jnp.maximum(own_top, far_top)
    own_scale, far_scale = jnp.exp(own_top - top), jnp.exp(far_top - top)
    both_b = own_b * own_scale + far_b * far_scale
    total = both_b[:, :, ONE_LANE : ONE_LANE + 1]
    both_b = both_b / total * head_values[None]
    paired = (own_p * own_scale + far_p * far_scale) / total
    mbuf[:, 0] = paired
    sums = jnp.sum(both_b, axis=1)
    first = heads * ch
    third = heads * nv
    moved = [roll(sums, -a * third, 1) - rb[9 + a] for a in range(3)]
    pointed = [sum(rb[3 * a + b] * moved[a] for a in range(3)) for b in range(3)]
    norms = jnp.sqrt(pointed[0] * pointed[0] + pointed[1] * pointed[1] + pointed[2] * pointed[2] + 1.0)
    joined = sums
    for b in range(3):
        joined = jnp.where(
            (lane16 >= first + b * third) & (lane16 < first + (b + 1) * third),
            roll(pointed[b], b * third, 1),
            joined,
        )
    norms = jnp.where((lane16 >= first) & (lane16 < first + third), norms, 0.0)
    features = jnp.concatenate([joined, norms], axis=1).astype(BF16)
    update = jnp.dot(features, wp[...], preferred_element_type=F32)
    for h in range(heads):
        update += jnp.dot(
            mbuf[:, 0, h, :].astype(BF16), w_out[h, short:, :], preferred_element_type=F32
        )

    xbuf[x] = update
    for d in range(1, nx):
        pltpu.make_async_remote_copy(
            src_ref=xbuf.at[x],
            dst_ref=xbuf.at[x],
            send_sem=x_sem.at[0],
            recv_sem=x_sem.at[1],
            device_id={"head": lax.rem(x + d, nx)},
            device_id_type=MESH,
        ).start()
    x_all = pltpu.make_async_remote_copy(
        src_ref=xbuf.at[0 : nx - 1],
        dst_ref=xbuf.at[0 : nx - 1],
        send_sem=x_sem.at[0],
        recv_sem=x_sem.at[1],
        device_id={"head": lax.rem(x + 1, nx)},
        device_id_type=MESH,
    )
    if nx > 1:
        x_all.wait_recv()
    update = xbuf[0]
    for k in range(1, nx):
        update = update + xbuf[k]
    mixed = single[mine, :].astype(F32) + update
    count = mixed.shape[1]
    gains = jnp.concatenate([gain[k : k + 1, :] for k in range(count // LANES)], axis=1)
    centre = jnp.sum(mixed, axis=1, keepdims=True) * (1.0 / count)
    apart = mixed - centre
    variance = jnp.sum(apart * apart, axis=1, keepdims=True) * (1.0 / count)
    result = (apart * lax.rsqrt(variance + 1e-05) * gains).astype(BF16)
    out_single[mine, :] = result
    sbuf[0] = result.astype(F32)
    give_s = pltpu.make_async_remote_copy(
        src_ref=sbuf.at[0],
        dst_ref=sbuf.at[1],
        send_sem=s_sem.at[0],
        recv_sem=s_sem.at[1],
        device_id={"pair": other},
        device_id_type=MESH,
    )

    groups = LANES // half
    motion = lax.dot_general(
        w_motion,
        jnp.concatenate([result] * groups, axis=0),
        NT,
        preferred_element_type=F32,
    )
    m = [jnp.broadcast_to(motion[k : k + 1, :], (SUB, LANES)) for k in range(6)]
    qa = 1.0 / jnp.sqrt(1.0 + m[0] * m[0] + m[1] * m[1] + m[2] * m[2])
    qb, qc, qd = m[0] * qa, m[1] * qa, m[2] * qa
    aa, bb, cc, dd = qa * qa, qb * qb, qc * qc, qd * qd
    ab, ac, ad = qa * qb, qa * qc, qa * qd
    bc, bd, cd = qb * qc, qb * qd, qc * qd
    spin = [
        [aa + bb - cc - dd, 2.0 * (bc - ad), 2.0 * (bd + ac)],
        [2.0 * (bc + ad), aa - bb + cc - dd, 2.0 * (cd - ab)],
        [2.0 * (bd - ac), 2.0 * (cd + ab), aa - bb - cc + dd],
    ]
    column = lax.rem(comp8, 3)
    packed = rsel[3]
    for b in range(3):
        value = jnp.where(column == 0, spin[b][0], jnp.where(column == 1, spin[b][1], spin[b][2]))
        value = jnp.where(comp8 < 9, value, m[3 + b])
        packed = packed + rsel[b] * value
    lines = fbuf.shape[1]
    me = z * 2 + p
    fbuf[me] = packed[0:lines, :]

    steps = sorted(
        ((d, c) for d in range(n) for c in (0, 1) if (d, c) != (0, 0)),
        key=lambda s: (-min(s[0], n - s[0]), s[1]),
    )
    for d, c in steps:
        device = {"blk": lax.rem(z + d, n), "pair": p if c == 0 else other}
        pltpu.make_async_remote_copy(
            src_ref=fbuf.at[me],
            dst_ref=fbuf.at[me],
            send_sem=f_sem.at[0],
            recv_sem=f_sem.at[1],
            device_id=device,
            device_id_type=MESH,
        ).start()
    give_s.start()
    give_s.wait_recv()
    out_single[theirs, :] = sbuf[1].astype(BF16)
    f_all = pltpu.make_async_remote_copy(
        src_ref=fbuf.at[0 : 2 * n - 1],
        dst_ref=fbuf.at[0 : 2 * n - 1],
        send_sem=f_sem.at[0],
        recv_sem=f_sem.at[1],
        device_id={"pair": other},
        device_id_type=MESH,
    )
    f_all.wait_recv()

    gap = (lax.broadcasted_iota(jnp.int32, (SUB, LANES), 0) - part8) & (SUB - 1)
    for t in range(2 * n // groups):
        for line_number in range(2):
            tile = fbuf[t * groups : (t + 1) * groups, line_number, :]
            out = tile
            for s in range(1, groups):
                out = jnp.where(gap == s, roll(roll(tile, s, 0), -half * s, 1), out)
            height = 8 if line_number == 0 else 4
            out_frames[8 * line_number : 8 * line_number + height, t * LANES : (t + 1) * LANES] = out[:height]

    def sent(count, sem):
        pltpu.make_async_remote_copy(
            src_ref=held_block(buf, 0, count),
            dst_ref=held_block(buf, 0, count),
            send_sem=send_sem.at[sem],
            recv_sem=recv_sem.at[0],
            device_id={"blk": lax.rem(z + 1, n)},
            device_id_type=MESH,
        ).wait_send()

    @pl.when(p == 1)
    def _():
        sent(n - 1, 0)
        sent(n - 1 - len(children[0]) + len(anchors) - 1, 1)

    @pl.when(p == 0)
    def _():
        sent(len(children[0]), 0)

    if nx > 1:
        x_all.wait_send()
    f_all.wait_send()
    give.wait_send()
    give_s.wait_send()


def hand_over(single_in, frames_in, single_out, frames_out):
    single_out[...] = single_in[...]
    frames_out[...] = frames_in[...]


def body(n, nx, *args):
    (
        single,
        pair,
        frames,
        chain,
        mask,
        w_q,
        w_kv,
        w_qp,
        w_kvp,
        w_pb,
        head_w,
        chain_b,
        w_out,
        gain,
        w_bb,
    ) = args
    rows, half = single.shape[0], pair.shape[2]
    heads = w_pb.shape[1]
    ch = w_q.shape[1] // heads
    pq = w_qp.shape[1] // (3 * heads)
    nv = w_kvp.shape[1] // (3 * heads) - pq
    chunk = min(8, n)
    order, anchors, children = gather_plan(n, 4 if n >= 16 else 2, chunk, 0.9, 0.72, 1.0)
    deltas = sorted({d for kids in children.values() for _, d in kids})
    deltas = sorted(set(deltas) | {-d for d in deltas})
    deltas = [d for i, d in enumerate(deltas) if d % n not in {e % n for e in deltas[:i]}]
    cfg = (n, nx, heads, ch, pq, nv, half, chunk, order, anchors, children, deltas)
    hots, masks = constants(heads, ch, pq, nv)
    hots = [jnp.asarray(h, BF16) for h in hots]
    masks = jnp.asarray(masks, F32)
    vmem = pl.BlockSpec(memory_space=pltpu.VMEM)
    hbm = pl.BlockSpec(memory_space=pl.ANY)
    loads = [
        frames,
        chain.reshape(1, rows),
        mask.reshape(1, rows),
        single,
        w_kv.T,
        w_kvp.T,
        hots[2],
        hots[1],
        hots[0],
        w_q.T,
        w_qp.T,
        w_pb.T,
        head_w.reshape(1, heads),
        chain_b.reshape(1, heads),
        gain.reshape(-1, LANES),
        w_bb.T,
        w_out,
        hots[3],
        hots[4],
        hots[5],
        hots[6],
        masks,
    ]
    cfg += (len(loads),)
    specs = [hbm] + [hbm] * len(loads)
    marks = 3 * pq + 2
    span = chunk * half
    width = w_out.shape[2]
    scratch = [pltpu.VMEM(a.shape, a.dtype) for a in loads] + [
        pltpu.SemaphoreType.DMA((len(loads),)),
        pltpu.VMEM((rows, n, half, LANES), BF16),
        pltpu.VMEM((n * PIECES, QUARTER, LANES), F32),
        pltpu.VMEM((len(anchors) * PIECES, QUARTER, LANES), F32),
        pltpu.VMEM((16, rows), F32),
        pltpu.VMEM((rows, 16), F32),
        pltpu.VMEM((rows, SUB, n * half), F32),
        pltpu.VMEM((rows, marks, SUB, LANES), F32),
        pltpu.VMEM((2, rows * SUB, LANES), BF16),
        pltpu.VMEM((LANES // SUB, SUB, span), F32),
        pltpu.VMEM((rows, SUB, span), F32),
        pltpu.VMEM((rows, SUB, span), F32),
        pltpu.VMEM((rows, SUB, LANES), F32),
        pltpu.VMEM((rows, 2, SUB, LANES), F32),
        pltpu.VMEM((half, 2, SUB, LANES), F32),
        pltpu.VMEM((nx, half, width), F32),
        pltpu.VMEM((2 * n, 2, LANES), F32),
        pltpu.VMEM((2, half, width), F32),
        pltpu.VMEM((2 * LANES, width), BF16),
        pltpu.VMEM((12, half, LANES), F32),
        pltpu.VMEM((4, SUB, LANES), F32),
        pltpu.SemaphoreType.DMA,
        pltpu.SemaphoreType.DMA((2,)),
        pltpu.SemaphoreType.DMA((2 * len(anchors) + n // chunk,)),
        pltpu.SemaphoreType.DMA((2,)),
        pltpu.SemaphoreType.DMA((2,)),
        pltpu.SemaphoreType.DMA((2,)),
        pltpu.SemaphoreType.DMA((2,)),
    ]
    results = pl.pallas_call(
        functools.partial(kernel, cfg),
        out_shape=(
            jax.ShapeDtypeStruct(single.shape, BF16),
            jax.ShapeDtypeStruct((12, n * rows), F32),
        ),
        in_specs=specs,
        out_specs=(vmem, vmem),
        scratch_shapes=scratch,
        compiler_params=pltpu.CompilerParams(collective_id=0, has_side_effects=True),
        name="layer",
    )(pair, *loads)
    return pl.pallas_call(
        hand_over,
        out_shape=(
            jax.ShapeDtypeStruct(single.shape, BF16),
            jax.ShapeDtypeStruct((12, n * rows), F32),
        ),
        in_specs=[vmem, vmem],
        out_specs=(vmem, vmem),
        name="results",
    )(*results)


def solution(mesh):
    placed = (
        P(("groups", "blk"), None),
        P(("groups", "blk"), None, "pair", None),
        P(None, ("groups", "blk")),
        P(("groups", "blk")),
        P(("groups", "blk")),
        P(None, "head"),
        P(None, "head"),
        P(None, "head"),
        P(None, "head"),
        P(None, "head"),
        P("head"),
        P("head"),
        P("head", None, None),
        P(),
        P(),
    )
    return jax.shard_map(
        functools.partial(body, mesh.shape["blk"], mesh.shape["head"]),
        mesh=mesh,
        in_specs=placed,
        out_specs=(P(("groups", "blk"), None), P(None, "groups")),
        check_vma=False,
    )
```
